8 devices in a mesh: dp: 2 (over z, y), sp: 4 (over x, core).
Axes of the slice: x: 2, y: 2, z: 1, core: 2. Of those that a mesh axis runs over, the one named last changes fastest.
Arguments:
- pair_rep: float32 [256, 128, 128], P(('dp', 'sp')), parts along dimension 0
- w_qkvg_s: bfloat16 [128, 512], replicated
- w_bias_s: bfloat16 [4, 128], replicated
- w_out_s: bfloat16 [128, 128], replicated
- w_qkvg_e: bfloat16 [128, 512], replicated
- w_bias_e: bfloat16 [4, 128], replicated
- w_out_e: bfloat16 [128, 128], replicated
- w_one: bfloat16 [128, 512], replicated
- w_two: bfloat16 [512, 128], replicated
Outputs:
- output: float32 [256, 128, 128], P(('dp', 'sp')), parts along dimension 0
There are 2 independent parts. The reference program is written for one: setup_inputs(seed, part) draws one part's arguments, and reference() takes and returns one part's arrays. A program takes and returns all parts, laid end to end along the dimension named above; an argument that names none is the same for every part.
All inputs are finite; a program needn't handle non-finite values.
Results may differ from the reference program's by a relative error of at most 0.00995982.
Values are sent between devices in bfloat16 or wider.
A program may use at most 1 GiB of HBM per device.

```python
import jax
import jax.numpy as jnp
from jax import lax

N = 128
C_Z = 128
HEADS = 4
HEAD_DIM = C_Z // HEADS
HIDDEN = 4 * C_Z
LN_EPS = 1e-5
OUT_SCALE = (N / 16) ** 0.5


def setup_inputs(seed: int = 0, part: int = 0) -> dict:
    root_key = jax.random.key(seed)
    part_key = jax.random.fold_in(root_key, part)
    shared = jax.random.split(jax.random.fold_in(root_key, 65537), 8)
    in_scale = C_Z ** -0.5
    hid_scale = HIDDEN ** -0.5
    pair_rep = jax.random.normal(part_key, (N, N, C_Z), jnp.float32)
    w_qkvg_s = jax.random.normal(shared[0], (C_Z, 4 * C_Z), jnp.float32) * in_scale
    w_bias_s = jax.random.normal(shared[1], (HEADS, C_Z), jnp.float32) * in_scale
    w_out_s = jax.random.normal(shared[2], (C_Z, C_Z), jnp.float32) * (in_scale * OUT_SCALE)
    w_qkvg_e = jax.random.normal(shared[3], (C_Z, 4 * C_Z), jnp.float32) * in_scale
    w_bias_e = jax.random.normal(shared[4], (HEADS, C_Z), jnp.float32) * in_scale
    w_out_e = jax.random.normal(shared[5], (C_Z, C_Z), jnp.float32) * (in_scale * OUT_SCALE)
    w_one = jax.random.normal(shared[6], (C_Z, HIDDEN), jnp.float32) * in_scale
    w_two = jax.random.normal(shared[7], (HIDDEN, C_Z), jnp.float32) * hid_scale
    return {
        "pair_rep": pair_rep,
        "w_qkvg_s": w_qkvg_s.astype(jnp.bfloat16),
        "w_bias_s": w_bias_s.astype(jnp.bfloat16),
        "w_out_s": w_out_s.astype(jnp.bfloat16),
        "w_qkvg_e": w_qkvg_e.astype(jnp.bfloat16),
        "w_bias_e": w_bias_e.astype(jnp.bfloat16),
        "w_out_e": w_out_e.astype(jnp.bfloat16),
        "w_one": w_one.astype(jnp.bfloat16),
        "w_two": w_two.astype(jnp.bfloat16),
    }


def layer_norm(values):
    vals_f = values.astype(jnp.float32)
    mean_c = jnp.mean(vals_f, axis=-1, keepdims=True)
    centered = vals_f - mean_c
    variance = jnp.mean(centered * centered, axis=-1, keepdims=True)
    return (centered * lax.rsqrt(variance + LN_EPS)).astype(jnp.bfloat16)


def bias_table(pair_in, w_bias):
    def one_row(row_in):
        return jnp.dot(layer_norm(row_in), w_bias.T, preferred_element_type=jnp.float32).astype(jnp.bfloat16)
    return jnp.transpose(lax.map(one_row, pair_in), (2, 0, 1))


def row_update(row_in, bias_full, w_qkvg, w_out):
    seq_len = row_in.shape[0]
    projected = jnp.dot(layer_norm(row_in), w_qkvg, preferred_element_type=jnp.float32)
    split_shape = (seq_len, HEADS, HEAD_DIM)
    queries = projected[:, :C_Z].astype(jnp.bfloat16).reshape(split_shape).astype(jnp.float32)
    key_vecs = projected[:, C_Z:2 * C_Z].astype(jnp.bfloat16).reshape(split_shape).astype(jnp.float32)
    val_vecs = projected[:, 2 * C_Z:3 * C_Z].astype(jnp.bfloat16).reshape(split_shape).astype(jnp.float32)
    gate_vals = jax.nn.sigmoid(projected[:, 3 * C_Z:]).reshape(split_shape)
    scores = jnp.einsum('jhd,khd->hjk', queries, key_vecs) * HEAD_DIM ** -0.5 + bias_full.astype(jnp.float32)
    attn_prob = jax.nn.softmax(scores, axis=-1).astype(jnp.bfloat16).astype(jnp.float32)
    attn_out = jnp.einsum('hjk,khd->jhd', attn_prob, val_vecs)
    gated_out = (attn_out * gate_vals).astype(jnp.bfloat16).reshape(seq_len, C_Z)
    return jnp.dot(gated_out, w_out, preferred_element_type=jnp.float32)


def tri_attention(pair_in, w_qkvg, w_bias, w_out):
    bias_full = bias_table(pair_in, w_bias)

    def one_row(row_in):
        return row_update(row_in, bias_full, w_qkvg, w_out)
    return lax.map(one_row, pair_in)


def reference(pair_rep, w_qkvg_s, w_bias_s, w_out_s, w_qkvg_e, w_bias_e, w_out_e, w_one, w_two):
    pair_one = pair_rep + tri_attention(pair_rep, w_qkvg_s, w_bias_s, w_out_s)
    pair_trans = jnp.swapaxes(pair_one.astype(jnp.bfloat16), 0, 1)
    end_upd = tri_attention(pair_trans, w_qkvg_e, w_bias_e, w_out_e)

    def finish_row(row_pair):
        trans_row, upd_row = row_pair
        pair_two = trans_row.astype(jnp.float32) + upd_row
        hidden = jax.nn.relu(jnp.dot(layer_norm(pair_two), w_one, preferred_element_type=jnp.float32))
        trans_out = jnp.dot(hidden.astype(jnp.bfloat16), w_two, preferred_element_type=jnp.float32)
        return (upd_row + trans_out).astype(jnp.bfloat16)

    delta_trans = lax.map(finish_row, (pair_trans, end_upd))
    return pair_one + jnp.swapaxes(delta_trans, 0, 1).astype(jnp.float32)
```

```python
import functools

import jax
import jax.numpy as jnp
from jax import lax
from jax.experimental import pallas as pl
from jax.experimental.pallas import tpu as pltpu
from jax.sharding import PartitionSpec as P

MESH = pl.DeviceIdType.MESH
EPS = 1e-5
LOG2E = 1.4426950408889634
BF = jnp.bfloat16
F32 = jnp.float32


def dot(a, b):
    return jnp.dot(a, b, preferred_element_type=F32)


def dot_tn(a, b):
    return lax.dot_general(a, b, (((0,), (0,)), ((), ())), preferred_element_type=F32)


def norm_t(xt):
    mean = jnp.sum(xt, axis=0, keepdims=True) * (1.0 / xt.shape[0])
    cen = xt - mean
    var = jnp.sum(cen * cen, axis=0, keepdims=True) * (1.0 / xt.shape[0])
    return (cen * lax.rsqrt(var + EPS)).astype(BF)


def sigmoid(x):
    return 0.5 * jnp.tanh(0.5 * x) + 0.5


def attend(kn, qt, vt, bias_ref, heads):
    hd, n = qt.shape
    d = hd // heads
    scale = LOG2E * d ** -0.5
    outs = []
    for pair in range(heads // 2):
        cols = []
        for h in (2 * pair, 2 * pair + 1):
            parts = []
            if h:
                parts.append(jnp.zeros((h * d, n), BF))
            parts.append(qt[h * d:(h + 1) * d])
            if h < heads - 1:
                parts.append(jnp.zeros(((heads - 1 - h) * d, n), BF))
            cols.append(jnp.concatenate(parts, axis=0))
        s = dot(kn, jnp.concatenate(cols, axis=1)) * scale + bias_ref[:, 2 * pair * n:(2 * pair + 2) * n]
        e = jnp.exp2(s - jnp.max(s, axis=0, keepdims=True))
        p = (e * (1.0 / jnp.sum(e, axis=0, keepdims=True))).astype(BF)
        o = dot(vt[2 * pair * d:(2 * pair + 2) * d], p)
        outs += [o[:d, :n], o[d:, n:]]
    return jnp.concatenate(outs, axis=0)


def project(wt, ut, n, qv_ref, kn_ref, g_ref, p):
    c = ut.shape[0]
    qv_ref[p, :c] = dot(wt[0:c], ut).astype(BF)
    kt = dot(wt[c:2 * c], ut).astype(BF)
    kn_ref[2 * p] = kt[:, :n].T
    kn_ref[2 * p + 1] = kt[:, n:].T
    qv_ref[p, c:] = dot(wt[2 * c:3 * c], ut).astype(BF)
    g_ref[p] = sigmoid(dot(wt[3 * c:], ut))


def kernel(z_hbm, wqs, wbs, wos, wqe, wbe, woe, w1, w2, y_hbm,
           z, ut, qv, kn, g, bloc, bsend, ball, biast, hsend, hcol, besend, beall, dsend, drecv, y,
           wqst, wqet, woet, w1t, w2t,
           zsem, ysem, bs_s, bs_r, h_s, h_r, be_s, be_r, d_s, d_r):
    rows, n, c = z.shape
    heads = wbs.shape[0]
    dp, sp = lax.axis_index("dp"), lax.axis_index("sp")
    x, core = sp // 2, sp % 2
    peers = [2 * (1 - x) + core, 2 * (1 - x) + 1 - core, 2 * x + 1 - core]
    mine = pl.multiple_of(sp * rows, rows)
    zchunks = 4
    zr = rows // zchunks

    def zcopy(i):
        return pltpu.make_async_copy(z_hbm.at[pl.ds(i * zr, zr)], z.at[pl.ds(i * zr, zr)], zsem.at[i])

    for i in range(zchunks):
        zcopy(i).start()
    bar = pltpu.get_barrier_semaphore()
    for t in peers:
        pl.semaphore_signal(bar, inc=1, device_id=(dp, t), device_id_type=MESH)

    def remote(src, dst, ssem, rsem, t):
        return pltpu.make_async_remote_copy(src, dst, ssem, rsem, device_id=(dp, t), device_id_type=MESH)

    wqst[...] = wqs[...].T
    wqet[...] = wqe[...].T
    woet[...] = woe[...].T
    w1t[...] = w1[...].T
    w2t[...] = w2[...].T

    for i in range(zchunks):
        zcopy(i).wait()

        def ln_pair(p, _):
            u = norm_t(jnp.concatenate([z[2 * p].T, z[2 * p + 1].T], axis=1))
            ut[p] = u
            b = dot(wbs[...], u)
            bloc[:, 2 * p] = b[:, :n]
            bloc[:, 2 * p + 1] = b[:, n:]
            return _
        lax.fori_loop(i * zr // 2, (i + 1) * zr // 2, ln_pair, 0)
    bsend[...] = bloc[...].astype(BF)
    ball[:, pl.ds(mine, rows)] = bsend[...]
    pl.semaphore_wait(bar, 3)
    bias_sends = []
    for k, t in enumerate(peers):
        cp = remote(bsend, ball.at[:, pl.ds(mine, rows)], bs_s.at[k], bs_r.at[sp], t)
        cp.start()
        bias_sends.append(cp)

    def proj_pair(p, _):
        project(wqst, ut[p], n, qv, kn, g, p)
        return _
    lax.fori_loop(0, rows // 2, proj_pair, 0)
    for k, t in enumerate(peers):
        remote(bsend, ball.at[:, pl.ds(pl.multiple_of(t * rows, rows), rows)], bs_s.at[k], bs_r.at[t], t).wait_recv()
    for h in range(heads):
        biast[:, h * n:(h + 1) * n] = ball[h].astype(F32).T * LOG2E

    def start_pair(p, _):
        ogs = []
        for r in range(2):
            o = attend(kn[2 * p + r], qv[p, :c, r * n:(r + 1) * n], qv[p, c:, r * n:(r + 1) * n], biast, heads)
            ogs.append((o * g[p, :, r * n:(r + 1) * n]).astype(BF))
        upd = dot_tn(jnp.concatenate(ogs, axis=1), wos[...])
        uts = []
        for r in range(2):
            z1 = z[2 * p + r] + upd[r * n:(r + 1) * n]
            z[2 * p + r] = z1
            uts.append(z1.astype(BF).astype(F32).T)
        b = dot(wbe[...], norm_t(jnp.concatenate(uts, axis=1)))
        bloc[:, 2 * p] = b[:, :n]
        bloc[:, 2 * p + 1] = b[:, n:]
        return _

    groups = rows // 16
    chunks = 4
    cols = rows // chunks
    h_sends = []
    for gi in range(groups):
        lax.fori_loop(gi * 8, (gi + 1) * 8, start_pair, 0)

        def shuffle(jb, _):
            j0 = pl.multiple_of(jb * 8, 8)
            blk = jnp.swapaxes(z[gi * 16:(gi + 1) * 16, pl.ds(j0, 8)], 0, 1)
            hsend[pl.ds(j0, 8), gi * 16:(gi + 1) * 16] = blk.astype(BF)
            return _
        lax.fori_loop(0, n // 8, shuffle, 0)
        dst_rows = pl.ds(pl.multiple_of(mine + gi * 16, 16), 16)
        for ch in range(chunks):
            for k, t in enumerate(peers):
                cp = remote(hsend.at[pl.ds(t * rows + ch * cols, cols), gi * 16:(gi + 1) * 16],
                            hcol.at[ch * cols:(ch + 1) * cols, dst_rows],
                            h_s.at[gi, ch, k], h_r.at[gi, ch, sp], t)
                cp.start()
                h_sends.append(cp)
        hcol[:, dst_rows] = hsend[pl.ds(mine, rows), gi * 16:(gi + 1) * 16]
    besend[...] = bloc[...].astype(BF)
    beall[:, pl.ds(mine, rows)] = besend[...]
    for k, t in enumerate(peers):
        cp = remote(besend, beall.at[:, pl.ds(mine, rows)], be_s.at[k], be_r.at[sp], t)
        cp.start()
        bias_sends.append(cp)
    for k, t in enumerate(peers):
        remote(besend, beall.at[:, pl.ds(pl.multiple_of(t * rows, rows), rows)], be_s.at[k], be_r.at[t], t).wait_recv()
    for h in range(heads):
        biast[:, h * n:(h + 1) * n] = beall[h].astype(F32) * LOG2E

    def end_pair(p, _):
        wt = jnp.concatenate([hcol[2 * p].astype(F32).T, hcol[2 * p + 1].astype(F32).T], axis=1)
        project(wqet, norm_t(wt), n, qv, kn, g, p)
        ogs = []
        for r in range(2):
            o = attend(kn[2 * p + r], qv[p, :c, r * n:(r + 1) * n], qv[p, c:, r * n:(r + 1) * n], biast, heads)
            ogs.append((o * g[p, :, r * n:(r + 1) * n]).astype(BF))
        e = dot(woet[...], jnp.concatenate(ogs, axis=1))
        hid = jnp.maximum(dot(w1t[...], norm_t(wt + e)), 0.0).astype(BF)
        delta = (e + dot(w2t[...], hid)).astype(BF)
        dsend[2 * p] = delta[:, :n].T
        dsend[2 * p + 1] = delta[:, n:].T
        return _

    d_sends = []
    for ch in range(chunks):
        for gi in range(groups):
            for k, t in enumerate(peers):
                remote(hsend.at[pl.ds(t * rows + ch * cols, cols), gi * 16:(gi + 1) * 16],
                       hcol.at[ch * cols:(ch + 1) * cols, pl.ds(pl.multiple_of(t * rows + gi * 16, 16), 16)],
                       h_s.at[gi, ch, k], h_r.at[gi, ch, t], t).wait_recv()
        lax.fori_loop(ch * cols // 2, (ch + 1) * cols // 2, end_pair, 0)
        for k, t in enumerate(peers):
            cp = remote(dsend.at[ch * cols:(ch + 1) * cols, pl.ds(pl.multiple_of(t * rows, rows), rows)],
                        drecv.at[pl.ds(mine + ch * cols, cols)],
                        d_s.at[ch, k], d_r.at[ch, sp], t)
            cp.start()
            d_sends.append(cp)
    drecv[pl.ds(mine, rows)] = dsend[:, pl.ds(mine, rows)]

    def final_block(j0):
        for gi in range(groups):
            blk = jnp.swapaxes(drecv[pl.ds(j0, 8), gi * 16:(gi + 1) * 16].astype(F32), 0, 1)
            y[gi * 16:(gi + 1) * 16, pl.ds(j0, 8)] = z[gi * 16:(gi + 1) * 16, pl.ds(j0, 8)] + blk

    for ch in range(chunks):
        final_block(pl.multiple_of(mine + ch * cols, 8))
    for ch in range(chunks):
        for k, t in enumerate(peers):
            remote(dsend.at[ch * cols:(ch + 1) * cols, pl.ds(pl.multiple_of(t * rows, rows), rows)],
                   drecv.at[pl.ds(t * rows + ch * cols, cols)],
                   d_s.at[ch, k], d_r.at[ch, t], t).wait_recv()
            final_block(pl.multiple_of(t * rows + ch * cols, 8))
    ycopy = pltpu.make_async_copy(y, y_hbm, ysem)
    ycopy.start()
    for cp in bias_sends + h_sends + d_sends:
        cp.wait_send()
    ycopy.wait()


def solution(mesh):
    row_spec = P(('dp', 'sp'), None, None)
    sp = mesh.shape['sp']

    def local_fn(pair_loc, wqs, wbs, wos, wqe, wbe, woe, w1, w2):
        rows, n, c = pair_loc.shape
        heads = wbs.shape[0]
        dma = pltpu.SemaphoreType.DMA
        vmem = pl.BlockSpec(memory_space=pltpu.VMEM)
        return pl.pallas_call(
            kernel,
            out_shape=jax.ShapeDtypeStruct(pair_loc.shape, F32),
            in_specs=[pl.BlockSpec(memory_space=pl.ANY)] + [vmem] * 8,
            out_specs=pl.BlockSpec(memory_space=pl.ANY),
            scratch_shapes=[
                pltpu.VMEM((rows, n, c), F32),
                pltpu.VMEM((rows // 2, c, 2 * n), BF),
                pltpu.VMEM((rows // 2, 2 * c, 2 * n), BF),
                pltpu.VMEM((rows, n, c), BF),
                pltpu.VMEM((rows // 2, c, 2 * n), F32),
                pltpu.VMEM((heads, rows, n), F32),
                pltpu.VMEM((heads, rows, n), BF),
                pltpu.VMEM((heads, n, n), BF),
                pltpu.VMEM((n, heads * n), F32),
                pltpu.VMEM((n, rows, c), BF),
                pltpu.VMEM((rows, n, c), BF),
                pltpu.VMEM((heads, rows, n), BF),
                pltpu.VMEM((heads, n, n), BF),
                pltpu.VMEM((rows, n, c), BF),
                pltpu.VMEM((n, rows, c), BF),
                pltpu.VMEM((rows, n, c), F32),
                pltpu.VMEM(wqs.shape[::-1], BF),
                pltpu.VMEM(wqe.shape[::-1], BF),
                pltpu.VMEM(woe.shape[::-1], BF),
                pltpu.VMEM(w1.shape[::-1], BF),
                pltpu.VMEM(w2.shape[::-1], BF),
                dma((4,)), dma,
                dma((3,)), dma((sp,)),
                dma((rows // 16, 4, 3)), dma((rows // 16, 4, sp)),
                dma((3,)), dma((sp,)),
                dma((4, 3)), dma((4, sp)),
            ],
            compiler_params=pltpu.CompilerParams(collective_id=0, has_side_effects=True, vmem_limit_bytes=60 * 2 ** 20),
            name="pair_block",
        )(pair_loc, wqs, wbs, wos, wqe, wbe, woe, w1, w2)

    return jax.shard_map(local_fn, mesh=mesh, in_specs=(row_spec,) + (P(),) * 8, out_specs=row_spec, check_vma=False)
```

```python
import functools

import jax
import jax.numpy as jnp
from jax import lax
from jax.experimental import pallas as pl
from jax.experimental.pallas import tpu as pltpu
from jax.sharding import PartitionSpec as P

MESH = pl.DeviceIdType.MESH
EPS = 1e-5
LOG2E = 1.4426950408889634
BF = jnp.bfloat16
F32 = jnp.float32


def dot(a, b):
    return jnp.dot(a, b, preferred_element_type=F32)


def dot_tn(a, b):
    return lax.dot_general(a, b, (((0,), (0,)), ((), ())), preferred_element_type=F32)


def norm_t(xt):
    mean = jnp.sum(xt, axis=0, keepdims=True) * (1.0 / xt.shape[0])
    cen = xt - mean
    var = jnp.sum(cen * cen, axis=0, keepdims=True) * (1.0 / xt.shape[0])
    return (cen * lax.rsqrt(var + EPS)).astype(BF)


def sigmoid(x):
    return 0.5 * jnp.tanh(0.5 * x) + 0.5


def block_diag(qt, pair, heads):
    hd, n = qt.shape
    d = hd // heads
    cols = []
    for h in (2 * pair, 2 * pair + 1):
        parts = []
        if h:
            parts.append(jnp.zeros((h * d, n), BF))
        parts.append(qt[h * d:(h + 1) * d])
        if h < heads - 1:
            parts.append(jnp.zeros(((heads - 1 - h) * d, n), BF))
        cols.append(jnp.concatenate(parts, axis=0))
    return jnp.concatenate(cols, axis=1)


def stage_scores(kn, qv, s, p, heads):
    c, n = kn.shape[1:]
    for r in range(2):
        keys = kn[2 * p + r]
        qt = qv[p, :c, r * n:(r + 1) * n]
        for pair in range(heads // 2):
            s[r, :, 2 * pair * n:(2 * pair + 2) * n] = dot(keys, block_diag(qt, pair, heads))


def stage_mix(s, biast, qv, g, og, p, heads):
    n = s.shape[1]
    c = qv.shape[1] // 2
    d = c // heads
    scale = LOG2E * d ** -0.5
    for r in range(2):
        for pair in range(heads // 2):
            probs = []
            for h in (2 * pair, 2 * pair + 1):
                t = s[r, :, h * n:(h + 1) * n] * scale + biast[:, h * n:(h + 1) * n]
                e = jnp.exp2(t - jnp.max(t, axis=0, keepdims=True))
                probs.append((e * (1.0 / jnp.sum(e, axis=0, keepdims=True))).astype(BF))
            rows = slice(c + 2 * pair * d, c + (2 * pair + 2) * d)
            o = dot(qv[p, rows, r * n:(r + 1) * n], jnp.concatenate(probs, axis=1))
            for i in range(2):
                h = 2 * pair + i
                out = o[i * d:(i + 1) * d, i * n:(i + 1) * n] * g[p, h * d:(h + 1) * d, r * n:(r + 1) * n]
                og[p, h * d:(h + 1) * d, r * n:(r + 1) * n] = out.astype(BF)


def project(wt, u, n, qv_ref, kn_ref, g_ref, p):
    c = u.shape[0]
    qv_ref[p, :c] = dot(wt[0:c], u).astype(BF)
    kt = dot(wt[c:2 * c], u).astype(BF)
    kn_ref[2 * p] = kt[:, :n].T
    kn_ref[2 * p + 1] = kt[:, n:].T
    qv_ref[p, c:] = dot(wt[2 * c:3 * c], u).astype(BF)
    g_ref[p] = sigmoid(dot(wt[3 * c:], u))


def kernel(z_hbm, wqs, wbs, wos, wqe, wbe, woe, w1, w2, y_hbm,
           z, ut, qv, kn, g, bloc, bsend, ball, biast, hsend, hcol, besend, beall, dsend, drecv, y, s, og, eb, u2,
           wqst, wqet, woet, w1t, w2t,
           zsem, ysem, bs_s, bs_r, h_s, h_r, be_s, be_r, d_s, d_r):
    rows, n, c = z.shape
    heads = wbs.shape[0]
    dp, sp = lax.axis_index("dp"), lax.axis_index("sp")
    x, core = sp // 2, sp % 2
    peers = [2 * (1 - x) + core, 2 * (1 - x) + 1 - core, 2 * x + 1 - core]
    mine = pl.multiple_of(sp * rows, rows)
    zchunks = 4
    zr = rows // zchunks

    def zcopy(i):
        return pltpu.make_async_copy(z_hbm.at[pl.ds(i * zr, zr)], z.at[pl.ds(i * zr, zr)], zsem.at[i])

    for i in range(zchunks):
        zcopy(i).start()
    bar = pltpu.get_barrier_semaphore()
    for t in peers:
        pl.semaphore_signal(bar, inc=1, device_id=(dp, t), device_id_type=MESH)

    def remote(src, dst, ssem, rsem, t):
        return pltpu.make_async_remote_copy(src, dst, ssem, rsem, device_id=(dp, t), device_id_type=MESH)

    wqst[...] = wqs[...].T
    wqet[...] = wqe[...].T
    woet[...] = woe[...].T
    w1t[...] = w1[...].T
    w2t[...] = w2[...].T

    for i in range(zchunks):
        zcopy(i).wait()

        def ln_pair(p, _):
            u = norm_t(jnp.concatenate([z[2 * p].T, z[2 * p + 1].T], axis=1))
            ut[p] = u
            b = dot(wbs[...], u)
            bloc[:, 2 * p] = b[:, :n]
            bloc[:, 2 * p + 1] = b[:, n:]
            return _
        lax.fori_loop(i * zr // 2, (i + 1) * zr // 2, ln_pair, 0)
    bsend[...] = bloc[...].astype(BF)
    ball[:, pl.ds(mine, rows)] = bsend[...]
    pl.semaphore_wait(bar, 3)
    bias_sends = []
    for k, t in enumerate(peers):
        cp = remote(bsend, ball.at[:, pl.ds(mine, rows)], bs_s.at[k], bs_r.at[sp], t)
        cp.start()
        bias_sends.append(cp)

    def proj_pair(p, _):
        project(wqst, ut[p], n, qv, kn, g, p)
        return _
    lax.fori_loop(0, rows // 2, proj_pair, 0)
    for k, t in enumerate(peers):
        remote(bsend, ball.at[:, pl.ds(pl.multiple_of(t * rows, rows), rows)], bs_s.at[k], bs_r.at[t], t).wait_recv()
    for h in range(heads):
        biast[:, h * n:(h + 1) * n] = ball[h].astype(F32).T * LOG2E

    last = rows // 2 - 1

    def lag(t, by):
        return jnp.clip(t - by, 0, last)

    def start_step(t, _):
        p = lag(t, 3)
        u = norm_t(jnp.concatenate([y[2 * p].astype(BF).astype(F32).T, y[2 * p + 1].astype(BF).astype(F32).T], axis=1))
        b = dot(wbe[...], u)
        bloc[:, 2 * p] = b[:, :n]
        bloc[:, 2 * p + 1] = b[:, n:]
        p = lag(t, 2)
        upd = dot_tn(og[p], wos[...])
        y[2 * p] = z[2 * p] + upd[:n]
        y[2 * p + 1] = z[2 * p + 1] + upd[n:]
        stage_mix(s, biast, qv, g, og, lag(t, 1), heads)
        stage_scores(kn, qv, s, lag(t, 0), heads)
        return _

    groups = rows // 16
    chunks = 4
    cols = rows // chunks
    h_sends = []
    for gi in range(groups):
        lax.fori_loop(gi * 8 + 2 * (gi > 0), (gi + 1) * 8 + 2 + (gi == groups - 1), start_step, 0)

        def shuffle(jb, _):
            j0 = pl.multiple_of(jb * 8, 8)
            blk = jnp.swapaxes(y[gi * 16:(gi + 1) * 16, pl.ds(j0, 8)], 0, 1)
            hsend[pl.ds(j0, 8), gi * 16:(gi + 1) * 16] = blk.astype(BF)
            return _
        lax.fori_loop(0, n // 8, shuffle, 0)
        dst_rows = pl.ds(pl.multiple_of(mine + gi * 16, 16), 16)
        for ch in range(chunks):
            for k, t in enumerate(peers):
                cp = remote(hsend.at[pl.ds(t * rows + ch * cols, cols), gi * 16:(gi + 1) * 16],
                            hcol.at[ch * cols:(ch + 1) * cols, dst_rows],
                            h_s.at[gi, ch, k], h_r.at[gi, ch, sp], t)
                cp.start()
                h_sends.append(cp)
        hcol[:, dst_rows] = hsend[pl.ds(mine, rows), gi * 16:(gi + 1) * 16]
    besend[...] = bloc[...].astype(BF)
    beall[:, pl.ds(mine, rows)] = besend[...]
    for k, t in enumerate(peers):
        cp = remote(besend, beall.at[:, pl.ds(mine, rows)], be_s.at[k], be_r.at[sp], t)
        cp.start()
        bias_sends.append(cp)
    for k, t in enumerate(peers):
        remote(besend, beall.at[:, pl.ds(pl.multiple_of(t * rows, rows), rows)], be_s.at[k], be_r.at[t], t).wait_recv()
    for h in range(heads):
        biast[:, h * n:(h + 1) * n] = beall[h].astype(F32) * LOG2E

    def end_step(t, _):
        p = lag(t, 4)
        hid = jnp.maximum(dot(w1t[...], u2[p % 2]), 0.0).astype(BF)
        delta = (eb[p % 2] + dot(w2t[...], hid)).astype(BF)
        dsend[2 * p] = delta[:, :n].T
        dsend[2 * p + 1] = delta[:, n:].T
        p = lag(t, 3)
        wt = jnp.concatenate([hcol[2 * p].astype(F32).T, hcol[2 * p + 1].astype(F32).T], axis=1)
        e = dot(woet[...], og[p])
        eb[p % 2] = e
        u2[p % 2] = norm_t(wt + e)
        stage_mix(s, biast, qv, g, og, lag(t, 2), heads)
        stage_scores(kn, qv, s, lag(t, 1), heads)
        p = lag(t, 0)
        wt = jnp.concatenate([hcol[2 * p].astype(F32).T, hcol[2 * p + 1].astype(F32).T], axis=1)
        project(wqet, norm_t(wt), n, qv, kn, g, p)
        return _

    d_sends = []
    per = cols // 2
    for ch in range(chunks + 1):
        if ch < chunks:
            for gi in range(groups):
                for k, t in enumerate(peers):
                    remote(hsend.at[pl.ds(t * rows + ch * cols, cols), gi * 16:(gi + 1) * 16],
                           hcol.at[ch * cols:(ch + 1) * cols, pl.ds(pl.multiple_of(t * rows + gi * 16, 16), 16)],
                           h_s.at[gi, ch, k], h_r.at[gi, ch, t], t).wait_recv()
        lax.fori_loop(ch * per, (ch + 1) * per, end_step, 0)
        if ch:
            for k, t in enumerate(peers):
                cp = remote(dsend.at[(ch - 1) * cols:ch * cols, pl.ds(pl.multiple_of(t * rows, rows), rows)],
                            drecv.at[pl.ds(mine + (ch - 1) * cols, cols)],
                            d_s.at[ch - 1, k], d_r.at[ch - 1, sp], t)
                cp.start()
                d_sends.append(cp)
    drecv[pl.ds(mine, rows)] = dsend[:, pl.ds(mine, rows)]

    def final_block(j0):
        for gi in range(groups):
            blk = jnp.swapaxes(drecv[pl.ds(j0, 8), gi * 16:(gi + 1) * 16].astype(F32), 0, 1)
            y[gi * 16:(gi + 1) * 16, pl.ds(j0, 8)] += blk

    for ch in range(chunks):
        final_block(pl.multiple_of(mine + ch * cols, 8))
    for ch in range(chunks):
        for k, t in enumerate(peers):
            remote(dsend.at[ch * cols:(ch + 1) * cols, pl.ds(pl.multiple_of(t * rows, rows), rows)],
                   drecv.at[pl.ds(t * rows + ch * cols, cols)],
                   d_s.at[ch, k], d_r.at[ch, t], t).wait_recv()
            final_block(pl.multiple_of(t * rows + ch * cols, 8))
    ycopy = pltpu.make_async_copy(y, y_hbm, ysem)
    ycopy.start()
    for cp in bias_sends + h_sends + d_sends:
        cp.wait_send()
    ycopy.wait()


def solution(mesh):
    row_spec = P(('dp', 'sp'), None, None)
    sp = mesh.shape['sp']

    def local_fn(pair_loc, wqs, wbs, wos, wqe, wbe, woe, w1, w2):
        rows, n, c = pair_loc.shape
        heads = wbs.shape[0]
        dma = pltpu.SemaphoreType.DMA
        vmem = pl.BlockSpec(memory_space=pltpu.VMEM)
        return pl.pallas_call(
            kernel,
            out_shape=jax.ShapeDtypeStruct(pair_loc.shape, F32),
            in_specs=[pl.BlockSpec(memory_space=pl.ANY)] + [vmem] * 8,
            out_specs=pl.BlockSpec(memory_space=pl.ANY),
            scratch_shapes=[
                pltpu.VMEM((rows, n, c), F32),
                pltpu.VMEM((rows // 2, c, 2 * n), BF),
                pltpu.VMEM((rows // 2, 2 * c, 2 * n), BF),
                pltpu.VMEM((rows, n, c), BF),
                pltpu.VMEM((rows // 2, c, 2 * n), F32),
                pltpu.VMEM((heads, rows, n), F32),
                pltpu.VMEM((heads, rows, n), BF),
                pltpu.VMEM((heads, n, n), BF),
                pltpu.VMEM((n, heads * n), F32),
                pltpu.VMEM((n, rows, c), BF),
                pltpu.VMEM((rows, n, c), BF),
                pltpu.VMEM((heads, rows, n), BF),
                pltpu.VMEM((heads, n, n), BF),
                pltpu.VMEM((rows, n, c), BF),
                pltpu.VMEM((n, rows, c), BF),
                pltpu.VMEM((rows, n, c), F32),
                pltpu.VMEM((2, n, heads * n), F32),
                pltpu.VMEM((rows // 2, c, 2 * n), BF),
                pltpu.VMEM((2, c, 2 * n), F32),
                pltpu.VMEM((2, c, 2 * n), BF),
                pltpu.VMEM(wqs.shape[::-1], BF),
                pltpu.VMEM(wqe.shape[::-1], BF),
                pltpu.VMEM(woe.shape[::-1], BF),
                pltpu.VMEM(w1.shape[::-1], BF),
                pltpu.VMEM(w2.shape[::-1], BF),
                dma((4,)), dma,
                dma((3,)), dma((sp,)),
                dma((rows // 16, 4, 3)), dma((rows // 16, 4, sp)),
                dma((3,)), dma((sp,)),
                dma((4, 3)), dma((4, sp)),
            ],
            compiler_params=pltpu.CompilerParams(collective_id=0, has_side_effects=True, vmem_limit_bytes=60 * 2 ** 20),
            name="pair_block",
        )(pair_loc, wqs, wbs, wos, wqe, wbe, woe, w1, w2)

    return jax.shard_map(local_fn, mesh=mesh, in_specs=(row_spec,) + (P(),) * 8, out_specs=row_spec, check_vma=False)
```

```python
import functools

import jax
import jax.numpy as jnp
from jax import lax
from jax.experimental import pallas as pl
from jax.experimental.pallas import tpu as pltpu
from jax.sharding import PartitionSpec as P

MESH = pl.DeviceIdType.MESH
EPS = 1e-5
LOG2E = 1.4426950408889634
BF = jnp.bfloat16
F32 = jnp.float32


def dot(a, b):
    return jnp.dot(a, b, preferred_element_type=F32)


def dot_tn(a, b):
    return lax.dot_general(a, b, (((0,), (0,)), ((), ())), preferred_element_type=F32)


def norm_t(xt):
    mean = jnp.sum(xt, axis=0, keepdims=True) * (1.0 / xt.shape[0])
    cen = xt - mean
    var = jnp.sum(cen * cen, axis=0, keepdims=True) * (1.0 / xt.shape[0])
    return (cen * lax.rsqrt(var + EPS)).astype(BF)


def sigmoid(x):
    return 0.5 * jnp.tanh(0.5 * x) + 0.5


def block_diag(qt, pair, heads):
    hd, n = qt.shape
    d = hd // heads
    cols = []
    for h in (2 * pair, 2 * pair + 1):
        parts = []
        if h:
            parts.append(jnp.zeros((h * d, n), BF))
        parts.append(qt[h * d:(h + 1) * d])
        if h < heads - 1:
            parts.append(jnp.zeros(((heads - 1 - h) * d, n), BF))
        cols.append(jnp.concatenate(parts, axis=0))
    return jnp.concatenate(cols, axis=1)


def stage_scores(kn, qv, s, p, heads):
    c, n = kn.shape[1:]
    for r in range(2):
        keys = kn[2 * p + r]
        qt = qv[p, :c, r * n:(r + 1) * n]
        for pair in range(heads // 2):
            s[r, :, 2 * pair * n:(2 * pair + 2) * n] = dot(keys, block_diag(qt, pair, heads))


def stage_mix(s, biast, qv, g, og, p, heads):
    n = s.shape[1]
    c = qv.shape[1] // 2
    d = c // heads
    scale = LOG2E * d ** -0.5
    for r in range(2):
        for pair in range(heads // 2):
            probs = []
            for h in (2 * pair, 2 * pair + 1):
                t = s[r, :, h * n:(h + 1) * n] * scale + biast[:, h * n:(h + 1) * n]
                e = jnp.exp2(t - jnp.max(t, axis=0, keepdims=True))
                probs.append((e * (1.0 / jnp.sum(e, axis=0, keepdims=True))).astype(BF))
            rows = slice(c + 2 * pair * d, c + (2 * pair + 2) * d)
            o = dot(qv[p, rows, r * n:(r + 1) * n], jnp.concatenate(probs, axis=1))
            for i in range(2):
                h = 2 * pair + i
                out = o[i * d:(i + 1) * d, i * n:(i + 1) * n] * g[p, h * d:(h + 1) * d, r * n:(r + 1) * n]
                og[p, h * d:(h + 1) * d, r * n:(r + 1) * n] = out.astype(BF)


def norm_blocks(src, ut, b0, count):
    for r in range(count):
        ut[b0 + r] = norm_t(src[b0 + r])


def head_rows(wb):
    heads, c = wb.shape
    rep = jnp.broadcast_to(wb.astype(F32)[:, None, :], (heads, 8, c)).reshape(heads * 8, c)
    row = lax.broadcasted_iota(jnp.int32, rep.shape, 0) % 8
    return jnp.concatenate([jnp.where(row == j, rep, 0.0) for j in range(8)], axis=1).astype(BF)


def bias_rows(w8, ub, dst, swap=None):
    heads, rows, n = dst.shape
    c = ub.shape[1]
    half = n // 2
    for i in range(rows // 16):
        r0, r1 = [dot(w8, ub[s * rows // 2 + 8 * i:s * rows // 2 + 8 * i + 8].reshape(8 * c, n)) for s in range(2)]
        parts = []
        for lane in (0, half):
            own, oth = r0[:, lane:lane + half], r1[:, lane:lane + half]
            row = jnp.concatenate([own, oth], axis=1)
            if swap is not None:
                row = jnp.where(swap, jnp.concatenate([oth, own], axis=1), row)
            parts.append(row.reshape(heads, 8, n))
        first, second = parts
        dst[:, 16 * i:16 * i + 16] = jnp.concatenate([first[:, :4], second[:, :4], first[:, 4:], second[:, 4:]], axis=1).astype(BF)


def low_half(shape):
    return lax.broadcasted_iota(jnp.int32, shape, 1) < shape[1] // 2


def pair_project(wt, ub, qb, kt_ref, vst, g, p, npair, heads):
    own, oth = ub[p], ub[npair + p]
    c, n = own.shape
    d, half = c // heads, n // 2
    u = jnp.concatenate([own, oth], axis=1)
    q = dot(wt[0:c], u).astype(BF)
    qb[p] = q[:, :n]
    qb[npair + p] = q[:, n:]
    u_row = jnp.concatenate([own[:, :half], oth[:, :half], own[:, half:], oth[:, half:]], axis=1)
    k = dot(wt[c:2 * c], u_row).astype(BF)
    v = dot(wt[2 * c:3 * c], u_row).astype(BF)
    for h in range(heads):
        for i in range(2):
            rows = pl.ds((h % 2) * 2 * d + i * d, d)
            kt_ref[h // 2, rows] = k[h * d:(h + 1) * d, i * n:(i + 1) * n]
            vst[p, h // 2, rows] = v[h * d:(h + 1) * d, i * n:(i + 1) * n]
    gate = sigmoid(dot(wt[3 * c:], u))
    g[p] = gate[:, :n]
    g[npair + p] = gate[:, n:]


def block_scores(kn, qb, s, slot, b, p, heads):
    c, n = qb.shape[1:]
    d = c // heads
    low = low_half((d, n))
    zero = jnp.zeros((d, n), BF)
    for pair in range(heads // 2):
        rows = []
        for i in range(2):
            q = qb[b, (2 * pair + i) * d:(2 * pair + i + 1) * d]
            for part in (jnp.where(low, q, zero), jnp.where(low, zero, q)):
                rows.append(jnp.concatenate([part, zero] if i == 0 else [zero, part], axis=1))
        s[slot, :, 2 * pair * n:(2 * pair + 2) * n] = dot(kn[p, pair], jnp.concatenate(rows, axis=0))


def softmax_t(t):
    e = jnp.exp2(t - jnp.max(t, axis=0, keepdims=True))
    return (e * (1.0 / jnp.sum(e, axis=0, keepdims=True))).astype(BF)


def block_mix(s, slot, biast, side, vst, g, og, b, p, heads):
    c, n = og.shape[1:]
    d = c // heads
    low = low_half((d, n))
    for h in range(heads):
        t = s[slot, :, h * n:(h + 1) * n] * (LOG2E * d ** -0.5) + biast[side, :, h * n:(h + 1) * n]
        o = dot(vst[p, h // 2, (h % 2) * 2 * d:(h % 2 + 1) * 2 * d], softmax_t(t))
        og[b, h * d:(h + 1) * d] = (jnp.where(low, o[:d], o[d:]) * g[b, h * d:(h + 1) * d]).astype(BF)


def project(wt, u, n, qv_ref, kt_ref, g_ref, p):
    c = u.shape[0]
    qv_ref[p, :c] = dot(wt[0:c], u).astype(BF)
    kt_ref[...] = dot(wt[c:2 * c], u).astype(BF)
    qv_ref[p, c:] = dot(wt[2 * c:3 * c], u).astype(BF)
    g_ref[p] = sigmoid(dot(wt[3 * c:], u))


def turn_keys(kt_ref, kn_ref, p):
    n = kn_ref.shape[1]
    kn_ref[2 * p] = kt_ref[:, :n].T
    kn_ref[2 * p + 1] = kt_ref[:, n:].T


def kernel(z_hbm, wqs_h, wbs_h, wos_h, wqe_h, wbe_h, woe_h, w1_h, w2_h, y,
           zs, z1, ub, qb, vst, knp, gb, ogb, bsend, ball, biasp, hsend,
           hcol, qv, kn, g, og, besend, beall, biast, dsend, drecv, s, eb, u2, kt, ktp,
           wqs, wbs, wos, wqe, wbe, woe, w1, w2, wqst, wqet, woet, w1t, w2t, wbs8, wbe8,
           zsem, wsem, bs_s, bs_r, h_s, h_r, o_s, o_r, be_s, be_r, d_s, d_r):
    rows, n, c = y.shape
    npair = rows // 2
    half = n // 2
    heads = wbs.shape[0]
    dp, sp = lax.axis_index("dp"), lax.axis_index("sp")
    x, core = sp // 2, sp % 2
    peers = [2 * (1 - x) + core, 2 * (1 - x) + 1 - core, 2 * x + 1 - core]
    mine = pl.multiple_of(sp * rows, rows)

    def zcopy(ci, i):
        q, side = ci // 2, ci % 2
        return pltpu.make_async_copy(z_hbm.at[q, i, :, pl.ds(pl.multiple_of((x + side) % 2 * half, half), half)],
                                     zs.at[pl.ds(side * npair + 4 * q, 4), pl.ds(i * half, half)], zsem.at[ci, i])

    def wcopy(i):
        src = (wbs_h, wqs_h, wqe_h, woe_h, w1_h, w2_h, wbe_h, wos_h)[i]
        return pltpu.make_async_copy(src, (wbs, wqs, wqe, woe, w1, w2, wbe, wos)[i], wsem.at[i])

    for ci in range(8):
        zcopy(ci, 0).start()
        zcopy(ci, 1).start()
        if ci == 1:
            wcopy(0).start()
            wcopy(1).start()
    for i in range(2, 8):
        wcopy(i).start()
    bar = pltpu.get_barrier_semaphore()
    for t in peers:
        pl.semaphore_signal(bar, inc=1, device_id=(dp, t), device_id_type=MESH)

    def remote(src, dst, ssem, rsem, t):
        return pltpu.make_async_remote_copy(src, dst, ssem, rsem, device_id=(dp, t), device_id_type=MESH)

    def chunk_base(ci):
        return ci % 2 * npair + ci // 2 * 4

    def ln_step(ci, _):
        norm_blocks(y, ub, chunk_base(jnp.maximum(ci - 1, 0)), 4)
        zcopy(ci, 0).wait()
        zcopy(ci, 1).wait()
        b0 = chunk_base(ci)
        for r in range(4):
            y[b0 + r] = zs[b0 + r].T
        return _
    lax.fori_loop(0, 8, ln_step, 0)
    norm_blocks(y, ub, chunk_base(7), 4)
    wcopy(0).wait()
    wbs8[...] = head_rows(wbs[...])
    bias_rows(wbs8[...], ub, bsend)
    ball[:, pl.ds(pl.multiple_of(core * rows, rows), rows)] = bsend[...]
    pl.semaphore_wait(bar, 3)

    def bias_copy(k, t, owner):
        return remote(bsend, ball.at[:, pl.ds(pl.multiple_of((half if k < 2 else 0) + owner % 2 * rows, rows), rows)],
                      bs_s.at[k], bs_r.at[owner], t)

    def end_bias_copy(k, t, owner):
        return remote(besend, beall.at[:, pl.ds(pl.multiple_of(owner * rows, rows), rows)], be_s.at[k], be_r.at[owner], t)

    for k in (2, 0, 1):
        bias_copy(k, peers[k], sp).start()

    for i in range(1, 8):
        wcopy(i).wait()
    wqst[...] = wqs[...].T
    last = npair - 1

    def lag(t, by):
        return jnp.clip(t - by, 0, last)

    def proj_step(p, _):
        for pair in range(heads // 2):
            knp[jnp.maximum(p - 1, 0), pair] = ktp[pair].T
        pair_project(wqst, ub, qb, ktp, vst, gb, p, npair, heads)
        return _

    def start_bias(side):
        for h in range(heads):
            rws = ball[h, side * half:(side + 1) * half].astype(F32)
            tr = jnp.concatenate([rws, rws], axis=0).T * LOG2E
            if side:
                tr = jnp.concatenate([tr[half:], tr[:half]], axis=0)
            biasp[side, :, h * n:(h + 1) * n] = tr

    def start_step(t, _):
        b = lag(t, 3) * 2
        for r in range(2):
            ub[b + r] = norm_t(z1[b + r].astype(BF).astype(F32).T)
        b = lag(t, 2) * 2
        upd = dot_tn(jnp.concatenate([ogb[b], ogb[b + 1]], axis=1), wos[...])
        z1[b] = zs[b] + upd[:n]
        z1[b + 1] = zs[b + 1] + upd[n:]
        b = lag(t, 1) * 2
        for r in range(2):
            block_mix(s, r, biasp, b // npair, vst, gb, ogb, b + r, b % npair + r, heads)
        b = lag(t, 0) * 2
        for r in range(2):
            block_scores(knp, qb, s, r, b + r, b % npair + r, heads)
        return _

    chunks = 4
    cols = rows // chunks
    groups = [(0, 8), (8, 8), (16, 16)]
    near = [(0, 16), (16, 16)]

    def h_copy(gi, ch, k, t, owner):
        r0, size = groups[gi]
        return remote(hsend.at[0, pl.ds(t % 2 * rows + ch * cols, cols), r0:r0 + size],
                      hcol.at[pl.ds(ch * cols, cols), pl.ds(pl.multiple_of(owner * rows + r0, 8), size)],
                      h_s.at[gi, ch, k], h_r.at[gi, ch, owner], t)

    def near_copy(gi, owner):
        r0, size = near[gi]
        return remote(hsend.at[1, pl.ds(pl.multiple_of((1 - core) * rows, rows), rows), r0:r0 + size],
                      hcol.at[:, pl.ds(pl.multiple_of(owner * rows + r0, 8), size)],
                      o_s.at[gi], o_r.at[gi], peers[2])

    def shuffle_rows(side, r0, size):
        def body(jb, _):
            j0 = pl.multiple_of(jb * 8, 8)
            parts = []
            for q in range(r0 // 8, (r0 + size) // 8):
                for i in range(2):
                    parts.append(z1[side * npair + 4 * q:side * npair + 4 * q + 4, pl.ds(i * half + j0, 8)])
            blk = jnp.swapaxes(jnp.concatenate(parts, axis=0), 0, 1)
            hsend[side, pl.ds(j0, 8), r0:r0 + size] = blk.astype(BF)
            return _
        lax.fori_loop(0, half // 8, body, 0)

    def send_h(gi, chs):
        for ch in chs:
            for k in range(2):
                h_copy(gi, ch, k, peers[k], sp).start()

    def turn_keys_of(p):
        for pair in range(heads // 2):
            knp[p, pair] = ktp[pair].T

    lax.fori_loop(0, npair // 2, proj_step, 0, unroll=2)
    turn_keys_of(npair // 2 - 1)
    bias_copy(2, peers[2], peers[2]).wait_recv()
    start_bias(0)
    lax.fori_loop(0, 4, start_step, 0, unroll=2)
    shuffle_rows(0, 0, 8)
    send_h(0, range(chunks))
    lax.fori_loop(npair // 2, npair, proj_step, 0, unroll=2)
    turn_keys_of(last)
    lax.fori_loop(4, 6, start_step, 0, unroll=2)
    shuffle_rows(0, 8, 8)
    send_h(1, range(chunks))
    for k in range(2):
        bias_copy(k, peers[k], peers[k]).wait_recv()
    start_bias(1)
    lax.fori_loop(6, 10, start_step, 0, unroll=2)
    shuffle_rows(0, 16, 16)
    send_h(2, [0])
    lax.fori_loop(10, 14, start_step, 0, unroll=2)
    shuffle_rows(1, 0, 16)
    near_copy(0, sp).start()
    lax.fori_loop(14, 18, start_step, 0, unroll=2)
    for r in range(2):
        ub[rows - 2 + r] = norm_t(z1[rows - 2 + r].astype(BF).astype(F32).T)
    wbe8[...] = head_rows(wbe[...])
    bias_rows(wbe8[...], ub, besend, x == 1)
    for k in range(3):
        end_bias_copy(k, peers[k], sp).start()
    send_h(2, range(1, chunks))
    beall[:, pl.ds(mine, rows)] = besend[...]
    shuffle_rows(1, 16, 16)
    near_copy(1, sp).start()
    hcol[:, pl.ds(mine, rows)] = hsend[1, pl.ds(pl.multiple_of(core * rows, rows), rows)]
    wqet[...] = wqe[...].T
    woet[...] = woe[...].T
    w1t[...] = w1[...].T
    w2t[...] = w2[...].T
    for k in range(3):
        end_bias_copy(k, peers[k], peers[k]).wait_recv()
    for h in range(heads):
        biast[:, h * n:(h + 1) * n] = beall[h].astype(F32) * LOG2E
    for gi in range(2):
        near_copy(gi, peers[2]).wait_recv()

    def end_step(t, _):
        p = lag(t, 4)
        hid = jnp.maximum(dot(w1t[...], u2[p % 2]), 0.0).astype(BF)
        delta = (eb[p % 2] + dot(w2t[...], hid)).astype(BF)
        dsend[2 * p] = delta[:, :n].T
        dsend[2 * p + 1] = delta[:, n:].T
        p = lag(t, 3)
        wt = jnp.concatenate([hcol[2 * p].astype(F32).T, hcol[2 * p + 1].astype(F32).T], axis=1)
        e = dot(woet[...], og[p])
        eb[p % 2] = e
        u2[p % 2] = norm_t(wt + e)
        stage_mix(s, biast, qv, g, og, lag(t, 2), heads)
        turn_keys(kt, kn, lag(t, 1))
        stage_scores(kn, qv, s, lag(t, 1), heads)
        p = lag(t, 0)
        wt = jnp.concatenate([hcol[2 * p].astype(F32).T, hcol[2 * p + 1].astype(F32).T], axis=1)
        project(wqet, norm_t(wt), n, qv, kt, g, p)
        return _

    pieces = 8
    pc = rows // pieces

    def d_copy(q, k, t, owner, first_col):
        return remote(dsend.at[pl.ds(q * pc, pc), pl.ds(pl.multiple_of(t * rows, rows), rows)],
                      drecv.at[pl.ds(first_col + q * pc, pc)], d_s.at[q, k], d_r.at[q, owner], t)

    my_cols = pl.multiple_of((2 * (1 - x) + core) * rows, rows)

    def segment(i, _):
        @pl.when(i % 2 + 8 * (i // pieces) == 0)
        def _wait():
            for gi in range(len(groups)):
                for k in range(2):
                    h_copy(gi, i // 2, k, peers[k], peers[k]).wait_recv()
        end_step(2 * i, 0)
        end_step(2 * i + 1, 0)

        @pl.when(i >= 2)
        def _send():
            for k, t in enumerate(peers):
                d_copy(i - 2, k, t, sp, my_cols).start()
        return _
    lax.fori_loop(0, pieces + 2, segment, 0)
    drecv[pl.ds(my_cols, rows)] = dsend[:, pl.ds(mine, rows)]

    def final_block(side, owner_core, first_col, ch):
        j0 = pl.multiple_of(first_col + ch * cols, 8)
        jj = owner_core * rows + ch * cols
        for gi in range(rows // 16):
            blk = jnp.swapaxes(drecv[pl.ds(j0, 8), gi * 16:(gi + 1) * 16].astype(F32), 0, 1)
            for q in range(2):
                for i in range(2):
                    b0 = side * npair + 4 * (2 * gi + q)
                    part = z1[b0:b0 + 4, pl.ds(pl.multiple_of(i * half + jj, 8), 8)]
                    r0 = 8 * (2 * gi + q) + 4 * i
                    y[r0:r0 + 4, pl.ds(j0, 8)] = part + blk[8 * q + 4 * i:8 * q + 4 * i + 4]

    for ch in range(chunks):
        final_block(1, core, my_cols, ch)
    for ch in range(chunks):
        for k in (2, 0, 1):
            t = peers[k]
            first_col = pl.multiple_of((2 * x + t % 2 if k < 2 else 2 * (1 - x) + t % 2) * rows, rows)
            for q in range(ch * pieces // chunks, (ch + 1) * pieces // chunks):
                d_copy(q, k, t, t, first_col).wait_recv()
            final_block(0 if k < 2 else 1, t % 2, first_col, ch)
    for k, t in enumerate(peers):
        bias_copy(k, t, sp).wait_send()
        end_bias_copy(k, t, sp).wait_send()
        for ch in range(chunks):
            for gi in range(len(groups)):
                if k < 2:
                    h_copy(gi, ch, k, t, sp).wait_send()
        for q in range(pieces):
            d_copy(q, k, t, sp, my_cols).wait_send()
    for gi in range(2):
        near_copy(gi, sp).wait_send()


def solution(mesh):
    row_spec = P(('dp', 'sp'), None, None)
    sp = mesh.shape['sp']

    def local_fn(pair_loc, wqs, wbs, wos, wqe, wbe, woe, w1, w2):
        rows, n, c = pair_loc.shape
        heads = wbs.shape[0]
        dma = pltpu.SemaphoreType.DMA
        vm = pltpu.VMEM
        weights = (wqs, wbs, wos, wqe, wbe, woe, w1, w2)
        npair = rows // 2
        args = (pair_loc.reshape(rows // 8, 2, 4, n, c),) + weights
        return pl.pallas_call(
            kernel,
            out_shape=vm(pair_loc.shape, F32),
            in_specs=[pl.BlockSpec(memory_space=pltpu.HBM)] * 9,
            out_specs=pl.BlockSpec(memory_space=vm),
            scratch_shapes=[
                vm((rows, n, c), F32), vm((rows, n, c), F32), vm((rows, c, n), BF), vm((rows, c, n), BF),
                vm((npair, 2, c, n), BF), vm((npair, 2, n, c), BF), vm((rows, c, n), F32), vm((rows, c, n), BF),
                vm((heads, rows, n), BF), vm((heads, n, n), BF), vm((2, n, heads * n), F32), vm((2, n // 2, rows, c), BF),
                vm((rows, n, c), BF), vm((npair, 2 * c, 2 * n), BF), vm((rows, n, c), BF), vm((npair, c, 2 * n), F32),
                vm((npair, c, 2 * n), BF), vm((heads, rows, n), BF), vm((heads, n, n), BF), vm((n, heads * n), F32),
                vm((rows, n, c), BF), vm((n, rows, c), BF), vm((2, n, heads * n), F32),
                vm((2, c, 2 * n), F32), vm((2, c, 2 * n), BF), vm((c, 2 * n), BF), vm((2, c, n), BF),
                *[vm(w.shape, BF) for w in weights],
                vm(wqs.shape[::-1], BF), vm(wqe.shape[::-1], BF), vm(woe.shape[::-1], BF),
                vm(w1.shape[::-1], BF), vm(w2.shape[::-1], BF),
                vm((heads * 8, 8 * c), BF), vm((heads * 8, 8 * c), BF),
                dma((8, 2)), dma((8,)), dma((3,)), dma((sp,)), dma((3, 4, 3)), dma((3, 4, sp)), dma((2,)), dma((2,)),
                dma((3,)), dma((sp,)), dma((8, 3)), dma((8, sp)),
            ],
            compiler_params=pltpu.CompilerParams(collective_id=0, has_side_effects=True, vmem_limit_bytes=36 * 2 ** 20),
            name="pair_block",
        )(*[pltpu.with_memory_space_constraint(a, pltpu.HBM) for a in args])

    return jax.shard_map(local_fn, mesh=mesh, in_specs=(row_spec,) + (P(),) * 8, out_specs=row_spec, check_vma=False)
```

```python
import functools

import jax
import jax.numpy as jnp
from jax import lax
from jax.experimental import pallas as pl
from jax.experimental.pallas import tpu as pltpu
from jax.sharding import PartitionSpec as P

MESH = pl.DeviceIdType.MESH
EPS = 1e-5
LOG2E = 1.4426950408889634
BF = jnp.bfloat16
F32 = jnp.float32


def dot(a, b):
    return jnp.dot(a, b, preferred_element_type=F32)


def dot_tn(a, b):
    return lax.dot_general(a, b, (((0,), (0,)), ((), ())), preferred_element_type=F32)


def norm_t(xt):
    mean = jnp.sum(xt, axis=0, keepdims=True) * (1.0 / xt.shape[0])
    cen = xt - mean
    var = jnp.sum(cen * cen, axis=0, keepdims=True) * (1.0 / xt.shape[0])
    return (cen * lax.rsqrt(var + EPS)).astype(BF)


def sigmoid(x):
    return 0.5 * jnp.tanh(0.5 * x) + 0.5


def block_diag(qt, pair, heads):
    hd, n = qt.shape
    d = hd // heads
    cols = []
    for h in (2 * pair, 2 * pair + 1):
        parts = []
        if h:
            parts.append(jnp.zeros((h * d, n), BF))
        parts.append(qt[h * d:(h + 1) * d])
        if h < heads - 1:
            parts.append(jnp.zeros(((heads - 1 - h) * d, n), BF))
        cols.append(jnp.concatenate(parts, axis=0))
    return jnp.concatenate(cols, axis=1)


def stage_scores(kn, qv, s, p, heads):
    c, n = kn.shape[1:]
    for r in range(2):
        keys = kn[2 * p + r]
        qt = qv[p, :c, r * n:(r + 1) * n]
        for pair in range(heads // 2):
            s[r, :, 2 * pair * n:(2 * pair + 2) * n] = dot(keys, block_diag(qt, pair, heads))


def stage_mix(s, biast, qv, g, og, p, heads):
    n = s.shape[1]
    c = qv.shape[1] // 2
    d = c // heads
    scale = LOG2E * d ** -0.5
    for r in range(2):
        for pair in range(heads // 2):
            probs = []
            for h in (2 * pair, 2 * pair + 1):
                t = s[r, :, h * n:(h + 1) * n] * scale + biast[:, h * n:(h + 1) * n]
                e = jnp.exp2(t - jnp.max(t, axis=0, keepdims=True))
                probs.append((e * (1.0 / jnp.sum(e, axis=0, keepdims=True))).astype(BF))
            rows = slice(c + 2 * pair * d, c + (2 * pair + 2) * d)
            o = dot(qv[p, rows, r * n:(r + 1) * n], jnp.concatenate(probs, axis=1))
            for i in range(2):
                h = 2 * pair + i
                out = o[i * d:(i + 1) * d, i * n:(i + 1) * n] * g[p, h * d:(h + 1) * d, r * n:(r + 1) * n]
                og[p, h * d:(h + 1) * d, r * n:(r + 1) * n] = out.astype(BF)


def norm_blocks(src, ut, b0, count):
    for r in range(count):
        ut[b0 + r] = norm_t(src[b0 + r])


def head_rows(wb):
    heads, c = wb.shape
    rep = jnp.broadcast_to(wb.astype(F32)[:, None, :], (heads, 16, c)).reshape(heads * 16, c)
    row = lax.broadcasted_iota(jnp.int32, rep.shape, 0) % 16 // 2
    return jnp.concatenate([jnp.where(row == j, rep, 0.0) for j in range(8)], axis=1).astype(BF)


def bias_rows(w8, ub, dst, i, swap=None):
    heads, rows, n = dst.shape
    c = ub.shape[1]
    half = n // 2
    r0, r1 = [dot(w8, ub[s * rows // 2 + 8 * i:s * rows // 2 + 8 * i + 8].reshape(8 * c, n)) for s in range(2)]
    first, second = [(r0[:, lane:lane + half], r1[:, lane:lane + half]) for lane in (0, half)]
    even = lax.broadcasted_iota(jnp.int32, r0.shape, 0) % 2 == 0
    res = jnp.where(even, jnp.concatenate(first, axis=1), jnp.concatenate(second, axis=1))
    if swap is not None:
        res = jnp.where(swap, jnp.concatenate([res[:, half:], res[:, :half]], axis=1), res)
    dst[:, 16 * i:16 * i + 16] = res.reshape(heads, 16, n).astype(BF)


def low_half(shape):
    return lax.broadcasted_iota(jnp.int32, shape, 1) < shape[1] // 2


def pair_project(wt, ub, qb, kt_ref, vst, g, p, npair, heads):
    own, oth = ub[p], ub[npair + p]
    c, n = own.shape
    d, half = c // heads, n // 2
    u = jnp.concatenate([own, oth], axis=1)
    q = dot(wt[0:c], u).astype(BF)
    qb[p] = q[:, :n]
    qb[npair + p] = q[:, n:]
    u_row = jnp.concatenate([own[:, :half], oth[:, :half], own[:, half:], oth[:, half:]], axis=1)
    k = dot(wt[c:2 * c], u_row).astype(BF)
    v = dot(wt[2 * c:3 * c], u_row).astype(BF)
    for h in range(heads):
        for i in range(2):
            rows = pl.ds((h % 2) * 2 * d + i * d, d)
            kt_ref[h // 2, rows] = k[h * d:(h + 1) * d, i * n:(i + 1) * n]
            vst[p, h // 2, rows] = v[h * d:(h + 1) * d, i * n:(i + 1) * n]
    gate = sigmoid(dot(wt[3 * c:], u))
    g[p] = gate[:, :n]
    g[npair + p] = gate[:, n:]


def block_scores(kn, qb, s, slot, b, p, heads):
    c, n = qb.shape[1:]
    d = c // heads
    low = low_half((d, n))
    zero = jnp.zeros((d, n), BF)
    for pair in range(heads // 2):
        rows = []
        for i in range(2):
            q = qb[b, (2 * pair + i) * d:(2 * pair + i + 1) * d]
            for part in (jnp.where(low, q, zero), jnp.where(low, zero, q)):
                rows.append(jnp.concatenate([part, zero] if i == 0 else [zero, part], axis=1))
        s[slot, :, 2 * pair * n:(2 * pair + 2) * n] = dot(kn[p, pair], jnp.concatenate(rows, axis=0))


def softmax_t(t):
    e = jnp.exp2(t - jnp.max(t, axis=0, keepdims=True))
    return (e * (1.0 / jnp.sum(e, axis=0, keepdims=True))).astype(BF)


def block_mix(s, slot, biast, side, vst, g, og, b, p, heads):
    c, n = og.shape[1:]
    d = c // heads
    low = low_half((d, n))
    for h in range(heads):
        t = s[slot, :, h * n:(h + 1) * n] * (LOG2E * d ** -0.5) + biast[side, :, h * n:(h + 1) * n]
        o = dot(vst[p, h // 2, (h % 2) * 2 * d:(h % 2 + 1) * 2 * d], softmax_t(t))
        og[b, h * d:(h + 1) * d] = (jnp.where(low, o[:d], o[d:]) * g[b, h * d:(h + 1) * d]).astype(BF)


def project(wt, u, n, qv_ref, kt_ref, g_ref, p):
    c = u.shape[0]
    qv_ref[p, :c] = dot(wt[0:c], u).astype(BF)
    kt_ref[...] = dot(wt[c:2 * c], u).astype(BF)
    qv_ref[p, c:] = dot(wt[2 * c:3 * c], u).astype(BF)
    g_ref[p] = sigmoid(dot(wt[3 * c:], u))


def turn_keys(kt_ref, kn_ref, p):
    n = kn_ref.shape[1]
    kn_ref[2 * p] = kt_ref[:, :n].T
    kn_ref[2 * p + 1] = kt_ref[:, n:].T


def kernel(z_hbm, wqs_h, wbs_h, wos_h, wqe_h, wbe_h, woe_h, w1_h, w2_h, y,
           zs4, z1, ub, qb, vst, knp, gb, ogb, bsend, ball, biasp, hsend,
           hcol, qv, kn, g, og, besend, beall, biast, dsend, drecv, s, eb, u2, kt, ktp,
           wqs, wbs, wos, wqe, wbe, woe, w1, w2, wqst, wqet, woet, w1t, w2t, wbs8, wbe8,
           zsem, wsem, bs_s, bs_r, h_s, h_r, o_s, o_r, be_s, be_r, d_s, d_r):
    rows, n, c = y.shape
    npair = rows // 2
    half = n // 2
    heads = wbs.shape[0]
    dp, sp = lax.axis_index("dp"), lax.axis_index("sp")
    x, core = sp // 2, sp % 2
    peers = [2 * (1 - x) + core, 2 * (1 - x) + 1 - core, 2 * x + 1 - core]
    mine = pl.multiple_of(sp * rows, rows)

    def zcopy(ci):
        q, side = ci // 2, ci % 2
        return pltpu.make_async_copy(z_hbm.at[pl.ds(4 * q, 4), :, (x + side) % 2],
                                     zs4.at[pl.ds(side * npair + 4 * q, 4)], zsem.at[ci])

    def wcopy(i):
        src = (wbs_h, wqs_h, wqe_h, woe_h, w1_h, w2_h, wbe_h, wos_h)[i]
        return pltpu.make_async_copy(src, (wbs, wqs, wqe, woe, w1, w2, wbe, wos)[i], wsem.at[i])

    wcopy(0).start()
    wcopy(6).start()
    for ci in range(8):
        zcopy(ci).start()
    for i in (1, 7, 2, 3, 4, 5):
        wcopy(i).start()
    bar = pltpu.get_barrier_semaphore()
    for t in peers:
        pl.semaphore_signal(bar, inc=1, device_id=(dp, t), device_id_type=MESH)

    def remote(src, dst, ssem, rsem, t):
        return pltpu.make_async_remote_copy(src, dst, ssem, rsem, device_id=(dp, t), device_id_type=MESH)

    wcopy(0).wait()
    wcopy(6).wait()
    wbs8[...] = head_rows(wbs[...])
    wbe8[...] = head_rows(wbe[...])

    def chunk_base(ci):
        return ci % 2 * npair + ci // 2 * 4

    def ln_step(ci, _):
        for side in range(2):
            zcopy(2 * ci + side).wait()
        for side in range(2):
            norm_blocks(y, ub, chunk_base(jnp.maximum(2 * ci - 2, 0) + side), 4)
        for side in range(2):
            b0 = chunk_base(2 * ci + side)
            for r in range(4):
                y[b0 + r] = zs4[b0 + r].reshape(n, c).T
        return _
    lax.fori_loop(0, 4, ln_step, 0)
    bias_rows(wbs8[...], ub, bsend, 0)
    for side in range(2):
        norm_blocks(y, ub, chunk_base(6 + side), 4)
    for i in range(1, rows // 16):
        bias_rows(wbs8[...], ub, bsend, i)
    ball[:, pl.ds(pl.multiple_of(core * rows, rows), rows)] = bsend[...]
    pl.semaphore_wait(bar, 3)

    def bias_copy(k, t, owner):
        return remote(bsend, ball.at[:, pl.ds(pl.multiple_of((half if k < 2 else 0) + owner % 2 * rows, rows), rows)],
                      bs_s, bs_r.at[k // 2], t)

    def end_bias_copy(i, t):
        return remote(besend.at[:, 16 * i:16 * i + 16], beall.at[:, pl.ds(pl.multiple_of(mine + 16 * i, 16), 16)], be_s, be_r, t)

    def sent(ref, sem):
        remote(ref, ref, sem, sem, peers[0]).wait_send()

    def arrived(ref, sem):
        remote(ref, ref, sem, sem, peers[0]).wait_recv()

    for k in (2, 0, 1):
        bias_copy(k, peers[k], sp).start()

    wcopy(1).wait()
    wcopy(7).wait()
    wqst[...] = wqs[...].T
    def start_project(*pairs):
        for p in pairs:
            pair_project(wqst, ub, qb, ktp.at[p % 2], vst, gb, p, npair, heads)
        for p in pairs:
            for pair in range(heads // 2):
                knp[p, pair] = ktp[p % 2, pair].T

    def start_bias(side):
        for h in range(heads):
            rws = ball[h, side * half:(side + 1) * half].astype(F32)
            tr = jnp.concatenate([rws, rws], axis=0).T * LOG2E
            if side:
                tr = jnp.concatenate([tr[half:], tr[:half]], axis=0)
            biasp[side, :, h * n:(h + 1) * n] = tr

    def start_out(b):
        upd = dot_tn(jnp.concatenate([ogb[b], ogb[b + 1]], axis=1), wos[...])
        z1[b] = zs4[b].reshape(n, c) + upd[:n]
        z1[b + 1] = zs4[b + 1].reshape(n, c) + upd[n:]
    def start_norm(b):
        for r in range(2):
            ub[b + r] = norm_t(z1[b + r].astype(BF).astype(F32).T)

    def start_mix(b):
        for r in range(2):
            block_mix(s, r, biasp, b // npair, vst, gb, ogb, b + r, b % npair + r, heads)

    def start_scores(b):
        for r in range(2):
            block_scores(knp, qb, s, r, b + r, b % npair + r, heads)

    def start_step(t, _):
        for by, stage in ((3, start_norm), (2, start_out), (1, start_mix), (0, start_scores)):
            if not isinstance(t, int) or 0 <= t - by < npair:
                stage(2 * (t - by))
        return _

    chunks = 4
    cols = rows // chunks
    groups = [(0, 8), (8, 8), (16, 16)]
    near = [(0, 16), (16, 16)]

    def h_copy(gi, ch, k, t, owner):
        r0, size = groups[gi]
        return remote(hsend.at[0, pl.ds(t % 2 * rows + ch * cols, cols), r0:r0 + size],
                      hcol.at[pl.ds(ch * cols, cols), pl.ds(pl.multiple_of(owner * rows + r0, 8), size)],
                      h_s, h_r.at[ch], t)

    def near_copy(gi, owner):
        r0, size = near[gi]
        return remote(hsend.at[1, pl.ds(pl.multiple_of((1 - core) * rows, rows), rows), r0:r0 + size],
                      hcol.at[:, pl.ds(pl.multiple_of(owner * rows + r0, 8), size)],
                      o_s, o_r, peers[2])

    def shuffle_rows(side, r0, size):
        def body(jb, _):
            j0 = pl.multiple_of(jb * 8, 8)
            parts = []
            for row in range(r0, r0 + size):
                b = side * npair + row // 2
                parts.append(z1[b:b + 1, pl.ds(row % 2 * half + j0, 8)])
            blk = jnp.swapaxes(jnp.concatenate(parts, axis=0), 0, 1)
            hsend[side, pl.ds(j0, 8), r0:r0 + size] = blk.astype(BF)
            return _
        lax.fori_loop(0, half // 8, body, 0)

    def send_h(gi, chs):
        for ch in chs:
            for k in range(2):
                h_copy(gi, ch, k, peers[k], sp).start()

    start_project(0, 1)
    start_project(2, 3)
    arrived(ball.at[:, 0:rows], bs_r.at[1])
    start_bias(0)
    start_scores(0)
    start_mix(0)
    start_scores(2)
    start_out(0)
    start_mix(2)
    start_out(2)
    shuffle_rows(0, 0, 8)
    send_h(0, range(chunks))
    start_project(4, 5)
    start_scores(4)
    start_project(6, 7)
    start_norm(0)
    start_mix(4)
    start_scores(6)
    start_project(8, 9)
    start_norm(2)
    start_out(4)
    start_mix(6)
    start_scores(8)
    start_project(10, 11)
    start_step(5, 0)
    shuffle_rows(0, 8, 8)
    send_h(1, range(chunks))
    arrived(ball.at[:, 0:2 * rows], bs_r.at[0])
    start_bias(1)
    for t in (6, 7):
        start_project(2 * t, 2 * t + 1)
        start_step(t, 0)
    for t in (8, 9):
        start_step(t, 0)
    shuffle_rows(0, 16, 16)
    send_h(2, [0])
    h_copy(2, 1, 0, peers[0], sp).start()
    lax.fori_loop(10, 14, start_step, 0, unroll=4)
    shuffle_rows(1, 0, 16)
    near_copy(0, sp).start()
    start_step(14, 0)
    bias_rows(wbe8[...], ub, besend, 0, x == 1)
    for k in range(3):
        end_bias_copy(0, peers[k]).start()
    for t in range(15, npair + 3):
        start_step(t, 0)
    bias_rows(wbe8[...], ub, besend, 1, x == 1)
    for k in range(3):
        end_bias_copy(1, peers[k]).start()
    h_copy(2, 1, 1, peers[1], sp).start()
    beall[:, pl.ds(mine, rows)] = besend[...]
    shuffle_rows(1, 16, 16)
    near_copy(1, sp).start()
    hcol[:, pl.ds(mine, rows)] = hsend[1, pl.ds(pl.multiple_of(core * rows, rows), rows)]
    for i in range(2, 6):
        wcopy(i).wait()
    wqet[...] = wqe[...].T
    woet[...] = woe[...].T
    w1t[...] = w1[...].T
    w2t[...] = w2[...].T
    sent(ball.at[:, 0:3 * rows], bs_s)

    def end_delta(p):
        hid = jnp.maximum(dot(w1t[...], u2[p % 2]), 0.0).astype(BF)
        delta = (eb[p % 2] + dot(w2t[...], hid)).astype(BF)
        dsend[2 * p] = delta[:, :n].T
        dsend[2 * p + 1] = delta[:, n:].T

    def columns(p):
        return jnp.concatenate([hcol[2 * p].astype(F32).T, hcol[2 * p + 1].astype(F32).T], axis=1)

    def end_out(p):
        e = dot(woet[...], og[p])
        eb[p % 2] = e
        u2[p % 2] = norm_t(columns(p) + e)

    def end_mix(p):
        stage_mix(s, biast, qv, g, og, p, heads)

    def end_scores(p):
        turn_keys(kt, kn, p)
        stage_scores(kn, qv, s, p, heads)

    def end_project(p):
        project(wqet, norm_t(columns(p)), n, qv, kt, g, p)

    def end_step(t):
        for by, stage in ((4, end_delta), (3, end_out), (2, end_mix), (1, end_scores), (0, end_project)):
            if not isinstance(t, int) or 0 <= t - by < npair:
                stage(t - by)

    def d_copy(q, count, t, first_col):
        return remote(dsend.at[pl.ds(2 * q, 2 * count), pl.ds(pl.multiple_of(t * rows, rows), rows)],
                      drecv.at[pl.ds(first_col + 2 * q, 2 * count)], d_s, d_r.at[q // (npair // chunks)], t)

    my_cols = pl.multiple_of((2 * (1 - x) + core) * rows, rows)

    def send_d(q, count):
        for t in peers:
            d_copy(q, count, t, my_cols).start()

    def wait_h(ch):
        arrived(hcol.at[pl.ds(ch * cols, cols), 0:2 * rows], h_r.at[ch])

    sent(ball.at[:, 0:3 * rows], be_s)
    send_h(2, [2])
    arrived(hcol.at[:, 0:rows], o_r)
    wait_h(0)
    end_step(0)
    end_step(1)
    send_h(2, [3])
    arrived(beall.at[:, 0:3 * rows], be_r)
    for h in range(heads):
        biast[:, h * n:(h + 1) * n] = beall[h].astype(F32) * LOG2E
    end_step(2)
    end_step(3)

    def segment(i, _):
        @pl.when(i % 2 == 0)
        def _wait():
            wait_h(i // 2)
        end_step(2 * i)
        send_d(2 * i - 4, 1)
        end_step(2 * i + 1)
        send_d(2 * i - 3, 1)
        return _
    lax.fori_loop(2, npair // 2, segment, 0)
    for t in range(npair, npair + 4):
        end_step(t)
        send_d(t - 4, 1)
    drecv[pl.ds(my_cols, rows)] = dsend[:, pl.ds(mine, rows)]

    def final_block(side, owner_core, first_col, ch):
        j0 = pl.multiple_of(first_col + ch * cols, 8)
        jj = owner_core * rows + ch * cols
        for gi in range(rows // 16):
            blk = jnp.swapaxes(drecv[pl.ds(j0, 8), gi * 16:(gi + 1) * 16].astype(F32), 0, 1)
            for r in range(16):
                row = 16 * gi + r
                part = z1[side * npair + row // 2, pl.ds(pl.multiple_of(row % 2 * half + jj, 8), 8)]
                y[row, pl.ds(j0, 8)] = part + blk[r]

    for ch in range(chunks):
        final_block(1, core, my_cols, ch)
    for ch in range(chunks):
        arrived(drecv.at[0:3 * cols], d_r.at[ch])
        for k in (2, 0, 1):
            t = peers[k]
            first_col = pl.multiple_of((2 * x + t % 2 if k < 2 else 2 * (1 - x) + t % 2) * rows, rows)
            final_block(0 if k < 2 else 1, t % 2, first_col, ch)
    sent(hsend.at[0], h_s)
    sent(hcol.at[:, 0:rows], o_s)
    sent(dsend.at[:, 0:3 * rows], d_s)


def solution(mesh):
    row_spec = P(('dp', 'sp'), None, None)
    sp = mesh.shape['sp']

    def local_fn(pair_loc, wqs, wbs, wos, wqe, wbe, woe, w1, w2):
        rows, n, c = pair_loc.shape
        heads = wbs.shape[0]
        dma = pltpu.SemaphoreType.DMA
        vm = pltpu.VMEM
        weights = (wqs, wbs, wos, wqe, wbe, woe, w1, w2)
        npair = rows // 2
        args = (pair_loc.reshape(npair, 2, 2, n // 2, c),) + weights
        return pl.pallas_call(
            kernel,
            out_shape=vm(pair_loc.shape, F32),
            in_specs=[pl.BlockSpec(memory_space=pltpu.HBM)] * 9,
            out_specs=pl.BlockSpec(memory_space=vm),
            scratch_shapes=[
                vm((rows, 2, n // 2, c), F32), vm((rows, n, c), F32), vm((rows, c, n), BF), vm((rows, c, n), BF),
                vm((npair, 2, c, n), BF), vm((npair, 2, n, c), BF), vm((rows, c, n), F32), vm((rows, c, n), BF),
                vm((heads, rows, n), BF), vm((heads, n, n), BF), vm((2, n, heads * n), F32), vm((2, n // 2, rows, c), BF),
                vm((rows, n, c), BF), vm((npair, 2 * c, 2 * n), BF), vm((rows, n, c), BF), vm((npair, c, 2 * n), F32),
                vm((npair, c, 2 * n), BF), vm((heads, rows, n), BF), vm((heads, n, n), BF), vm((n, heads * n), F32),
                vm((rows, n, c), BF), vm((n, rows, c), BF), vm((2, n, heads * n), F32),
                vm((2, c, 2 * n), F32), vm((2, c, 2 * n), BF), vm((c, 2 * n), BF), vm((2, 2, c, n), BF),
                *[vm(w.shape, BF) for w in weights],
                vm(wqs.shape[::-1], BF), vm(wqe.shape[::-1], BF), vm(woe.shape[::-1], BF),
                vm(w1.shape[::-1], BF), vm(w2.shape[::-1], BF),
                vm((heads * 16, 8 * c), BF), vm((heads * 16, 8 * c), BF),
                dma((8,)), dma((8,)), dma, dma((2,)), dma, dma((4,)), dma, dma, dma, dma, dma, dma((4,)),
            ],
            compiler_params=pltpu.CompilerParams(collective_id=0, has_side_effects=True, vmem_limit_bytes=36 * 2 ** 20),
            name="pair_block",
        )(*[pltpu.with_memory_space_constraint(a, pltpu.HBM) for a in args])

    return jax.shard_map(local_fn, mesh=mesh, in_specs=(row_spec,) + (P(),) * 8, out_specs=row_spec, check_vma=False)
```

```python
import functools

import jax
import jax.numpy as jnp
from jax import lax
from jax.experimental import pallas as pl
from jax.experimental.pallas import tpu as pltpu
from jax.sharding import PartitionSpec as P

MESH = pl.DeviceIdType.MESH
EPS = 1e-5
LOG2E = 1.4426950408889634
BF = jnp.bfloat16
F32 = jnp.float32


def dot(a, b):
    return jnp.dot(a, b, preferred_element_type=F32)


def dot_tn(a, b):
    return lax.dot_general(a, b, (((0,), (0,)), ((), ())), preferred_element_type=F32)


def norm_t(xt):
    mean = jnp.sum(xt, axis=0, keepdims=True) * (1.0 / xt.shape[0])
    cen = xt - mean
    var = jnp.sum(cen * cen, axis=0, keepdims=True) * (1.0 / xt.shape[0])
    return (cen * lax.rsqrt(var + EPS)).astype(BF)


def sigmoid(x):
    return 0.5 * jnp.tanh(0.5 * x) + 0.5


def block_diag(qt, pair, heads):
    hd, n = qt.shape
    d = hd // heads
    cols = []
    for h in (2 * pair, 2 * pair + 1):
        parts = []
        if h:
            parts.append(jnp.zeros((h * d, n), BF))
        parts.append(qt[h * d:(h + 1) * d])
        if h < heads - 1:
            parts.append(jnp.zeros(((heads - 1 - h) * d, n), BF))
        cols.append(jnp.concatenate(parts, axis=0))
    return jnp.concatenate(cols, axis=1)


def stage_scores(kn, qv, s, p, heads):
    c, n = kn.shape[1:]
    for r in range(2):
        keys = kn[2 * p + r]
        qt = qv[p, :c, r * n:(r + 1) * n]
        for pair in range(heads // 2):
            s[r, :, 2 * pair * n:(2 * pair + 2) * n] = dot(keys, block_diag(qt, pair, heads))


def stage_mix(s, biast, qv, g, og, p, heads):
    n = s.shape[1]
    c = qv.shape[1] // 2
    d = c // heads
    scale = LOG2E * d ** -0.5
    for r in range(2):
        for pair in range(heads // 2):
            probs = []
            for h in (2 * pair, 2 * pair + 1):
                t = s[r, :, h * n:(h + 1) * n] * scale + biast[:, h * n:(h + 1) * n]
                e = jnp.exp2(t - jnp.max(t, axis=0, keepdims=True))
                probs.append((e * (1.0 / jnp.sum(e, axis=0, keepdims=True))).astype(BF))
            rows = slice(c + 2 * pair * d, c + (2 * pair + 2) * d)
            o = dot(qv[p, rows, r * n:(r + 1) * n], jnp.concatenate(probs, axis=1))
            for i in range(2):
                h = 2 * pair + i
                out = o[i * d:(i + 1) * d, i * n:(i + 1) * n] * g[p, h * d:(h + 1) * d, r * n:(r + 1) * n]
                og[p, h * d:(h + 1) * d, r * n:(r + 1) * n] = out.astype(BF)


def norm_blocks(src, ut, b0, count):
    for r in range(count):
        ut[b0 + r] = norm_t(src[b0 + r])


def head_rows(wb):
    heads, c = wb.shape
    rep = jnp.broadcast_to(wb.astype(F32)[:, None, :], (heads, 16, c)).reshape(heads * 16, c)
    row = lax.broadcasted_iota(jnp.int32, rep.shape, 0) % 16 // 2
    return jnp.concatenate([jnp.where(row == j, rep, 0.0) for j in range(8)], axis=1).astype(BF)


def bias_rows(w8, ub, dst, i, swap=None):
    heads, rows, n = dst.shape
    c = ub.shape[1]
    half = n // 2
    r0, r1 = [dot(w8, ub[s * rows // 2 + 8 * i:s * rows // 2 + 8 * i + 8].reshape(8 * c, n)) for s in range(2)]
    first, second = [(r0[:, lane:lane + half], r1[:, lane:lane + half]) for lane in (0, half)]
    even = lax.broadcasted_iota(jnp.int32, r0.shape, 0) % 2 == 0
    res = jnp.where(even, jnp.concatenate(first, axis=1), jnp.concatenate(second, axis=1))
    if swap is not None:
        res = jnp.where(swap, jnp.concatenate([res[:, half:], res[:, :half]], axis=1), res)
    dst[:, 16 * i:16 * i + 16] = res.reshape(heads, 16, n).astype(BF)


def low_half(shape):
    return lax.broadcasted_iota(jnp.int32, shape, 1) < shape[1] // 2


def pair_project(wt, ub, qb, kt_ref, vst, g, p, npair, heads):
    own, oth = ub[p], ub[npair + p]
    c, n = own.shape
    d, half = c // heads, n // 2
    u = jnp.concatenate([own, oth], axis=1)
    q = dot(wt[0:c], u).astype(BF)
    qb[p] = q[:, :n]
    qb[npair + p] = q[:, n:]
    u_row = jnp.concatenate([own[:, :half], oth[:, :half], own[:, half:], oth[:, half:]], axis=1)
    k = dot(wt[c:2 * c], u_row).astype(BF)
    v = dot(wt[2 * c:3 * c], u_row).astype(BF)
    for h in range(heads):
        for i in range(2):
            rows = pl.ds((h % 2) * 2 * d + i * d, d)
            kt_ref[h // 2, rows] = k[h * d:(h + 1) * d, i * n:(i + 1) * n]
            vst[p, h // 2, rows] = v[h * d:(h + 1) * d, i * n:(i + 1) * n]
    gate = sigmoid(dot(wt[3 * c:], u))
    g[p] = gate[:, :n]
    g[npair + p] = gate[:, n:]


def block_scores(kn, qb, s, slot, b, p, heads):
    c, n = qb.shape[1:]
    d = c // heads
    low = low_half((d, n))
    zero = jnp.zeros((d, n), BF)
    for pair in range(heads // 2):
        rows = []
        for i in range(2):
            q = qb[b, (2 * pair + i) * d:(2 * pair + i + 1) * d]
            for part in (jnp.where(low, q, zero), jnp.where(low, zero, q)):
                rows.append(jnp.concatenate([part, zero] if i == 0 else [zero, part], axis=1))
        s[slot, :, 2 * pair * n:(2 * pair + 2) * n] = dot(kn[p, pair], jnp.concatenate(rows, axis=0))


def softmax_t(t):
    e = jnp.exp2(t - jnp.max(t, axis=0, keepdims=True))
    return (e * (1.0 / jnp.sum(e, axis=0, keepdims=True))).astype(BF)


def block_mix(s, slot, biast, side, vst, g, og, b, p, heads):
    c, n = og.shape[1:]
    d = c // heads
    low = low_half((d, n))
    for h in range(heads):
        t = s[slot, :, h * n:(h + 1) * n] * (LOG2E * d ** -0.5) + biast[side, :, h * n:(h + 1) * n]
        o = dot(vst[p, h // 2, (h % 2) * 2 * d:(h % 2 + 1) * 2 * d], softmax_t(t))
        og[b, h * d:(h + 1) * d] = (jnp.where(low, o[:d], o[d:]) * g[b, h * d:(h + 1) * d]).astype(BF)


def project(wt, u, n, qv_ref, kt_ref, g_ref, p):
    c = u.shape[0]
    qv_ref[p, :c] = dot(wt[0:c], u).astype(BF)
    kt_ref[...] = dot(wt[c:2 * c], u).astype(BF)
    qv_ref[p, c:] = dot(wt[2 * c:3 * c], u).astype(BF)
    g_ref[p] = sigmoid(dot(wt[3 * c:], u))


def turn_keys(kt_ref, kn_ref, p):
    n = kn_ref.shape[1]
    kn_ref[2 * p] = kt_ref[:, :n].T
    kn_ref[2 * p + 1] = kt_ref[:, n:].T


def kernel(z_hbm, wqs_h, wbs_h, wos_h, wqe_h, wbe_h, woe_h, w1_h, w2_h, y,
           zs4, z1, ub, qb, vst, knp, gb, ogb, bsend, ball, biasp, hsend,
           hcol, qv, kn, g, og, besend, beall, biast, dsend, drecv, s, eb, u2, kt, ktp,
           wqs, wbs, wos, wqe, wbe, woe, w1, w2, wqst, wqet, woet, w1t, w2t, wbs8, wbe8,
           zsem, wsem, bs_s, bs_r, h_s, h_r, o_s, o_r, be_s, be_r, d_s, d_r):
    rows, n, c = y.shape
    npair = rows // 2
    half = n // 2
    heads = wbs.shape[0]
    dp, sp = lax.axis_index("dp"), lax.axis_index("sp")
    x, core = sp // 2, sp % 2
    peers = [2 * (1 - x) + core, 2 * (1 - x) + 1 - core, 2 * x + 1 - core]
    mine = pl.multiple_of(sp * rows, rows)

    def zcopy(ci):
        q, side = ci // 2, ci % 2
        return pltpu.make_async_copy(z_hbm.at[pl.ds(4 * q, 4), :, (x + side) % 2],
                                     zs4.at[pl.ds(side * npair + 4 * q, 4)], zsem.at[ci])

    def wcopy(i):
        src = (wbs_h, wqs_h, wqe_h, woe_h, w1_h, w2_h, wbe_h, wos_h)[i]
        return pltpu.make_async_copy(src, (wbs, wqs, wqe, woe, w1, w2, wbe, wos)[i], wsem.at[i])

    wcopy(0).start()
    wcopy(6).start()
    for ci in range(8):
        zcopy(ci).start()
    for i in (1, 7, 2, 3, 4, 5):
        wcopy(i).start()
    bar = pltpu.get_barrier_semaphore()
    for t in peers:
        pl.semaphore_signal(bar, inc=1, device_id=(dp, t), device_id_type=MESH)

    def remote(src, dst, ssem, rsem, t):
        return pltpu.make_async_remote_copy(src, dst, ssem, rsem, device_id=(dp, t), device_id_type=MESH)

    wcopy(0).wait()
    wcopy(6).wait()
    wbs8[...] = head_rows(wbs[...])
    wbe8[...] = head_rows(wbe[...])

    def chunk_base(ci):
        return ci % 2 * npair + ci // 2 * 4

    def ln_step(ci, _):
        for side in range(2):
            zcopy(2 * ci + side).wait()
        for side in range(2):
            norm_blocks(y, ub, chunk_base(jnp.maximum(2 * ci - 2, 0) + side), 4)
        for side in range(2):
            b0 = chunk_base(2 * ci + side)
            for r in range(4):
                y[b0 + r] = zs4[b0 + r].reshape(n, c).T
        return _
    lax.fori_loop(0, 4, ln_step, 0)
    bias_rows(wbs8[...], ub, bsend, 0)
    for side in range(2):
        norm_blocks(y, ub, chunk_base(6 + side), 4)
    for i in range(1, rows // 16):
        bias_rows(wbs8[...], ub, bsend, i)
    ball[:, pl.ds(pl.multiple_of(core * rows, rows), rows)] = bsend[...]
    pl.semaphore_wait(bar, 3)

    def bias_copy(k, t, owner):
        return remote(bsend, ball.at[:, pl.ds(pl.multiple_of((half if k < 2 else 0) + owner % 2 * rows, rows), rows)],
                      bs_s, bs_r.at[k // 2], t)

    def end_bias_part(owner, i):
        return beall.at[:, pl.ds(pl.multiple_of(owner * rows + 16 * i, 16), 16)]

    def end_bias_send(i):
        part = besend.at[:, 16 * i:16 * i + 16]
        for k in ((0, 2), range(3))[i]:
            remote(part, end_bias_part(sp, i), be_s, be_r.at[2 if k == 2 else i], peers[k]).start()

    def end_bias_forward():
        part = end_bias_part(peers[0], 0)
        arrived(part, be_r.at[0])
        remote(part, part, be_s, be_r.at[2], peers[2]).start()

    def sent(ref, sem):
        remote(ref, ref, sem, sem, peers[0]).wait_send()

    def arrived(ref, sem):
        remote(ref, ref, sem, sem, peers[0]).wait_recv()

    for k in (2, 0, 1):
        bias_copy(k, peers[k], sp).start()

    wcopy(1).wait()
    wcopy(7).wait()
    wqst[...] = wqs[...].T
    def start_project(*pairs):
        for p in pairs:
            pair_project(wqst, ub, qb, ktp.at[p % 2], vst, gb, p, npair, heads)
        for p in pairs:
            for pair in range(heads // 2):
                knp[p, pair] = ktp[p % 2, pair].T

    def start_bias(side):
        for h in range(heads):
            rws = ball[h, side * half:(side + 1) * half].astype(F32)
            tr = jnp.concatenate([rws, rws], axis=0).T * LOG2E
            if side:
                tr = jnp.concatenate([tr[half:], tr[:half]], axis=0)
            biasp[side, :, h * n:(h + 1) * n] = tr

    def start_out(b):
        upd = dot_tn(jnp.concatenate([ogb[b], ogb[b + 1]], axis=1), wos[...])
        z1[b] = zs4[b].reshape(n, c) + upd[:n]
        z1[b + 1] = zs4[b + 1].reshape(n, c) + upd[n:]
    def start_norm(b):
        for r in range(2):
            ub[b + r] = norm_t(z1[b + r].astype(BF).astype(F32).T)

    def start_mix(b):
        for r in range(2):
            block_mix(s, r, biasp, b // npair, vst, gb, ogb, b + r, b % npair + r, heads)

    def start_scores(b):
        for r in range(2):
            block_scores(knp, qb, s, r, b + r, b % npair + r, heads)

    def start_step(t, _):
        for by, stage in ((3, start_norm), (2, start_out), (1, start_mix), (0, start_scores)):
            if not isinstance(t, int) or 0 <= t - by < npair:
                stage(2 * (t - by))
        return _

    chunks = 4
    cols = rows // chunks
    groups = [(0, 8), (8, 8), (16, 16)]
    near = [(0, 16), (16, 16)]

    def h_copy(gi, ch, k, t, owner):
        r0, size = groups[gi]
        return remote(hsend.at[0, pl.ds(t % 2 * rows + ch * cols, cols), r0:r0 + size],
                      hcol.at[pl.ds(ch * cols, cols), pl.ds(pl.multiple_of(owner * rows + r0, 8), size)],
                      h_s, h_r.at[ch], t)

    def near_copy(gi, owner):
        r0, size = near[gi]
        return remote(hsend.at[1, pl.ds(pl.multiple_of((1 - core) * rows, rows), rows), r0:r0 + size],
                      hcol.at[:, pl.ds(pl.multiple_of(owner * rows + r0, 8), size)],
                      o_s, o_r, peers[2])

    def shuffle_rows(side, r0, size):
        def body(jb, _):
            j0 = pl.multiple_of(jb * 8, 8)
            parts = []
            for row in range(r0, r0 + size):
                b = side * npair + row // 2
                parts.append(z1[b:b + 1, pl.ds(row % 2 * half + j0, 8)])
            blk = jnp.swapaxes(jnp.concatenate(parts, axis=0), 0, 1)
            hsend[side, pl.ds(j0, 8), r0:r0 + size] = blk.astype(BF)
            return _
        lax.fori_loop(0, half // 8, body, 0)

    def send_h(gi, chs):
        for ch in chs:
            for k in range(2):
                h_copy(gi, ch, k, peers[k], sp).start()

    start_project(0, 1)
    start_project(2, 3)
    start_scores(0)
    arrived(ball.at[:, 0:rows], bs_r.at[1])
    start_bias(0)
    start_mix(0)
    start_scores(2)
    start_out(0)
    start_mix(2)
    start_out(2)
    shuffle_rows(0, 0, 8)
    send_h(0, range(chunks))
    start_project(4, 5)
    start_scores(4)
    start_project(6, 7)
    start_norm(0)
    start_mix(4)
    start_scores(6)
    start_project(8, 9)
    start_norm(2)
    start_out(4)
    start_mix(6)
    start_scores(8)
    start_project(10, 11)
    start_step(5, 0)
    shuffle_rows(0, 8, 8)
    send_h(1, range(chunks))
    for t in (6, 7):
        start_project(2 * t, 2 * t + 1)
        start_step(t, 0)
    start_step(8, 0)
    arrived(ball.at[:, 0:2 * rows], bs_r.at[0])
    start_bias(1)
    start_step(9, 0)
    shuffle_rows(0, 16, 16)
    send_h(2, [0])
    lax.fori_loop(10, 14, start_step, 0, unroll=4)
    shuffle_rows(1, 0, 16)
    near_copy(0, sp).start()
    start_step(14, 0)
    bias_rows(wbe8[...], ub, besend, 0, x == 1)
    end_bias_send(0)
    for t in range(15, npair + 3):
        start_step(t, 0)
    bias_rows(wbe8[...], ub, besend, 1, x == 1)
    end_bias_send(1)
    beall[:, pl.ds(mine, rows)] = besend[...]
    shuffle_rows(1, 16, 16)
    near_copy(1, sp).start()
    send_h(2, [1])
    hcol[:, pl.ds(mine, rows)] = hsend[1, pl.ds(pl.multiple_of(core * rows, rows), rows)]
    for i in range(2, 6):
        wcopy(i).wait()
    wqet[...] = wqe[...].T
    woet[...] = woe[...].T
    w1t[...] = w1[...].T
    w2t[...] = w2[...].T
    sent(ball.at[:, 0:3 * rows], bs_s)

    def end_delta(p):
        hid = jnp.maximum(dot(w1t[...], u2[p % 2]), 0.0).astype(BF)
        delta = (eb[p % 2] + dot(w2t[...], hid)).astype(BF)
        dsend[2 * p] = delta[:, :n].T
        dsend[2 * p + 1] = delta[:, n:].T

    def columns(p):
        return jnp.concatenate([hcol[2 * p].astype(F32).T, hcol[2 * p + 1].astype(F32).T], axis=1)

    def end_out(p):
        e = dot(woet[...], og[p])
        eb[p % 2] = e
        u2[p % 2] = norm_t(columns(p) + e)

    def end_mix(p):
        stage_mix(s, biast, qv, g, og, p, heads)

    def end_scores(p):
        turn_keys(kt, kn, p)
        stage_scores(kn, qv, s, p, heads)

    def end_project(p):
        project(wqet, norm_t(columns(p)), n, qv, kt, g, p)

    def end_step(t):
        for by, stage in ((4, end_delta), (3, end_out), (2, end_mix), (1, end_scores), (0, end_project)):
            if not isinstance(t, int) or 0 <= t - by < npair:
                stage(t - by)

    def d_copy(q, count, t, first_col):
        return remote(dsend.at[pl.ds(2 * q, 2 * count), pl.ds(pl.multiple_of(t * rows, rows), rows)],
                      drecv.at[pl.ds(first_col + 2 * q, 2 * count)], d_s, d_r.at[q // (npair // chunks)], t)

    my_cols = pl.multiple_of((2 * (1 - x) + core) * rows, rows)

    def send_d(q, count):
        for t in peers:
            d_copy(q, count, t, my_cols).start()

    def wait_h(ch):
        arrived(hcol.at[pl.ds(ch * cols, cols), 0:2 * rows], h_r.at[ch])

    arrived(hcol.at[:, 0:rows], o_r)
    send_h(2, [2])
    end_bias_forward()
    send_h(2, [3])
    wait_h(0)
    end_step(0)
    end_step(1)
    arrived(beall.at[:, 0:rows], be_r.at[1])
    arrived(beall.at[:, 0:rows + 16], be_r.at[2])
    for h in range(heads):
        biast[:, h * n:(h + 1) * n] = beall[h].astype(F32) * LOG2E
    end_step(2)
    end_step(3)

    def segment(i, _):
        @pl.when(i % 2 == 0)
        def _wait():
            wait_h(i // 2)
        end_step(2 * i)
        end_step(2 * i + 1)
        send_d(2 * i - 4, 2)
        return _
    lax.fori_loop(2, npair // 2, segment, 0)
    for t in range(npair, npair + 4):
        end_step(t)
        send_d(t - 4, 1)
    drecv[pl.ds(my_cols, rows)] = dsend[:, pl.ds(mine, rows)]

    def final_block(side, owner_core, first_col, ch):
        j0 = pl.multiple_of(first_col + ch * cols, 8)
        jj = owner_core * rows + ch * cols
        for gi in range(rows // 16):
            blk = jnp.swapaxes(drecv[pl.ds(j0, 8), gi * 16:(gi + 1) * 16].astype(F32), 0, 1)
            for r in range(16):
                row = 16 * gi + r
                part = z1[side * npair + row // 2, pl.ds(pl.multiple_of(row % 2 * half + jj, 8), 8)]
                y[row, pl.ds(j0, 8)] = part + blk[r]

    for ch in range(chunks):
        final_block(1, core, my_cols, ch)
    for ch in range(chunks):
        arrived(drecv.at[0:3 * cols], d_r.at[ch])
        for k in (2, 0, 1):
            t = peers[k]
            first_col = pl.multiple_of((2 * x + t % 2 if k < 2 else 2 * (1 - x) + t % 2) * rows, rows)
            final_block(0 if k < 2 else 1, t % 2, first_col, ch)
    sent(hsend.at[0], h_s)
    sent(ball.at[:, 0:3 * rows], be_s)
    sent(hcol.at[:, 0:rows], o_s)
    sent(dsend.at[:, 0:3 * rows], d_s)


def solution(mesh):
    row_spec = P(('dp', 'sp'), None, None)
    sp = mesh.shape['sp']

    def local_fn(pair_loc, wqs, wbs, wos, wqe, wbe, woe, w1, w2):
        rows, n, c = pair_loc.shape
        heads = wbs.shape[0]
        dma = pltpu.SemaphoreType.DMA
        vm = pltpu.VMEM
        weights = (wqs, wbs, wos, wqe, wbe, woe, w1, w2)
        npair = rows // 2
        args = (pair_loc.reshape(npair, 2, 2, n // 2, c),) + weights
        return pl.pallas_call(
            kernel,
            out_shape=vm(pair_loc.shape, F32),
            in_specs=[pl.BlockSpec(memory_space=pltpu.HBM)] * 9,
            out_specs=pl.BlockSpec(memory_space=vm),
            scratch_shapes=[
                vm((rows, 2, n // 2, c), F32), vm((rows, n, c), F32), vm((rows, c, n), BF), vm((rows, c, n), BF),
                vm((npair, 2, c, n), BF), vm((npair, 2, n, c), BF), vm((rows, c, n), F32), vm((rows, c, n), BF),
                vm((heads, rows, n), BF), vm((heads, n, n), BF), vm((2, n, heads * n), F32), vm((2, n // 2, rows, c), BF),
                vm((rows, n, c), BF), vm((npair, 2 * c, 2 * n), BF), vm((rows, n, c), BF), vm((npair, c, 2 * n), F32),
                vm((npair, c, 2 * n), BF), vm((heads, rows, n), BF), vm((heads, n, n), BF), vm((n, heads * n), F32),
                vm((rows, n, c), BF), vm((n, rows, c), BF), vm((2, n, heads * n), F32),
                vm((2, c, 2 * n), F32), vm((2, c, 2 * n), BF), vm((c, 2 * n), BF), vm((2, 2, c, n), BF),
                *[vm(w.shape, BF) for w in weights],
                vm(wqs.shape[::-1], BF), vm(wqe.shape[::-1], BF), vm(woe.shape[::-1], BF),
                vm(w1.shape[::-1], BF), vm(w2.shape[::-1], BF),
                vm((heads * 16, 8 * c), BF), vm((heads * 16, 8 * c), BF),
                dma((8,)), dma((8,)), dma, dma((2,)), dma, dma((4,)), dma, dma, dma, dma((3,)), dma, dma((4,)),
            ],
            compiler_params=pltpu.CompilerParams(collective_id=0, has_side_effects=True, vmem_limit_bytes=36 * 2 ** 20),
            name="pair_block",
        )(*[pltpu.with_memory_space_constraint(a, pltpu.HBM) for a in args])

    return jax.shard_map(local_fn, mesh=mesh, in_specs=(row_spec,) + (P(),) * 8, out_specs=row_spec, check_vma=False)
```

```python
import functools

import jax
import jax.numpy as jnp
from jax import lax
from jax.experimental import pallas as pl
from jax.experimental.pallas import tpu as pltpu
from jax.sharding import PartitionSpec as P

MESH = pl.DeviceIdType.MESH
EPS = 1e-5
TILE = 8
GROUP = 16
LOG2E = 1.4426950408889634
BF = jnp.bfloat16
F32 = jnp.float32


def dot(a, b):
    return jnp.dot(a, b, preferred_element_type=F32)


def dot_tn(a, b):
    return lax.dot_general(a, b, (((0,), (0,)), ((), ())), preferred_element_type=F32)


def norm_t(xt):
    mean = jnp.sum(xt, axis=0, keepdims=True) * (1.0 / xt.shape[0])
    cen = xt - mean
    var = jnp.sum(cen * cen, axis=0, keepdims=True) * (1.0 / xt.shape[0])
    return (cen * lax.rsqrt(var + EPS)).astype(BF)


def sigmoid(x):
    return 0.5 * jnp.tanh(0.5 * x) + 0.5


def block_diag(qt, pair, heads):
    hd, n = qt.shape
    d = hd // heads
    cols = []
    for h in (2 * pair, 2 * pair + 1):
        parts = []
        if h:
            parts.append(jnp.zeros((h * d, n), BF))
        parts.append(qt[h * d:(h + 1) * d])
        if h < heads - 1:
            parts.append(jnp.zeros(((heads - 1 - h) * d, n), BF))
        cols.append(jnp.concatenate(parts, axis=0))
    return jnp.concatenate(cols, axis=1)


def stage_scores(kn, qv, s, p, heads):
    c, n = kn.shape[1:]
    for r in range(2):
        keys = kn[2 * p + r]
        qt = qv[p, :c, r * n:(r + 1) * n]
        for pair in range(heads // 2):
            s[r, :, 2 * pair * n:(2 * pair + 2) * n] = dot(keys, block_diag(qt, pair, heads))


def stage_mix(s, biast, qv, g, og, p, heads):
    n = s.shape[1]
    c = qv.shape[1] // 2
    d = c // heads
    scale = LOG2E * d ** -0.5
    for r in range(2):
        for pair in range(heads // 2):
            probs = []
            for h in (2 * pair, 2 * pair + 1):
                t = s[r, :, h * n:(h + 1) * n] * scale + biast[:, h * n:(h + 1) * n]
                e = jnp.exp2(t - jnp.max(t, axis=0, keepdims=True))
                probs.append((e * (1.0 / jnp.sum(e, axis=0, keepdims=True))).astype(BF))
            rows = slice(c + 2 * pair * d, c + (2 * pair + 2) * d)
            o = dot(qv[p, rows, r * n:(r + 1) * n], jnp.concatenate(probs, axis=1))
            for i in range(2):
                h = 2 * pair + i
                out = o[i * d:(i + 1) * d, i * n:(i + 1) * n] * g[p, h * d:(h + 1) * d, r * n:(r + 1) * n]
                og[p, h * d:(h + 1) * d, r * n:(r + 1) * n] = out.astype(BF)


def norm_blocks(src, ut, b0, count):
    for r in range(count):
        ut[b0 + r] = norm_t(src[b0 + r])


def head_rows(wb):
    heads, c = wb.shape
    rep = jnp.broadcast_to(wb.astype(F32)[:, None, :], (heads, GROUP, c)).reshape(heads * GROUP, c)
    row = lax.broadcasted_iota(jnp.int32, rep.shape, 0) % GROUP // 2
    return jnp.concatenate([jnp.where(row == j, rep, 0.0) for j in range(TILE)], axis=1).astype(BF)


def bias_rows(w8, ub, dst, i, swap=None):
    heads, rows, n = dst.shape
    c = ub.shape[1]
    half = n // 2
    r0, r1 = [dot(w8, ub[s * rows // 2 + TILE * i:s * rows // 2 + TILE * i + TILE].reshape(TILE * c, n)) for s in range(2)]
    first, second = [(r0[:, lane:lane + half], r1[:, lane:lane + half]) for lane in (0, half)]
    even = lax.broadcasted_iota(jnp.int32, r0.shape, 0) % 2 == 0
    res = jnp.where(even, jnp.concatenate(first, axis=1), jnp.concatenate(second, axis=1))
    if swap is not None:
        res = jnp.where(swap, jnp.concatenate([res[:, half:], res[:, :half]], axis=1), res)
    dst[:, GROUP * i:GROUP * i + GROUP] = res.reshape(heads, GROUP, n).astype(BF)


def low_half(shape):
    return lax.broadcasted_iota(jnp.int32, shape, 1) < shape[1] // 2


def pair_project(wt, ub, qb, kt_ref, vst, g, p, npair, heads):
    own, oth = ub[p], ub[npair + p]
    c, n = own.shape
    d, half = c // heads, n // 2
    u = jnp.concatenate([own, oth], axis=1)
    q = dot(wt[0:c], u).astype(BF)
    qb[p] = q[:, :n]
    qb[npair + p] = q[:, n:]
    u_row = jnp.concatenate([own[:, :half], oth[:, :half], own[:, half:], oth[:, half:]], axis=1)
    k = dot(wt[c:2 * c], u_row).astype(BF)
    v = dot(wt[2 * c:3 * c], u_row).astype(BF)
    for h in range(heads):
        for i in range(2):
            rows = pl.ds((h % 2) * 2 * d + i * d, d)
            kt_ref[h // 2, rows] = k[h * d:(h + 1) * d, i * n:(i + 1) * n]
            vst[p, h // 2, rows] = v[h * d:(h + 1) * d, i * n:(i + 1) * n]
    gate = sigmoid(dot(wt[3 * c:], u))
    g[p] = gate[:, :n]
    g[npair + p] = gate[:, n:]


def block_scores(kn, qb, s, slot, b, p, heads):
    c, n = qb.shape[1:]
    d = c // heads
    low = low_half((d, n))
    zero = jnp.zeros((d, n), BF)
    for pair in range(heads // 2):
        rows = []
        for i in range(2):
            q = qb[b, (2 * pair + i) * d:(2 * pair + i + 1) * d]
            for part in (jnp.where(low, q, zero), jnp.where(low, zero, q)):
                rows.append(jnp.concatenate([part, zero] if i == 0 else [zero, part], axis=1))
        s[slot, :, 2 * pair * n:(2 * pair + 2) * n] = dot(kn[p, pair], jnp.concatenate(rows, axis=0))


def softmax_t(t):
    e = jnp.exp2(t - jnp.max(t, axis=0, keepdims=True))
    return (e * (1.0 / jnp.sum(e, axis=0, keepdims=True))).astype(BF)


def block_mix(s, slot, biast, side, vst, g, og, b, p, heads):
    c, n = og.shape[1:]
    d = c // heads
    low = low_half((d, n))
    for h in range(heads):
        t = s[slot, :, h * n:(h + 1) * n] * (LOG2E * d ** -0.5) + biast[side, :, h * n:(h + 1) * n]
        o = dot(vst[p, h // 2, (h % 2) * 2 * d:(h % 2 + 1) * 2 * d], softmax_t(t))
        og[b, h * d:(h + 1) * d] = (jnp.where(low, o[:d], o[d:]) * g[b, h * d:(h + 1) * d]).astype(BF)


def project(wt, u, n, qv_ref, kt_ref, g_ref, p):
    c = u.shape[0]
    qv_ref[p, :c] = dot(wt[0:c], u).astype(BF)
    kt_ref[...] = dot(wt[c:2 * c], u).astype(BF)
    qv_ref[p, c:] = dot(wt[2 * c:3 * c], u).astype(BF)
    g_ref[p] = sigmoid(dot(wt[3 * c:], u))


def turn_keys(kt_ref, kn_ref, p):
    n = kn_ref.shape[1]
    kn_ref[2 * p] = kt_ref[:, :n].T
    kn_ref[2 * p + 1] = kt_ref[:, n:].T


def kernel(z_hbm, wqs_h, wbs_h, wos_h, wqe_h, wbe_h, woe_h, w1_h, w2_h, y,
           zs4, z1, ub, qb, vst, knp, gb, ogb, bsend, ball, biasp, hsend,
           hcol, qv, kn, g, og, besend, beall, biast, dsend, drecv, s, s_next, eb, u2, kt, ktp,
           wqs, wbs, wos, wqe, wbe, woe, w1, w2, wqst, wqet, woet, w1t, w2t, wbs8, wbe8,
           zsem, wsem, bs_s, bs_r, h_s, h_r, o_s, o_r, be_s, be_r, d_s, d_r):
    rows, n, c = y.shape
    npair = rows // 2
    half = n // 2
    heads = wbs.shape[0]
    dp, sp = lax.axis_index("dp"), lax.axis_index("sp")
    x, core = sp // 2, sp % 2
    peers = [2 * (1 - x) + core, 2 * (1 - x) + 1 - core, 2 * x + 1 - core]
    mine = pl.multiple_of(sp * rows, rows)

    def zcopy(ci):
        q, side = ci // 2, ci % 2
        return pltpu.make_async_copy(z_hbm.at[pl.ds(4 * q, 4), :, (x + side) % 2],
                                     zs4.at[pl.ds(side * npair + 4 * q, 4)], zsem.at[ci])

    def wcopy(i):
        src = (wbs_h, wqs_h, wqe_h, woe_h, w1_h, w2_h, wbe_h, wos_h)[i]
        return pltpu.make_async_copy(src, (wbs, wqs, wqe, woe, w1, w2, wbe, wos)[i], wsem.at[i])

    wcopy(0).start()
    wcopy(6).start()
    for ci in range(TILE):
        zcopy(ci).start()
    for i in (1, 7, 2, 3, 4, 5):
        wcopy(i).start()
    bar = pltpu.get_barrier_semaphore()
    for t in peers:
        pl.semaphore_signal(bar, inc=1, device_id=(dp, t), device_id_type=MESH)

    def remote(src, dst, ssem, rsem, t):
        return pltpu.make_async_remote_copy(src, dst, ssem, rsem, device_id=(dp, t), device_id_type=MESH)

    wcopy(0).wait()
    wcopy(6).wait()
    wbs8[...] = head_rows(wbs[...])
    wbe8[...] = head_rows(wbe[...])

    def chunk_base(ci):
        return ci % 2 * npair + ci // 2 * 4

    def ln_step(ci, _):
        for side in range(2):
            zcopy(2 * ci + side).wait()
        for side in range(2):
            norm_blocks(y, ub, chunk_base(jnp.maximum(2 * ci - 2, 0) + side), 4)
        for side in range(2):
            b0 = chunk_base(2 * ci + side)
            for r in range(4):
                y[b0 + r] = zs4[b0 + r].reshape(n, c).T
        return _
    lax.fori_loop(0, 4, ln_step, 0)
    bias_rows(wbs8[...], ub, bsend, 0)
    for side in range(2):
        norm_blocks(y, ub, chunk_base(6 + side), 4)
    for i in range(1, rows // GROUP):
        bias_rows(wbs8[...], ub, bsend, i)
    ball[:, pl.ds(pl.multiple_of(core * rows, rows), rows)] = bsend[...]
    pl.semaphore_wait(bar, 3)

    def bias_copy(k, t, owner):
        return remote(bsend, ball.at[:, pl.ds(pl.multiple_of((half if k < 2 else 0) + owner % 2 * rows, rows), rows)],
                      bs_s, bs_r.at[k // 2], t)

    def end_bias_part(owner, i):
        return beall.at[:, pl.ds(pl.multiple_of(owner * rows + GROUP * i, GROUP), GROUP)]

    def end_bias_send(i):
        part = besend.at[:, GROUP * i:GROUP * i + GROUP]
        for k in ((0, 2), range(3))[i]:
            remote(part, end_bias_part(sp, i), be_s, be_r.at[2 if k == 2 else i], peers[k]).start()

    def end_bias_forward():
        part = end_bias_part(peers[0], 0)
        arrived(part, be_r.at[0])
        remote(part, part, be_s, be_r.at[2], peers[2]).start()

    def sent(ref, sem):
        remote(ref, ref, sem, sem, peers[0]).wait_send()

    def arrived(ref, sem):
        remote(ref, ref, sem, sem, peers[0]).wait_recv()

    for k in (2, 0, 1):
        bias_copy(k, peers[k], sp).start()

    wcopy(1).wait()
    wcopy(7).wait()
    wqst[...] = wqs[...].T
    def start_project(*pairs):
        for p in pairs:
            pair_project(wqst, ub, qb, ktp.at[p % 2], vst, gb, p, npair, heads)
        for p in pairs:
            for pair in range(heads // 2):
                knp[p, pair] = ktp[p % 2, pair].T

    def start_bias(side):
        for h in range(heads):
            rws = ball[h, side * half:(side + 1) * half].astype(F32)
            tr = jnp.concatenate([rws, rws], axis=0).T * LOG2E
            if side:
                tr = jnp.concatenate([tr[half:], tr[:half]], axis=0)
            biasp[side, :, h * n:(h + 1) * n] = tr

    def start_out(b):
        upd = dot_tn(jnp.concatenate([ogb[b], ogb[b + 1]], axis=1), wos[...])
        z1[b] = zs4[b].reshape(n, c) + upd[:n]
        z1[b + 1] = zs4[b + 1].reshape(n, c) + upd[n:]
    def start_norm(b):
        for r in range(2):
            ub[b + r] = norm_t(z1[b + r].astype(BF).astype(F32).T)

    def start_mix(b, buf=s):
        for r in range(2):
            block_mix(buf, r, biasp, b // npair, vst, gb, ogb, b + r, b % npair + r, heads)

    def start_scores(b, buf=s):
        for r in range(2):
            block_scores(knp, qb, buf, r, b + r, b % npair + r, heads)

    def start_step(t, _):
        for by, stage in ((3, start_norm), (2, start_out), (1, start_mix), (0, start_scores)):
            if not isinstance(t, int) or 0 <= t - by < npair:
                stage(2 * (t - by))
        return _

    chunks = 4
    cols = rows // chunks
    groups = [(0, TILE), (TILE, TILE), (GROUP, GROUP)]
    near = [(0, GROUP), (GROUP, GROUP)]

    def h_copy(gi, ch, k, t, owner):
        r0, size = groups[gi]
        return remote(hsend.at[0, pl.ds(t % 2 * rows + ch * cols, cols), r0:r0 + size],
                      hcol.at[pl.ds(ch * cols, cols), pl.ds(pl.multiple_of(owner * rows + r0, TILE), size)],
                      h_s, h_r.at[ch], t)

    def near_copy(gi, owner):
        r0, size = near[gi]
        return remote(hsend.at[1, pl.ds(pl.multiple_of((1 - core) * rows, rows), rows), r0:r0 + size],
                      hcol.at[:, pl.ds(pl.multiple_of(owner * rows + r0, TILE), size)],
                      o_s, o_r, peers[2])

    def shuffle_rows(side, r0, size):
        def body(jb, _):
            j0 = pl.multiple_of(jb * TILE, TILE)
            parts = []
            for row in range(r0, r0 + size):
                b = side * npair + row // 2
                parts.append(z1[b:b + 1, pl.ds(row % 2 * half + j0, TILE)])
            blk = jnp.swapaxes(jnp.concatenate(parts, axis=0), 0, 1)
            hsend[side, pl.ds(j0, TILE), r0:r0 + size] = blk.astype(BF)
            return _
        lax.fori_loop(0, half // TILE, body, 0, unroll=2)

    def send_h(gi, chs):
        for ch in chs:
            for k in range(2):
                h_copy(gi, ch, k, peers[k], sp).start()

    start_project(0, 1)
    start_project(2, 3)
    start_scores(0)
    start_scores(2, s_next)
    arrived(ball.at[:, 0:rows], bs_r.at[1])
    start_bias(0)
    start_mix(0)
    start_mix(2, s_next)
    start_out(0)
    start_out(2)
    shuffle_rows(0, 0, TILE)
    send_h(0, range(chunks))
    start_project(4, 5)
    start_scores(4)
    start_project(6, 7)
    start_norm(0)
    start_mix(4)
    start_scores(6)
    start_project(TILE, 9)
    start_norm(2)
    start_out(4)
    start_mix(6)
    start_scores(TILE)
    start_project(10, 11)
    start_step(5, 0)
    shuffle_rows(0, TILE, TILE)
    send_h(1, range(chunks))
    for t in (6, 7):
        start_project(2 * t, 2 * t + 1)
        start_step(t, 0)
    start_step(TILE, 0)
    arrived(ball.at[:, 0:2 * rows], bs_r.at[0])
    start_bias(1)
    start_step(9, 0)
    shuffle_rows(0, GROUP, GROUP)
    send_h(2, [0])
    lax.fori_loop(10, 14, start_step, 0, unroll=4)
    shuffle_rows(1, 0, GROUP)
    near_copy(0, sp).start()
    start_step(14, 0)
    bias_rows(wbe8[...], ub, besend, 0, x == 1)
    end_bias_send(0)
    for t in range(15, npair + 3):
        start_step(t, 0)
    bias_rows(wbe8[...], ub, besend, 1, x == 1)
    end_bias_send(1)
    beall[:, pl.ds(mine, rows)] = besend[...]
    shuffle_rows(1, GROUP, GROUP)
    near_copy(1, sp).start()
    send_h(2, [1])
    hcol[:, pl.ds(mine, rows)] = hsend[1, pl.ds(pl.multiple_of(core * rows, rows), rows)]
    for i in range(2, 6):
        wcopy(i).wait()
    wqet[...] = wqe[...].T
    woet[...] = woe[...].T
    w1t[...] = w1[...].T
    w2t[...] = w2[...].T
    sent(ball.at[:, 0:3 * rows], bs_s)

    def end_delta(p):
        hid = jnp.maximum(dot(w1t[...], u2[p % 2]), 0.0).astype(BF)
        delta = (eb[p % 2] + dot(w2t[...], hid)).astype(BF)
        dsend[2 * p] = delta[:, :n].T
        dsend[2 * p + 1] = delta[:, n:].T

    def columns(p):
        return jnp.concatenate([hcol[2 * p].astype(F32).T, hcol[2 * p + 1].astype(F32).T], axis=1)

    def end_out(p):
        e = dot(woet[...], og[p])
        eb[p % 2] = e
        u2[p % 2] = norm_t(columns(p) + e)

    def end_mix(p):
        stage_mix(s, biast, qv, g, og, p, heads)

    def end_scores(p):
        turn_keys(kt, kn, p)
        stage_scores(kn, qv, s, p, heads)

    def end_project(p):
        project(wqet, norm_t(columns(p)), n, qv, kt, g, p)

    def end_step(t):
        for by, stage in ((4, end_delta), (3, end_out), (2, end_mix), (1, end_scores), (0, end_project)):
            if not isinstance(t, int) or 0 <= t - by < npair:
                stage(t - by)

    def d_copy(q, count, t, first_col):
        return remote(dsend.at[pl.ds(2 * q, 2 * count), pl.ds(pl.multiple_of(t * rows, rows), rows)],
                      drecv.at[pl.ds(first_col + 2 * q, 2 * count)], d_s, d_r.at[q // (npair // chunks)], t)

    my_cols = pl.multiple_of((2 * (1 - x) + core) * rows, rows)

    def send_d(q, count):
        for t in peers:
            d_copy(q, count, t, my_cols).start()

    def wait_h(ch):
        arrived(hcol.at[pl.ds(ch * cols, cols), 0:2 * rows], h_r.at[ch])

    arrived(hcol.at[:, 0:rows], o_r)
    send_h(2, [2])
    end_bias_forward()
    send_h(2, [3])
    wait_h(0)
    end_step(0)
    end_step(1)
    arrived(beall.at[:, 0:rows], be_r.at[1])
    arrived(beall.at[:, 0:rows + GROUP], be_r.at[2])
    for h in range(heads):
        biast[:, h * n:(h + 1) * n] = beall[h].astype(F32) * LOG2E
    end_step(2)
    end_step(3)

    def segment(i, _):
        @pl.when(i % 2 == 0)
        def _wait():
            wait_h(i // 2)
        end_step(2 * i)
        end_step(2 * i + 1)
        send_d(2 * i - 4, 2)
        return _
    lax.fori_loop(2, npair // 2, segment, 0)
    for t in range(npair, npair + 4):
        end_step(t)
        send_d(t - 4, 1)
    drecv[pl.ds(my_cols, rows)] = dsend[:, pl.ds(mine, rows)]

    def final_block(side, owner_core, first_col, ch):
        j0 = pl.multiple_of(first_col + ch * cols, TILE)
        jj = owner_core * rows + ch * cols
        for gi in range(rows // GROUP):
            blk = jnp.swapaxes(drecv[pl.ds(j0, TILE), gi * GROUP:(gi + 1) * GROUP].astype(F32), 0, 1)
            for r in range(GROUP):
                row = GROUP * gi + r
                part = z1[side * npair + row // 2, pl.ds(pl.multiple_of(row % 2 * half + jj, TILE), TILE)]
                y[row, pl.ds(j0, TILE)] = part + blk[r]

    for ch in range(chunks):
        final_block(1, core, my_cols, ch)
    for ch in range(chunks):
        arrived(drecv.at[0:3 * cols], d_r.at[ch])
        for k in (2, 0, 1):
            t = peers[k]
            first_col = pl.multiple_of((2 * x + t % 2 if k < 2 else 2 * (1 - x) + t % 2) * rows, rows)
            final_block(0 if k < 2 else 1, t % 2, first_col, ch)
    sent(hsend.at[0], h_s)
    sent(ball.at[:, 0:3 * rows], be_s)
    sent(hcol.at[:, 0:rows], o_s)
    sent(dsend.at[:, 0:3 * rows], d_s)


def solution(mesh):
    row_spec = P(('dp', 'sp'), None, None)
    sp = mesh.shape['sp']

    def local_fn(pair_loc, wqs, wbs, wos, wqe, wbe, woe, w1, w2):
        rows, n, c = pair_loc.shape
        heads = wbs.shape[0]
        dma = pltpu.SemaphoreType.DMA
        vm = pltpu.VMEM
        weights = (wqs, wbs, wos, wqe, wbe, woe, w1, w2)
        npair = rows // 2
        args = (pair_loc.reshape(npair, 2, 2, n // 2, c),) + weights
        return pl.pallas_call(
            kernel,
            out_shape=vm(pair_loc.shape, F32),
            in_specs=[pl.BlockSpec(memory_space=pltpu.HBM)] * 9,
            out_specs=pl.BlockSpec(memory_space=vm),
            scratch_shapes=[
                vm((rows, 2, n // 2, c), F32), vm((rows, n, c), F32), vm((rows, c, n), BF), vm((rows, c, n), BF),
                vm((npair, 2, c, n), BF), vm((npair, 2, n, c), BF), vm((rows, c, n), F32), vm((rows, c, n), BF),
                vm((heads, rows, n), BF), vm((heads, n, n), BF), vm((2, n, heads * n), F32), vm((2, n // 2, rows, c), BF),
                vm((rows, n, c), BF), vm((npair, 2 * c, 2 * n), BF), vm((rows, n, c), BF), vm((npair, c, 2 * n), F32),
                vm((npair, c, 2 * n), BF), vm((heads, rows, n), BF), vm((heads, n, n), BF), vm((n, heads * n), F32),
                vm((rows, n, c), BF), vm((n, rows, c), BF), vm((2, n, heads * n), F32), vm((2, n, heads * n), F32),
                vm((2, c, 2 * n), F32), vm((2, c, 2 * n), BF), vm((c, 2 * n), BF), vm((2, 2, c, n), BF),
                *[vm(w.shape, BF) for w in weights],
                vm(wqs.shape[::-1], BF), vm(wqe.shape[::-1], BF), vm(woe.shape[::-1], BF),
                vm(w1.shape[::-1], BF), vm(w2.shape[::-1], BF),
                vm((heads * GROUP, TILE * c), BF), vm((heads * GROUP, TILE * c), BF),
                dma((TILE,)), dma((TILE,)), dma, dma((2,)), dma, dma((4,)), dma, dma, dma, dma((3,)), dma, dma((4,)),
            ],
            compiler_params=pltpu.CompilerParams(collective_id=0, has_side_effects=True, vmem_limit_bytes=36 * 2 ** 20),
            name="pair_block",
        )(*[pltpu.with_memory_space_constraint(a, pltpu.HBM) for a in args])

    return jax.shard_map(local_fn, mesh=mesh, in_specs=(row_spec,) + (P(),) * TILE, out_specs=row_spec, check_vma=False)
```

```python
import functools

import jax
import jax.numpy as jnp
from jax import lax
from jax.experimental import pallas as pl
from jax.experimental.pallas import tpu as pltpu
from jax.sharding import PartitionSpec as P

MESH = pl.DeviceIdType.MESH
EPS = 1e-5
TILE = 8
GROUP = 16
LOG2E = 1.4426950408889634
BF = jnp.bfloat16
F32 = jnp.float32


def dot(a, b):
    return jnp.dot(a, b, preferred_element_type=F32)


def dot_tn(a, b):
    return lax.dot_general(a, b, (((0,), (0,)), ((), ())), preferred_element_type=F32)


def norm_t(xt):
    mean = jnp.sum(xt, axis=0, keepdims=True) * (1.0 / xt.shape[0])
    cen = xt - mean
    var = jnp.sum(cen * cen, axis=0, keepdims=True) * (1.0 / xt.shape[0])
    return (cen * lax.rsqrt(var + EPS)).astype(BF)


def sigmoid(x):
    return 0.5 * jnp.tanh(0.5 * x) + 0.5


def block_diag(qt, pair, heads):
    hd, n = qt.shape
    d = hd // heads
    cols = []
    for h in (2 * pair, 2 * pair + 1):
        parts = []
        if h:
            parts.append(jnp.zeros((h * d, n), BF))
        parts.append(qt[h * d:(h + 1) * d])
        if h < heads - 1:
            parts.append(jnp.zeros(((heads - 1 - h) * d, n), BF))
        cols.append(jnp.concatenate(parts, axis=0))
    return jnp.concatenate(cols, axis=1)


def stage_scores(kn, qv, s, p, heads):
    c, n = kn.shape[1:]
    for r in range(2):
        keys = kn[2 * p + r]
        qt = qv[p, :c, r * n:(r + 1) * n]
        for pair in range(heads // 2):
            s[r, :, 2 * pair * n:(2 * pair + 2) * n] = dot(keys, block_diag(qt, pair, heads))


def stage_mix(s, biast, qv, g, og, p, heads):
    n = s.shape[1]
    c = qv.shape[1] // 2
    d = c // heads
    scale = LOG2E * d ** -0.5
    for r in range(2):
        for pair in range(heads // 2):
            probs = []
            for h in (2 * pair, 2 * pair + 1):
                t = s[r, :, h * n:(h + 1) * n] * scale + biast[:, h * n:(h + 1) * n]
                e = jnp.exp2(t - jnp.max(t, axis=0, keepdims=True))
                probs.append((e * (1.0 / jnp.sum(e, axis=0, keepdims=True))).astype(BF))
            rows = slice(c + 2 * pair * d, c + (2 * pair + 2) * d)
            o = dot(qv[p, rows, r * n:(r + 1) * n], jnp.concatenate(probs, axis=1))
            for i in range(2):
                h = 2 * pair + i
                out = o[i * d:(i + 1) * d, i * n:(i + 1) * n] * g[p, h * d:(h + 1) * d, r * n:(r + 1) * n]
                og[p, h * d:(h + 1) * d, r * n:(r + 1) * n] = out.astype(BF)


def norm_blocks(src, ut, b0, count):
    for r in range(count):
        ut[b0 + r] = norm_t(src[b0 + r])


def head_rows(wb):
    heads, c = wb.shape
    rep = jnp.broadcast_to(wb.astype(F32)[:, None, :], (heads, GROUP, c)).reshape(heads * GROUP, c)
    row = lax.broadcasted_iota(jnp.int32, rep.shape, 0) % GROUP // 2
    return jnp.concatenate([jnp.where(row == j, rep, 0.0) for j in range(TILE)], axis=1).astype(BF)


def bias_rows(w8, ub, dst, i, swap=None):
    heads, rows, n = dst.shape
    c = ub.shape[1]
    half = n // 2
    r0, r1 = [dot(w8, ub[s * rows // 2 + TILE * i:s * rows // 2 + TILE * i + TILE].reshape(TILE * c, n)) for s in range(2)]
    first, second = [(r0[:, lane:lane + half], r1[:, lane:lane + half]) for lane in (0, half)]
    even = lax.broadcasted_iota(jnp.int32, r0.shape, 0) % 2 == 0
    res = jnp.where(even, jnp.concatenate(first, axis=1), jnp.concatenate(second, axis=1))
    if swap is not None:
        res = jnp.where(swap, jnp.concatenate([res[:, half:], res[:, :half]], axis=1), res)
    dst[:, GROUP * i:GROUP * i + GROUP] = res.reshape(heads, GROUP, n).astype(BF)


def low_half(shape):
    return lax.broadcasted_iota(jnp.int32, shape, 1) < shape[1] // 2


def pair_project(wt, ub, qb, kt_ref, vst, g, p, npair, heads):
    own, oth = ub[p], ub[npair + p]
    c, n = own.shape
    d, half = c // heads, n // 2
    u = jnp.concatenate([own, oth], axis=1)
    q = dot(wt[0:c], u).astype(BF)
    qb[p] = q[:, :n]
    qb[npair + p] = q[:, n:]
    u_row = jnp.concatenate([own[:, :half], oth[:, :half], own[:, half:], oth[:, half:]], axis=1)
    k = dot(wt[c:2 * c], u_row).astype(BF)
    v = dot(wt[2 * c:3 * c], u_row).astype(BF)
    for h in range(heads):
        for i in range(2):
            rows = pl.ds((h % 2) * 2 * d + i * d, d)
            kt_ref[h // 2, rows] = k[h * d:(h + 1) * d, i * n:(i + 1) * n]
            vst[p, h // 2, rows] = v[h * d:(h + 1) * d, i * n:(i + 1) * n]
    gate = sigmoid(dot(wt[3 * c:], u))
    g[p] = gate[:, :n]
    g[npair + p] = gate[:, n:]


def block_scores(kn, qb, s, slot, b, p, heads):
    c, n = qb.shape[1:]
    d = c // heads
    low = low_half((d, n))
    zero = jnp.zeros((d, n), BF)
    for pair in range(heads // 2):
        rows = []
        for i in range(2):
            q = qb[b, (2 * pair + i) * d:(2 * pair + i + 1) * d]
            for part in (jnp.where(low, q, zero), jnp.where(low, zero, q)):
                rows.append(jnp.concatenate([part, zero] if i == 0 else [zero, part], axis=1))
        s[slot, :, 2 * pair * n:(2 * pair + 2) * n] = dot(kn[p, pair], jnp.concatenate(rows, axis=0))


def softmax_t(t):
    e = jnp.exp2(t - jnp.max(t, axis=0, keepdims=True))
    return (e * (1.0 / jnp.sum(e, axis=0, keepdims=True))).astype(BF)


def block_mix(s, slot, biast, side, vst, g, og, b, p, heads):
    c, n = og.shape[1:]
    d = c // heads
    low = low_half((d, n))
    for h in range(heads):
        t = s[slot, :, h * n:(h + 1) * n] * (LOG2E * d ** -0.5) + biast[side, :, h * n:(h + 1) * n]
        o = dot(vst[p, h // 2, (h % 2) * 2 * d:(h % 2 + 1) * 2 * d], softmax_t(t))
        og[b, h * d:(h + 1) * d] = (jnp.where(low, o[:d], o[d:]) * g[b, h * d:(h + 1) * d]).astype(BF)


def project(wt, u, n, qv_ref, kt_ref, g_ref, p):
    c = u.shape[0]
    qv_ref[p, :c] = dot(wt[0:c], u).astype(BF)
    kt_ref[...] = dot(wt[c:2 * c], u).astype(BF)
    qv_ref[p, c:] = dot(wt[2 * c:3 * c], u).astype(BF)
    g_ref[p] = sigmoid(dot(wt[3 * c:], u))


def turn_keys(kt_ref, kn_ref, p):
    n = kn_ref.shape[1]
    kn_ref[2 * p] = kt_ref[:, :n].T
    kn_ref[2 * p + 1] = kt_ref[:, n:].T


def kernel(z_hbm, wqs_h, wbs_h, wos_h, wqe_h, wbe_h, woe_h, w1_h, w2_h, y,
           zs4, z1, ub, qb, vst, knp, gb, ogb, bsend, ball, biasp, hsend,
           hcol, qv, kn, g, og, besend, beall, biast, dsend, drecv, s, s_next, eb, u2, kt, ktp,
           wqs, wbs, wos, wqe, wbe, woe, w1, w2, wqst, wqet, woet, w1t, w2t, wbs8, wbe8,
           zsem, wsem, bs_s, bs_r, h_s, h_r, o_s, o_r, be_s, be_r, d_s, d_r):
    rows, n, c = y.shape
    npair = rows // 2
    half = n // 2
    heads = wbs.shape[0]
    dp, sp = lax.axis_index("dp"), lax.axis_index("sp")
    x, core = sp // 2, sp % 2
    peers = [2 * (1 - x) + core, 2 * (1 - x) + 1 - core, 2 * x + 1 - core]
    mine = pl.multiple_of(sp * rows, rows)

    def zcopy(ci):
        q, side = ci // 2, ci % 2
        return pltpu.make_async_copy(z_hbm.at[pl.ds(4 * q, 4), :, (x + side) % 2],
                                     zs4.at[pl.ds(side * npair + 4 * q, 4)], zsem.at[q])

    def wcopy(i):
        src = (wbs_h, wqs_h, wqe_h, woe_h, w1_h, w2_h, wbe_h, wos_h)[i]
        return pltpu.make_async_copy(src, (wbs, wqs, wqe, woe, w1, w2, wbe, wos)[i], wsem.at[(0, 1, 2, 2, 2, 2, 3, 4)[i]])

    wcopy(0).start()
    wcopy(6).start()
    for ci in range(TILE):
        zcopy(ci).start()
    for i in (1, 7, 2, 3, 4, 5):
        wcopy(i).start()
    bar = pltpu.get_barrier_semaphore()
    for t in peers:
        pl.semaphore_signal(bar, inc=1, device_id=(dp, t), device_id_type=MESH)

    def remote(src, dst, ssem, rsem, t):
        return pltpu.make_async_remote_copy(src, dst, ssem, rsem, device_id=(dp, t), device_id_type=MESH)

    def sent(ref, sem):
        remote(ref, ref, sem, sem, peers[0]).wait_send()

    def arrived(ref, sem):
        remote(ref, ref, sem, sem, peers[0]).wait_recv()

    wcopy(0).wait()
    wcopy(6).wait()
    wbs8[...] = head_rows(wbs[...])
    wbe8[...] = head_rows(wbe[...])

    def chunk_base(ci):
        return ci % 2 * npair + ci // 2 * 4

    def turn_chunks(q):
        arrived(zs4.at[0:TILE], zsem.at[q])
        for side in range(2):
            b0 = chunk_base(2 * q + side)
            for r in range(4):
                y[b0 + r] = zs4[b0 + r].reshape(n, c).T

    def norm_chunks(q):
        for side in range(2):
            norm_blocks(y, ub, chunk_base(2 * q + side), 4)

    turn_chunks(0)
    for q in range(1, 4):
        turn_chunks(q)
        norm_chunks(q - 1)
    norm_chunks(3)
    bias_rows(wbs8[...], ub, bsend, 0)
    for side in range(2):
        norm_blocks(y, ub, chunk_base(6 + side), 4)
    for i in range(1, rows // GROUP):
        bias_rows(wbs8[...], ub, bsend, i)
    ball[:, pl.ds(pl.multiple_of(core * rows, rows), rows)] = bsend[...]
    pl.semaphore_wait(bar, 3)

    def bias_copy(k, t, owner):
        return remote(bsend, ball.at[:, pl.ds(pl.multiple_of((half if k < 2 else 0) + owner % 2 * rows, rows), rows)],
                      bs_s, bs_r.at[k // 2], t)

    def end_bias_part(owner, i):
        return beall.at[:, pl.ds(pl.multiple_of(owner * rows + GROUP * i, GROUP), GROUP)]

    def end_bias_send(i):
        part = besend.at[:, GROUP * i:GROUP * i + GROUP]
        for k in ((0, 2), range(3))[i]:
            remote(part, end_bias_part(sp, i), be_s, be_r.at[2 if k == 2 else i], peers[k]).start()

    def end_bias_forward():
        part = end_bias_part(peers[0], 0)
        arrived(part, be_r.at[0])
        remote(part, part, be_s, be_r.at[2], peers[2]).start()

    for k in (2, 0, 1):
        bias_copy(k, peers[k], sp).start()

    wcopy(1).wait()
    wcopy(7).wait()
    wqst[...] = wqs[...].T
    def start_project(*pairs):
        for p in pairs:
            pair_project(wqst, ub, qb, ktp.at[p % 2], vst, gb, p, npair, heads)
        for p in pairs:
            for pair in range(heads // 2):
                knp[p, pair] = ktp[p % 2, pair].T

    def start_bias(side):
        for h in range(heads):
            rws = ball[h, side * half:(side + 1) * half]
            tr = jnp.concatenate([rws, rws], axis=0).T.astype(F32) * LOG2E
            if side:
                tr = jnp.concatenate([tr[half:], tr[:half]], axis=0)
            biasp[side, :, h * n:(h + 1) * n] = tr

    def start_out(b):
        upd = dot_tn(jnp.concatenate([ogb[b], ogb[b + 1]], axis=1), wos[...])
        z1[b] = zs4[b].reshape(n, c) + upd[:n]
        z1[b + 1] = zs4[b + 1].reshape(n, c) + upd[n:]
    def start_norm(b):
        for r in range(2):
            ub[b + r] = norm_t(z1[b + r].astype(BF).astype(F32).T)

    def start_mix(b, buf=s):
        for r in range(2):
            block_mix(buf, r, biasp, b // npair, vst, gb, ogb, b + r, b % npair + r, heads)

    def start_scores(b, buf=s):
        for r in range(2):
            block_scores(knp, qb, buf, r, b + r, b % npair + r, heads)

    def start_step(t, _):
        for by, stage in ((3, start_norm), (2, start_out), (1, start_mix), (0, start_scores)):
            if not isinstance(t, int) or 0 <= t - by < npair:
                stage(2 * (t - by))
        return _

    chunks = 4
    cols = rows // chunks
    groups = [(0, TILE), (TILE, TILE), (GROUP, GROUP)]
    near = [(0, GROUP), (GROUP, GROUP)]

    def h_copy(gi, ch, k, t, owner):
        r0, size = groups[gi]
        return remote(hsend.at[0, pl.ds(t % 2 * rows + ch * cols, cols), r0:r0 + size],
                      hcol.at[pl.ds(ch * cols, cols), pl.ds(pl.multiple_of(owner * rows + r0, TILE), size)],
                      h_s, h_r.at[ch], t)

    def near_copy(gi, owner):
        r0, size = near[gi]
        return remote(hsend.at[1, pl.ds(pl.multiple_of((1 - core) * rows, rows), rows), r0:r0 + size],
                      hcol.at[:, pl.ds(pl.multiple_of(owner * rows + r0, TILE), size)],
                      o_s, o_r, peers[2])

    def shuffle_rows(side, r0, size):
        def body(jb, _):
            j0 = pl.multiple_of(jb * TILE, TILE)
            parts = []
            for row in range(r0, r0 + size):
                b = side * npair + row // 2
                parts.append(z1[b:b + 1, pl.ds(row % 2 * half + j0, TILE)])
            blk = jnp.swapaxes(jnp.concatenate(parts, axis=0), 0, 1)
            hsend[side, pl.ds(j0, TILE), r0:r0 + size] = blk.astype(BF)
            return _
        lax.fori_loop(0, half // TILE, body, 0, unroll=8)

    def send_h(gi, chs):
        for ch in chs:
            for k in range(2):
                h_copy(gi, ch, k, peers[k], sp).start()

    start_project(0, 1)
    start_project(2, 3)
    start_scores(0)
    start_scores(2, s_next)
    arrived(ball.at[:, 0:rows], bs_r.at[1])
    start_bias(0)
    start_mix(0)
    start_mix(2, s_next)
    start_out(0)
    start_out(2)
    shuffle_rows(0, 0, TILE)
    send_h(0, range(chunks))
    start_project(4, 5)
    start_scores(4)
    start_project(6, 7)
    start_norm(0)
    start_mix(4)
    start_scores(6)
    start_project(TILE, 9)
    start_norm(2)
    start_out(4)
    start_mix(6)
    start_scores(TILE)
    start_project(10, 11)
    start_step(5, 0)
    shuffle_rows(0, TILE, TILE)
    send_h(1, range(chunks))
    for t in (6, 7):
        start_project(2 * t, 2 * t + 1)
        start_step(t, 0)
    start_step(TILE, 0)
    arrived(ball.at[:, 0:2 * rows], bs_r.at[0])
    start_bias(1)
    start_step(9, 0)
    shuffle_rows(0, GROUP, GROUP)
    send_h(2, [0])
    lax.fori_loop(10, 14, start_step, 0, unroll=4)
    shuffle_rows(1, 0, GROUP)
    near_copy(0, sp).start()
    start_step(14, 0)
    bias_rows(wbe8[...], ub, besend, 0, x == 1)
    end_bias_send(0)
    for t in range(15, npair + 3):
        start_step(t, 0)
    bias_rows(wbe8[...], ub, besend, 1, x == 1)
    end_bias_send(1)
    beall[:, pl.ds(mine, rows)] = besend[...]
    shuffle_rows(1, GROUP, GROUP)
    near_copy(1, sp).start()
    send_h(2, [1])
    hcol[:, pl.ds(mine, rows)] = hsend[1, pl.ds(pl.multiple_of(core * rows, rows), rows)]
    arrived(hcol.at[0:13], wsem.at[2])
    wqet[...] = wqe[...].T
    woet[...] = woe[...].T
    w1t[...] = w1[...].T
    w2t[...] = w2[...].T
    sent(ball.at[:, 0:3 * rows], bs_s)

    def end_delta(p):
        hid = jnp.maximum(dot(w1t[...], u2[p % 2]), 0.0).astype(BF)
        delta = (eb[p % 2] + dot(w2t[...], hid)).astype(BF)
        dsend[2 * p] = delta[:, :n].T
        dsend[2 * p + 1] = delta[:, n:].T

    def columns(p):
        return jnp.concatenate([hcol[2 * p].astype(F32).T, hcol[2 * p + 1].astype(F32).T], axis=1)

    def end_out(p):
        e = dot(woet[...], og[p])
        eb[p % 2] = e
        u2[p % 2] = norm_t(columns(p) + e)

    def end_mix(p):
        stage_mix(s, biast, qv, g, og, p, heads)

    def end_scores(p):
        turn_keys(kt, kn, p)
        stage_scores(kn, qv, s, p, heads)

    def end_project(p):
        project(wqet, norm_t(columns(p)), n, qv, kt, g, p)

    def end_step(t):
        for by, stage in ((4, end_delta), (3, end_out), (2, end_mix), (1, end_scores), (0, end_project)):
            if not isinstance(t, int) or 0 <= t - by < npair:
                stage(t - by)

    def d_copy(q, count, t, first_col):
        return remote(dsend.at[pl.ds(2 * q, 2 * count), pl.ds(pl.multiple_of(t * rows, rows), rows)],
                      drecv.at[pl.ds(first_col + 2 * q, 2 * count)], d_s, d_r.at[q // (npair // chunks)], t)

    my_cols = pl.multiple_of((2 * (1 - x) + core) * rows, rows)

    def send_d(q, count):
        for t in peers:
            d_copy(q, count, t, my_cols).start()

    def wait_h(ch):
        arrived(hcol.at[pl.ds(ch * cols, cols), 0:2 * rows], h_r.at[ch])

    arrived(hcol.at[:, 0:rows], o_r)
    send_h(2, [2])
    end_bias_forward()
    send_h(2, [3])
    wait_h(0)
    end_step(0)
    end_step(1)
    arrived(beall.at[:, 0:rows], be_r.at[1])
    arrived(beall.at[:, 0:rows + GROUP], be_r.at[2])
    for h in range(heads):
        biast[:, h * n:(h + 1) * n] = beall[h].astype(F32) * LOG2E
    end_step(2)
    end_step(3)

    def segment(i, _):
        @pl.when(i % 2 == 0)
        def _wait():
            wait_h(i // 2)
        end_step(2 * i)
        end_step(2 * i + 1)
        send_d(2 * i - 4, 2)
        return _
    lax.fori_loop(2, npair // 2, segment, 0)
    for t in range(npair, npair + 4):
        end_step(t)
        send_d(t - 4, 1)
    drecv[pl.ds(my_cols, rows)] = dsend[:, pl.ds(mine, rows)]

    def final_block(side, owner_core, first_col, ch):
        j0 = pl.multiple_of(first_col + ch * cols, TILE)
        jj = owner_core * rows + ch * cols
        for gi in range(rows // GROUP):
            blk = jnp.swapaxes(drecv[pl.ds(j0, TILE), gi * GROUP:(gi + 1) * GROUP].astype(F32), 0, 1)
            for r in range(GROUP):
                row = GROUP * gi + r
                part = z1[side * npair + row // 2, pl.ds(pl.multiple_of(row % 2 * half + jj, TILE), TILE)]
                y[row, pl.ds(j0, TILE)] = part + blk[r]

    for ch in range(chunks):
        final_block(1, core, my_cols, ch)
    for ch in range(chunks):
        arrived(drecv.at[0:3 * cols], d_r.at[ch])
        for k in (2, 0, 1):
            t = peers[k]
            first_col = pl.multiple_of((2 * x + t % 2 if k < 2 else 2 * (1 - x) + t % 2) * rows, rows)
            final_block(0 if k < 2 else 1, t % 2, first_col, ch)
    sent(hsend.at[0], h_s)
    sent(ball.at[:, 0:3 * rows], be_s)
    sent(hcol.at[:, 0:rows], o_s)
    sent(dsend.at[:, 0:3 * rows], d_s)


def solution(mesh):
    row_spec = P(('dp', 'sp'), None, None)
    sp = mesh.shape['sp']

    def local_fn(pair_loc, wqs, wbs, wos, wqe, wbe, woe, w1, w2):
        rows, n, c = pair_loc.shape
        heads = wbs.shape[0]
        dma = pltpu.SemaphoreType.DMA
        vm = pltpu.VMEM
        weights = (wqs, wbs, wos, wqe, wbe, woe, w1, w2)
        npair = rows // 2
        args = (pair_loc.reshape(npair, 2, 2, n // 2, c),) + weights
        return pl.pallas_call(
            kernel,
            out_shape=vm(pair_loc.shape, F32),
            in_specs=[pl.BlockSpec(memory_space=pltpu.HBM)] * 9,
            out_specs=pl.BlockSpec(memory_space=vm),
            scratch_shapes=[
                vm((rows, 2, n // 2, c), F32), vm((rows, n, c), F32), vm((rows, c, n), BF), vm((rows, c, n), BF),
                vm((npair, 2, c, n), BF), vm((npair, 2, n, c), BF), vm((rows, c, n), F32), vm((rows, c, n), BF),
                vm((heads, rows, n), BF), vm((heads, n, n), BF), vm((2, n, heads * n), F32), vm((2, n // 2, rows, c), BF),
                vm((rows, n, c), BF), vm((npair, 2 * c, 2 * n), BF), vm((rows, n, c), BF), vm((npair, c, 2 * n), F32),
                vm((npair, c, 2 * n), BF), vm((heads, rows, n), BF), vm((heads, n, n), BF), vm((n, heads * n), F32),
                vm((rows, n, c), BF), vm((n, rows, c), BF), vm((2, n, heads * n), F32), vm((2, n, heads * n), F32),
                vm((2, c, 2 * n), F32), vm((2, c, 2 * n), BF), vm((c, 2 * n), BF), vm((2, 2, c, n), BF),
                *[vm(w.shape, BF) for w in weights],
                vm(wqs.shape[::-1], BF), vm(wqe.shape[::-1], BF), vm(woe.shape[::-1], BF),
                vm(w1.shape[::-1], BF), vm(w2.shape[::-1], BF),
                vm((heads * GROUP, TILE * c), BF), vm((heads * GROUP, TILE * c), BF),
                dma((4,)), dma((5,)), dma, dma((2,)), dma, dma((4,)), dma, dma, dma, dma((3,)), dma, dma((4,)),
            ],
            compiler_params=pltpu.CompilerParams(collective_id=0, has_side_effects=True, vmem_limit_bytes=36 * 2 ** 20),
            name="pair_block",
        )(*[pltpu.with_memory_space_constraint(a, pltpu.HBM) for a in args])

    return jax.shard_map(local_fn, mesh=mesh, in_specs=(row_spec,) + (P(),) * TILE, out_specs=row_spec, check_vma=False)
```

```python
import functools

import jax
import jax.numpy as jnp
from jax import lax
from jax.experimental import pallas as pl
from jax.experimental.pallas import tpu as pltpu
from jax.sharding import PartitionSpec as P

MESH = pl.DeviceIdType.MESH
EPS = 1e-5
TILE = 8
GROUP = 16
LOG2E = 1.4426950408889634
BF = jnp.bfloat16
F32 = jnp.float32


def dot(a, b):
    return jnp.dot(a, b, preferred_element_type=F32)


def dot_tn(a, b):
    return lax.dot_general(a, b, (((0,), (0,)), ((), ())), preferred_element_type=F32)


def norm_t(xt):
    mean = jnp.sum(xt, axis=0, keepdims=True) * (1.0 / xt.shape[0])
    cen = xt - mean
    var = jnp.sum(cen * cen, axis=0, keepdims=True) * (1.0 / xt.shape[0])
    return (cen * lax.rsqrt(var + EPS)).astype(BF)


def sigmoid(x):
    return 0.5 * jnp.tanh(0.5 * x) + 0.5


def block_diag(qt, pair, heads):
    hd, n = qt.shape
    d = hd // heads
    cols = []
    for h in (2 * pair, 2 * pair + 1):
        parts = []
        if h:
            parts.append(jnp.zeros((h * d, n), BF))
        parts.append(qt[h * d:(h + 1) * d])
        if h < heads - 1:
            parts.append(jnp.zeros(((heads - 1 - h) * d, n), BF))
        cols.append(jnp.concatenate(parts, axis=0))
    return jnp.concatenate(cols, axis=1)


def stage_scores(kn, qv, s, p, heads):
    c, n = kn.shape[1:]
    for r in range(2):
        keys = kn[2 * p + r]
        qt = qv[p, :c, r * n:(r + 1) * n]
        for pair in range(heads // 2):
            s[r, :, 2 * pair * n:(2 * pair + 2) * n] = dot(keys, block_diag(qt, pair, heads))


def stage_mix(s, biast, qv, g, og, p, heads):
    n = s.shape[1]
    c = qv.shape[1] // 2
    d = c // heads
    scale = LOG2E * d ** -0.5
    for r in range(2):
        for pair in range(heads // 2):
            probs = []
            for h in (2 * pair, 2 * pair + 1):
                t = s[r, :, h * n:(h + 1) * n] * scale + biast[:, h * n:(h + 1) * n]
                e = jnp.exp2(t - jnp.max(t, axis=0, keepdims=True))
                probs.append((e * (1.0 / jnp.sum(e, axis=0, keepdims=True))).astype(BF))
            rows = slice(c + 2 * pair * d, c + (2 * pair + 2) * d)
            o = dot(qv[p, rows, r * n:(r + 1) * n], jnp.concatenate(probs, axis=1))
            for i in range(2):
                h = 2 * pair + i
                out = o[i * d:(i + 1) * d, i * n:(i + 1) * n] * g[p, h * d:(h + 1) * d, r * n:(r + 1) * n]
                og[p, h * d:(h + 1) * d, r * n:(r + 1) * n] = out.astype(BF)


def norm_blocks(src, ut, b0, count):
    for r in range(count):
        ut[b0 + r] = norm_t(src[b0 + r])


def head_rows(wb):
    heads, c = wb.shape
    rep = jnp.broadcast_to(wb.astype(F32)[:, None, :], (heads, GROUP, c)).reshape(heads * GROUP, c)
    row = lax.broadcasted_iota(jnp.int32, rep.shape, 0) % GROUP // 2
    return jnp.concatenate([jnp.where(row == j, rep, 0.0) for j in range(TILE)], axis=1).astype(BF)


def bias_rows(w8, ub, dst, i, swap=None):
    heads, rows, n = dst.shape
    c = ub.shape[1]
    half = n // 2
    r0, r1 = [dot(w8, ub[s * rows // 2 + TILE * i:s * rows // 2 + TILE * i + TILE].reshape(TILE * c, n)) for s in range(2)]
    first, second = [(r0[:, lane:lane + half], r1[:, lane:lane + half]) for lane in (0, half)]
    even = lax.broadcasted_iota(jnp.int32, r0.shape, 0) % 2 == 0
    res = jnp.where(even, jnp.concatenate(first, axis=1), jnp.concatenate(second, axis=1))
    if swap is not None:
        res = jnp.where(swap, jnp.concatenate([res[:, half:], res[:, :half]], axis=1), res)
    dst[:, GROUP * i:GROUP * i + GROUP] = res.reshape(heads, GROUP, n).astype(BF)


def low_half(shape):
    return lax.broadcasted_iota(jnp.int32, shape, 1) < shape[1] // 2


def pair_project(wt, ub, qb, kt_ref, vst, g, p, npair, heads):
    own, oth = ub[p], ub[npair + p]
    c, n = own.shape
    d, half = c // heads, n // 2
    u = jnp.concatenate([own, oth], axis=1)
    q = dot(wt[0:c], u).astype(BF)
    qb[p] = q[:, :n]
    qb[npair + p] = q[:, n:]
    u_row = jnp.concatenate([own[:, :half], oth[:, :half], own[:, half:], oth[:, half:]], axis=1)
    k = dot(wt[c:2 * c], u_row).astype(BF)
    v = dot(wt[2 * c:3 * c], u_row).astype(BF)
    for h in range(heads):
        for i in range(2):
            rows = pl.ds((h % 2) * 2 * d + i * d, d)
            kt_ref[h // 2, rows] = k[h * d:(h + 1) * d, i * n:(i + 1) * n]
            vst[p, h // 2, rows] = v[h * d:(h + 1) * d, i * n:(i + 1) * n]
    gate = sigmoid(dot(wt[3 * c:], u))
    g[p] = gate[:, :n]
    g[npair + p] = gate[:, n:]


def block_scores(kn, qb, s, slot, b, p, heads):
    c, n = qb.shape[1:]
    d = c // heads
    low = low_half((d, n))
    zero = jnp.zeros((d, n), BF)
    for pair in range(heads // 2):
        rows = []
        for i in range(2):
            q = qb[b, (2 * pair + i) * d:(2 * pair + i + 1) * d]
            for part in (jnp.where(low, q, zero), jnp.where(low, zero, q)):
                rows.append(jnp.concatenate([part, zero] if i == 0 else [zero, part], axis=1))
        s[slot, :, 2 * pair * n:(2 * pair + 2) * n] = dot(kn[p, pair], jnp.concatenate(rows, axis=0))


def softmax_t(t):
    e = jnp.exp2(t - jnp.max(t, axis=0, keepdims=True))
    return (e * (1.0 / jnp.sum(e, axis=0, keepdims=True))).astype(BF)


def block_mix(s, slot, biast, side, vst, g, og, b, p, heads):
    c, n = og.shape[1:]
    d = c // heads
    low = low_half((d, n))
    for h in range(heads):
        t = s[slot, :, h * n:(h + 1) * n] * (LOG2E * d ** -0.5) + biast[side, :, h * n:(h + 1) * n]
        o = dot(vst[p, h // 2, (h % 2) * 2 * d:(h % 2 + 1) * 2 * d], softmax_t(t))
        og[b, h * d:(h + 1) * d] = (jnp.where(low, o[:d], o[d:]) * g[b, h * d:(h + 1) * d]).astype(BF)


def project(wt, u, n, qv_ref, kt_ref, g_ref, p):
    c = u.shape[0]
    qv_ref[p, :c] = dot(wt[0:c], u).astype(BF)
    kt_ref[...] = dot(wt[c:2 * c], u).astype(BF)
    qv_ref[p, c:] = dot(wt[2 * c:3 * c], u).astype(BF)
    g_ref[p] = sigmoid(dot(wt[3 * c:], u))


def turn_keys(kt_ref, kn_ref, p):
    n = kn_ref.shape[1]
    kn_ref[2 * p] = kt_ref[:, :n].T
    kn_ref[2 * p + 1] = kt_ref[:, n:].T


def kernel(z_hbm, wqs_h, wbs_h, wos_h, wqe_h, wbe_h, woe_h, w1_h, w2_h, y,
           zs4, z1, ub, qb, vst, knp, gb, ogb, bsend, ball, biasp, hsend,
           hcol, qv, kn, g, og, besend, beall, biast, dsend, drecv, s, s_next, eb, u2, kt, ktp,
           wqs, wbs, wos, wqe, wbe, woe, w1, w2, wqst, wqet, woet, w1t, w2t, wbs8, wbe8,
           zsem, wsem, bs_s, bs_r, h_s, h_r, o_s, o_r, be_s, be_r, d_s, d_r):
    rows, n, c = y.shape
    npair = rows // 2
    half = n // 2
    heads = wbs.shape[0]
    dp, sp = lax.axis_index("dp"), lax.axis_index("sp")
    x, core = sp // 2, sp % 2
    peers = [2 * (1 - x) + core, 2 * (1 - x) + 1 - core, 2 * x + 1 - core]
    mine = pl.multiple_of(sp * rows, rows)

    def zcopy(ci):
        q, side = ci // 2, ci % 2
        return pltpu.make_async_copy(z_hbm.at[pl.ds(4 * q, 4), :, (x + side) % 2],
                                     zs4.at[pl.ds(side * npair + 4 * q, 4)], zsem.at[q])

    def wcopy(i):
        src = (wbs_h, wqs_h, wqe_h, woe_h, w1_h, w2_h, wbe_h, wos_h)[i]
        return pltpu.make_async_copy(src, (wbs, wqs, wqe, woe, w1, w2, wbe, wos)[i], wsem.at[(0, 1, 2, 2, 2, 2, 3, 4)[i]])

    wcopy(0).start()
    wcopy(6).start()
    for ci in range(TILE):
        zcopy(ci).start()
    for i in (1, 7, 2, 3, 4, 5):
        wcopy(i).start()
    bar = pltpu.get_barrier_semaphore()
    for t in peers:
        pl.semaphore_signal(bar, inc=1, device_id=(dp, t), device_id_type=MESH)

    def remote(src, dst, ssem, rsem, t):
        return pltpu.make_async_remote_copy(src, dst, ssem, rsem, device_id=(dp, t), device_id_type=MESH)

    def sent(ref, sem):
        remote(ref, ref, sem, sem, peers[0]).wait_send()

    def arrived(ref, sem):
        remote(ref, ref, sem, sem, peers[0]).wait_recv()

    wcopy(0).wait()
    wcopy(6).wait()
    wbs8[...] = head_rows(wbs[...])
    wbe8[...] = head_rows(wbe[...])

    def chunk_base(ci):
        return ci % 2 * npair + ci // 2 * 4

    def turn_chunks(q):
        arrived(zs4.at[0:TILE], zsem.at[q])
        for side in range(2):
            b0 = chunk_base(2 * q + side)
            for r in range(4):
                y[b0 + r] = zs4[b0 + r].reshape(n, c).T

    def norm_chunks(q):
        for side in range(2):
            norm_blocks(y, ub, chunk_base(2 * q + side), 4)

    turn_chunks(0)
    for q in range(1, 4):
        turn_chunks(q)
        norm_chunks(q - 1)
    norm_chunks(3)
    bias_rows(wbs8[...], ub, bsend, 0)
    for side in range(2):
        norm_blocks(y, ub, chunk_base(6 + side), 4)
    for i in range(1, rows // GROUP):
        bias_rows(wbs8[...], ub, bsend, i)
    ball[:, pl.ds(pl.multiple_of(core * rows, rows), rows)] = bsend[...]
    pl.semaphore_wait(bar, 3)

    def bias_copy(k, t, owner):
        return remote(bsend, ball.at[:, pl.ds(pl.multiple_of((half if k < 2 else 0) + owner % 2 * rows, rows), rows)],
                      bs_s, bs_r.at[k // 2], t)

    def end_bias_part(owner, i):
        return beall.at[:, pl.ds(pl.multiple_of(owner * rows + GROUP * i, GROUP), GROUP)]

    def end_bias_send(i):
        part = besend.at[:, GROUP * i:GROUP * i + GROUP]
        for k in ((0, 2), range(3))[i]:
            remote(part, end_bias_part(sp, i), be_s, be_r.at[2 if k == 2 else i], peers[k]).start()

    def end_bias_forward():
        part = end_bias_part(peers[0], 0)
        arrived(part, be_r.at[0])
        remote(part, part, be_s, be_r.at[2], peers[2]).start()

    for k in (2, 0, 1):
        bias_copy(k, peers[k], sp).start()

    wcopy(1).wait()
    wcopy(7).wait()
    wqst[...] = wqs[...].T
    def start_project(*pairs):
        for p in pairs:
            pair_project(wqst, ub, qb, ktp.at[p % 2], vst, gb, p, npair, heads)
        for p in pairs:
            for pair in range(heads // 2):
                knp[p, pair] = ktp[p % 2, pair].T

    def start_bias(side):
        for h in range(heads):
            rws = ball[h, side * half:(side + 1) * half]
            tr = jnp.concatenate([rws, rws], axis=0).T.astype(F32) * LOG2E
            if side:
                tr = jnp.concatenate([tr[half:], tr[:half]], axis=0)
            biasp[side, :, h * n:(h + 1) * n] = tr

    def start_out(b):
        upd = dot_tn(jnp.concatenate([ogb[b], ogb[b + 1]], axis=1), wos[...])
        z1[b] = zs4[b].reshape(n, c) + upd[:n]
        z1[b + 1] = zs4[b + 1].reshape(n, c) + upd[n:]
    def start_norm(b):
        for r in range(2):
            ub[b + r] = norm_t(z1[b + r].astype(BF).astype(F32).T)

    def start_mix(b, buf=s):
        for r in range(2):
            block_mix(buf, r, biasp, b // npair, vst, gb, ogb, b + r, b % npair + r, heads)

    def start_scores(b, buf=s):
        for r in range(2):
            block_scores(knp, qb, buf, r, b + r, b % npair + r, heads)

    def start_step(t, _):
        for by, stage in ((3, start_norm), (2, start_out), (1, start_mix), (0, start_scores)):
            if not isinstance(t, int) or 0 <= t - by < npair:
                stage(2 * (t - by))
        return _

    chunks = 4
    cols = rows // chunks
    groups = [(0, TILE), (TILE, TILE), (GROUP, GROUP)]
    near = [(0, GROUP), (GROUP, GROUP)]

    def h_copy(gi, ch, k, t, owner):
        r0, size = groups[gi]
        return remote(hsend.at[0, pl.ds(t % 2 * rows + ch * cols, cols), r0:r0 + size],
                      hcol.at[pl.ds(ch * cols, cols), pl.ds(pl.multiple_of(owner * rows + r0, TILE), size)],
                      h_s, h_r.at[ch], t)

    def near_copy(gi, owner):
        r0, size = near[gi]
        return remote(hsend.at[1, pl.ds(pl.multiple_of((1 - core) * rows, rows), rows), r0:r0 + size],
                      hcol.at[:, pl.ds(pl.multiple_of(owner * rows + r0, TILE), size)],
                      o_s, o_r, peers[2])

    def shuffle_rows(side, r0, size):
        def body(jb, _):
            j0 = pl.multiple_of(jb * TILE, TILE)
            parts = []
            for row in range(r0, r0 + size):
                b = side * npair + row // 2
                parts.append(z1[b:b + 1, pl.ds(row % 2 * half + j0, TILE)])
            blk = jnp.swapaxes(jnp.concatenate(parts, axis=0), 0, 1)
            hsend[side, pl.ds(j0, TILE), r0:r0 + size] = blk.astype(BF)
            return _
        lax.fori_loop(0, half // TILE, body, 0, unroll=8)

    def send_h(gi, chs):
        for ch in chs:
            for k in range(2):
                h_copy(gi, ch, k, peers[k], sp).start()

    start_project(0, 1)
    start_project(2, 3)
    start_scores(0)
    start_scores(2, s_next)
    arrived(ball.at[:, 0:rows], bs_r.at[1])
    start_bias(0)
    start_mix(0)
    start_mix(2, s_next)
    start_out(0)
    start_out(2)
    shuffle_rows(0, 0, TILE)
    send_h(0, range(chunks))
    start_project(4, 5)
    start_scores(4)
    start_project(6, 7)
    start_norm(0)
    start_mix(4)
    start_scores(6)
    start_project(TILE, 9)
    start_norm(2)
    start_out(4)
    start_mix(6)
    start_scores(TILE)
    start_project(10, 11)
    start_step(5, 0)
    shuffle_rows(0, TILE, TILE)
    send_h(1, range(chunks))
    for t in (6, 7):
        start_project(2 * t, 2 * t + 1)
        start_step(t, 0)
    start_step(TILE, 0)
    arrived(ball.at[:, 0:2 * rows], bs_r.at[0])
    start_bias(1)
    start_step(9, 0)
    shuffle_rows(0, GROUP, GROUP)
    send_h(2, [0])
    lax.fori_loop(10, 14, start_step, 0, unroll=4)
    shuffle_rows(1, 0, GROUP)
    near_copy(0, sp).start()
    start_step(14, 0)
    bias_rows(wbe8[...], ub, besend, 0, x == 1)
    end_bias_send(0)
    for t in range(15, npair + 3):
        start_step(t, 0)
    bias_rows(wbe8[...], ub, besend, 1, x == 1)
    end_bias_send(1)
    beall[:, pl.ds(mine, rows)] = besend[...]
    shuffle_rows(1, GROUP, GROUP)
    near_copy(1, sp).start()
    send_h(2, [1])
    hcol[:, pl.ds(mine, rows)] = hsend[1, pl.ds(pl.multiple_of(core * rows, rows), rows)]
    arrived(hcol.at[0:13], wsem.at[2])
    wqet[...] = wqe[...].T
    woet[...] = woe[...].T
    w1t[...] = w1[...].T
    w2t[...] = w2[...].T
    sent(ball.at[:, 0:3 * rows], bs_s)

    def end_delta(p):
        hid = jnp.maximum(dot(w1t[...], u2[p % 2]), 0.0).astype(BF)
        delta = (eb[p % 2] + dot(w2t[...], hid)).astype(BF)
        dsend[2 * p] = delta[:, :n].T
        dsend[2 * p + 1] = delta[:, n:].T

    def columns(p):
        return jnp.concatenate([hcol[2 * p].astype(F32).T, hcol[2 * p + 1].astype(F32).T], axis=1)

    def end_out(p):
        e = dot(woet[...], og[p])
        eb[p % 2] = e
        u2[p % 2] = norm_t(columns(p) + e)

    def end_mix(p):
        stage_mix(s, biast, qv, g, og, p, heads)

    def end_scores(p):
        turn_keys(kt, kn, p)
        stage_scores(kn, qv, s, p, heads)

    def end_project(p):
        project(wqet, norm_t(columns(p)), n, qv, kt, g, p)

    def end_step(t):
        for by, stage in ((4, end_delta), (3, end_out), (2, end_mix), (1, end_scores), (0, end_project)):
            if not isinstance(t, int) or 0 <= t - by < npair:
                stage(t - by)

    def d_copy(q, count, k, t, first_col):
        return remote(dsend.at[pl.ds(2 * q, 2 * count), pl.ds(pl.multiple_of(t * rows, rows), rows)],
                      drecv.at[pl.ds(first_col + 2 * q, 2 * count)], d_s, d_r.at[chunks if k == 2 else q // (npair // chunks)], t)

    my_cols = pl.multiple_of((2 * (1 - x) + core) * rows, rows)

    def send_d(q, count):
        for k, t in enumerate(peers):
            d_copy(q, count, k, t, my_cols).start()

    def wait_h(ch):
        arrived(hcol.at[pl.ds(ch * cols, cols), 0:2 * rows], h_r.at[ch])

    arrived(hcol.at[:, 0:rows], o_r)
    send_h(2, [2])
    end_bias_forward()
    send_h(2, [3])
    wait_h(0)
    end_step(0)
    end_step(1)
    arrived(beall.at[:, 0:rows], be_r.at[1])
    arrived(beall.at[:, 0:rows + GROUP], be_r.at[2])
    for h in range(heads):
        biast[:, h * n:(h + 1) * n] = beall[h].astype(F32) * LOG2E
    end_step(2)
    end_step(3)

    def segment(i, _):
        @pl.when(i % 2 == 0)
        def _wait():
            wait_h(i // 2)
        end_step(2 * i)
        end_step(2 * i + 1)
        send_d(2 * i - 4, 2)
        return _
    lax.fori_loop(2, npair // 2, segment, 0)
    for t in range(npair, npair + 4):
        end_step(t)
        send_d(t - 4, 1)
    drecv[pl.ds(my_cols, rows)] = dsend[:, pl.ds(mine, rows)]

    def final_block(side, owner_core, first_col, ch):
        j0 = pl.multiple_of(first_col + ch * cols, TILE)
        jj = owner_core * rows + ch * cols
        for gi in range(rows // GROUP):
            blk = jnp.swapaxes(drecv[pl.ds(j0, TILE), gi * GROUP:(gi + 1) * GROUP].astype(F32), 0, 1)
            for r in range(GROUP):
                row = GROUP * gi + r
                part = z1[side * npair + row // 2, pl.ds(pl.multiple_of(row % 2 * half + jj, TILE), TILE)]
                y[row, pl.ds(j0, TILE)] = part + blk[r]

    for ch in range(chunks):
        final_block(1, core, my_cols, ch)
    arrived(drecv.at[0:rows], d_r.at[chunks])
    for ch in range(chunks):
        final_block(1, 1 - core, pl.multiple_of((2 * (1 - x) + 1 - core) * rows, rows), ch)
    for ch in range(chunks):
        arrived(drecv.at[0:2 * cols], d_r.at[ch])
        for t in peers[:2]:
            final_block(0, t % 2, pl.multiple_of((2 * x + t % 2) * rows, rows), ch)
    sent(hsend.at[0], h_s)
    sent(ball.at[:, 0:3 * rows], be_s)
    sent(hcol.at[:, 0:rows], o_s)
    sent(dsend.at[:, 0:3 * rows], d_s)


def solution(mesh):
    row_spec = P(('dp', 'sp'), None, None)
    sp = mesh.shape['sp']

    def local_fn(pair_loc, wqs, wbs, wos, wqe, wbe, woe, w1, w2):
        rows, n, c = pair_loc.shape
        heads = wbs.shape[0]
        dma = pltpu.SemaphoreType.DMA
        vm = pltpu.VMEM
        weights = (wqs, wbs, wos, wqe, wbe, woe, w1, w2)
        npair = rows // 2
        args = (pair_loc.reshape(npair, 2, 2, n // 2, c),) + weights
        return pl.pallas_call(
            kernel,
            out_shape=vm(pair_loc.shape, F32),
            in_specs=[pl.BlockSpec(memory_space=pltpu.HBM)] * 9,
            out_specs=pl.BlockSpec(memory_space=vm),
            scratch_shapes=[
                vm((rows, 2, n // 2, c), F32), vm((rows, n, c), F32), vm((rows, c, n), BF), vm((rows, c, n), BF),
                vm((npair, 2, c, n), BF), vm((npair, 2, n, c), BF), vm((rows, c, n), F32), vm((rows, c, n), BF),
                vm((heads, rows, n), BF), vm((heads, n, n), BF), vm((2, n, heads * n), F32), vm((2, n // 2, rows, c), BF),
                vm((rows, n, c), BF), vm((npair, 2 * c, 2 * n), BF), vm((rows, n, c), BF), vm((npair, c, 2 * n), F32),
                vm((npair, c, 2 * n), BF), vm((heads, rows, n), BF), vm((heads, n, n), BF), vm((n, heads * n), F32),
                vm((rows, n, c), BF), vm((n, rows, c), BF), vm((2, n, heads * n), F32), vm((2, n, heads * n), F32),
                vm((2, c, 2 * n), F32), vm((2, c, 2 * n), BF), vm((c, 2 * n), BF), vm((2, 2, c, n), BF),
                *[vm(w.shape, BF) for w in weights],
                vm(wqs.shape[::-1], BF), vm(wqe.shape[::-1], BF), vm(woe.shape[::-1], BF),
                vm(w1.shape[::-1], BF), vm(w2.shape[::-1], BF),
                vm((heads * GROUP, TILE * c), BF), vm((heads * GROUP, TILE * c), BF),
                dma((4,)), dma((5,)), dma, dma((2,)), dma, dma((4,)), dma, dma, dma, dma((3,)), dma, dma((5,)),
            ],
            compiler_params=pltpu.CompilerParams(collective_id=0, has_side_effects=True, vmem_limit_bytes=36 * 2 ** 20),
            name="pair_block",
        )(*[pltpu.with_memory_space_constraint(a, pltpu.HBM) for a in args])

    return jax.shard_map(local_fn, mesh=mesh, in_specs=(row_spec,) + (P(),) * TILE, out_specs=row_spec, check_vma=False)
```

```python
import functools

import jax
import jax.numpy as jnp
from jax import lax
from jax.experimental import pallas as pl
from jax.experimental.pallas import tpu as pltpu
from jax.sharding import PartitionSpec as P

MESH = pl.DeviceIdType.MESH
EPS = 1e-5
TILE = 8
GROUP = 16
LOG2E = 1.4426950408889634
BF = jnp.bfloat16
F32 = jnp.float32


def dot(a, b):
    return jnp.dot(a, b, preferred_element_type=F32)


def dot_tn(a, b):
    return lax.dot_general(a, b, (((0,), (0,)), ((), ())), preferred_element_type=F32)


def norm_t(xt):
    mean = jnp.sum(xt, axis=0, keepdims=True) * (1.0 / xt.shape[0])
    cen = xt - mean
    var = jnp.sum(cen * cen, axis=0, keepdims=True) * (1.0 / xt.shape[0])
    return (cen * lax.rsqrt(var + EPS)).astype(BF)


def sigmoid(x):
    return 0.5 * jnp.tanh(0.5 * x) + 0.5


def block_diag(qt, pair, heads):
    hd, n = qt.shape
    d = hd // heads
    cols = []
    for h in (2 * pair, 2 * pair + 1):
        parts = []
        if h:
            parts.append(jnp.zeros((h * d, n), BF))
        parts.append(qt[h * d:(h + 1) * d])
        if h < heads - 1:
            parts.append(jnp.zeros(((heads - 1 - h) * d, n), BF))
        cols.append(jnp.concatenate(parts, axis=0))
    return jnp.concatenate(cols, axis=1)


def stage_scores(kn, qv, s, p, heads):
    c, n = kn.shape[1:]
    for r in range(2):
        keys = kn[2 * p + r]
        qt = qv[p, :c, r * n:(r + 1) * n]
        for pair in range(heads // 2):
            s[r, :, 2 * pair * n:(2 * pair + 2) * n] = dot(keys, block_diag(qt, pair, heads))


def stage_mix(s, biast, qv, g, og, p, heads):
    n = s.shape[1]
    c = qv.shape[1] // 2
    d = c // heads
    scale = LOG2E * d ** -0.5
    for r in range(2):
        for pair in range(heads // 2):
            probs = []
            for h in (2 * pair, 2 * pair + 1):
                t = s[r, :, h * n:(h + 1) * n] * scale + biast[:, h * n:(h + 1) * n]
                e = jnp.exp2(t - jnp.max(t, axis=0, keepdims=True))
                probs.append((e * (1.0 / jnp.sum(e, axis=0, keepdims=True))).astype(BF))
            rows = slice(c + 2 * pair * d, c + (2 * pair + 2) * d)
            o = dot(qv[p, rows, r * n:(r + 1) * n], jnp.concatenate(probs, axis=1))
            for i in range(2):
                h = 2 * pair + i
                out = o[i * d:(i + 1) * d, i * n:(i + 1) * n] * g[p, h * d:(h + 1) * d, r * n:(r + 1) * n]
                og[p, h * d:(h + 1) * d, r * n:(r + 1) * n] = out.astype(BF)


def norm_blocks(src, ut, b0, count):
    for r in range(count):
        ut[b0 + r] = norm_t(src[b0 + r])


def head_rows(wb):
    heads, c = wb.shape
    rep = jnp.broadcast_to(wb.astype(F32)[:, None, :], (heads, GROUP, c)).reshape(heads * GROUP, c)
    row = lax.broadcasted_iota(jnp.int32, rep.shape, 0) % GROUP // 2
    return jnp.concatenate([jnp.where(row == j, rep, 0.0) for j in range(TILE)], axis=1).astype(BF)


def bias_rows(w8, ub, dst, i, swap=None):
    heads, rows, n = dst.shape
    c = ub.shape[1]
    half = n // 2
    r0, r1 = [dot(w8, ub[s * rows // 2 + TILE * i:s * rows // 2 + TILE * i + TILE].reshape(TILE * c, n)) for s in range(2)]
    first, second = [(r0[:, lane:lane + half], r1[:, lane:lane + half]) for lane in (0, half)]
    even = lax.broadcasted_iota(jnp.int32, r0.shape, 0) % 2 == 0
    res = jnp.where(even, jnp.concatenate(first, axis=1), jnp.concatenate(second, axis=1))
    if swap is not None:
        res = jnp.where(swap, jnp.concatenate([res[:, half:], res[:, :half]], axis=1), res)
    dst[:, GROUP * i:GROUP * i + GROUP] = res.reshape(heads, GROUP, n).astype(BF)


def low_half(shape):
    return lax.broadcasted_iota(jnp.int32, shape, 1) < shape[1] // 2


def pair_project(wt, ub, qb, kt_ref, vst, g, p, npair, heads):
    own, oth = ub[p], ub[npair + p]
    c, n = own.shape
    d, half = c // heads, n // 2
    u = jnp.concatenate([own, oth], axis=1)
    q = dot(wt[0:c], u).astype(BF)
    qb[p] = q[:, :n]
    qb[npair + p] = q[:, n:]
    u_row = jnp.concatenate([own[:, :half], oth[:, :half], own[:, half:], oth[:, half:]], axis=1)
    k = dot(wt[c:2 * c], u_row).astype(BF)
    v = dot(wt[2 * c:3 * c], u_row).astype(BF)
    for h in range(heads):
        for i in range(2):
            rows = pl.ds((h % 2) * 2 * d + i * d, d)
            kt_ref[h // 2, rows] = k[h * d:(h + 1) * d, i * n:(i + 1) * n]
            vst[p, h // 2, rows] = v[h * d:(h + 1) * d, i * n:(i + 1) * n]
    gate = sigmoid(dot(wt[3 * c:], u))
    g[p] = gate[:, :n]
    g[npair + p] = gate[:, n:]


def block_scores(kn, qb, s, slot, b, p, heads):
    c, n = qb.shape[1:]
    d = c // heads
    low = low_half((d, n))
    zero = jnp.zeros((d, n), BF)
    for pair in range(heads // 2):
        rows = []
        for i in range(2):
            q = qb[b, (2 * pair + i) * d:(2 * pair + i + 1) * d]
            for part in (jnp.where(low, q, zero), jnp.where(low, zero, q)):
                rows.append(jnp.concatenate([part, zero] if i == 0 else [zero, part], axis=1))
        s[slot, :, 2 * pair * n:(2 * pair + 2) * n] = dot(kn[p, pair], jnp.concatenate(rows, axis=0))


def softmax_t(t):
    e = jnp.exp2(t - jnp.max(t, axis=0, keepdims=True))
    return (e * (1.0 / jnp.sum(e, axis=0, keepdims=True))).astype(BF)


def block_mix(s, slot, biast, side, vst, g, og, b, p, heads):
    c, n = og.shape[1:]
    d = c // heads
    low = low_half((d, n))
    for h in range(heads):
        t = s[slot, :, h * n:(h + 1) * n] * (LOG2E * d ** -0.5) + biast[side, :, h * n:(h + 1) * n]
        o = dot(vst[p, h // 2, (h % 2) * 2 * d:(h % 2 + 1) * 2 * d], softmax_t(t))
        og[b, h * d:(h + 1) * d] = (jnp.where(low, o[:d], o[d:]) * g[b, h * d:(h + 1) * d]).astype(BF)


def project(wt, u, n, qv_ref, kt_ref, g_ref, p):
    c = u.shape[0]
    qv_ref[p, :c] = dot(wt[0:c], u).astype(BF)
    kt_ref[...] = dot(wt[c:2 * c], u).astype(BF)
    qv_ref[p, c:] = dot(wt[2 * c:3 * c], u).astype(BF)
    g_ref[p] = sigmoid(dot(wt[3 * c:], u))


def turn_keys(kt_ref, kn_ref, p):
    n = kn_ref.shape[1]
    kn_ref[2 * p] = kt_ref[:, :n].T
    kn_ref[2 * p + 1] = kt_ref[:, n:].T


def kernel(z_hbm, wqs_h, wbs_h, wos_h, wqe_h, wbe_h, woe_h, w1_h, w2_h, y,
           zs4, z1, ub, qb, vst, knp, gb, ogb, bsend, ball, biasp, hsend,
           hcol, qv, kn, g, og, besend, beall, biast, dsend, drecv, s, s_next, eb, u2, kt, ktp,
           wqs, wbs, wos, wqe, wbe, woe, w1, w2, wqst, wqet, woet, w1t, w2t, wbs8, wbe8,
           zsem, wsem, out_s, bs_r, h_r, o_r, be_r, d_r):
    rows, n, c = y.shape
    npair = rows // 2
    half = n // 2
    heads = wbs.shape[0]
    dp, sp = lax.axis_index("dp"), lax.axis_index("sp")
    x, core = sp // 2, sp % 2
    peers = [2 * (1 - x) + core, 2 * (1 - x) + 1 - core, 2 * x + 1 - core]
    mine = pl.multiple_of(sp * rows, rows)

    def zcopy(ci):
        q, side = ci // 2, ci % 2
        return pltpu.make_async_copy(z_hbm.at[pl.ds(4 * q, 4), :, (x + side) % 2],
                                     zs4.at[pl.ds(side * npair + 4 * q, 4)], zsem.at[q])

    def wcopy(i):
        src = (wbs_h, wqs_h, wqe_h, woe_h, w1_h, w2_h, wbe_h, wos_h)[i]
        return pltpu.make_async_copy(src, (wbs, wqs, wqe, woe, w1, w2, wbe, wos)[i], wsem.at[(0, 1, 2, 2, 2, 2, 3, 4)[i]])

    wcopy(0).start()
    wcopy(6).start()
    for ci in range(TILE):
        zcopy(ci).start()
    for i in (1, 7, 2, 3, 4, 5):
        wcopy(i).start()
    bar = pltpu.get_barrier_semaphore()
    for t in peers:
        pl.semaphore_signal(bar, inc=1, device_id=(dp, t), device_id_type=MESH)

    def remote(src, dst, ssem, rsem, t):
        return pltpu.make_async_remote_copy(src, dst, ssem, rsem, device_id=(dp, t), device_id_type=MESH)

    def sent(ref, sem):
        remote(ref, ref, sem, sem, peers[0]).wait_send()

    def arrived(ref, sem):
        remote(ref, ref, sem, sem, peers[0]).wait_recv()

    wcopy(0).wait()
    wcopy(6).wait()
    wbs8[...] = head_rows(wbs[...])
    wbe8[...] = head_rows(wbe[...])

    def chunk_base(ci):
        return ci % 2 * npair + ci // 2 * 4

    def turn_chunks(q):
        arrived(zs4.at[0:TILE], zsem.at[q])
        for side in range(2):
            b0 = chunk_base(2 * q + side)
            for r in range(4):
                y[b0 + r] = zs4[b0 + r].reshape(n, c).T

    def norm_chunks(q):
        for side in range(2):
            norm_blocks(y, ub, chunk_base(2 * q + side), 4)

    turn_chunks(0)
    for q in range(1, 4):
        turn_chunks(q)
        norm_chunks(q - 1)
    norm_chunks(3)
    bias_rows(wbs8[...], ub, bsend, 0)
    for side in range(2):
        norm_blocks(y, ub, chunk_base(6 + side), 4)
    for i in range(1, rows // GROUP):
        bias_rows(wbs8[...], ub, bsend, i)
    ball[:, pl.ds(pl.multiple_of(core * rows, rows), rows)] = bsend[...]
    pl.semaphore_wait(bar, 3)

    def bias_copy(k, t, owner):
        return remote(bsend, ball.at[:, pl.ds(pl.multiple_of((half if k < 2 else 0) + owner % 2 * rows, rows), rows)],
                      out_s, bs_r.at[k // 2], t)

    def end_bias_part(owner, i):
        return beall.at[:, pl.ds(pl.multiple_of(owner * rows + GROUP * i, GROUP), GROUP)]

    def end_bias_send(i):
        part = besend.at[:, GROUP * i:GROUP * i + GROUP]
        for k in ((0, 2), range(3))[i]:
            remote(part, end_bias_part(sp, i), out_s, be_r.at[2 if k == 2 else i], peers[k]).start()

    def end_bias_forward():
        part = end_bias_part(peers[0], 0)
        arrived(part, be_r.at[0])
        remote(part, part, out_s, be_r.at[2], peers[2]).start()

    for k in (2, 0, 1):
        bias_copy(k, peers[k], sp).start()

    wcopy(1).wait()
    wcopy(7).wait()
    wqst[...] = wqs[...].T
    def start_project(*pairs):
        for p in pairs:
            pair_project(wqst, ub, qb, ktp.at[p % 2], vst, gb, p, npair, heads)
        for p in pairs:
            for pair in range(heads // 2):
                knp[p, pair] = ktp[p % 2, pair].T

    def start_bias(side):
        for h in range(heads):
            rws = ball[h, side * half:(side + 1) * half]
            tr = jnp.concatenate([rws, rws], axis=0).T.astype(F32) * LOG2E
            if side:
                tr = jnp.concatenate([tr[half:], tr[:half]], axis=0)
            biasp[side, :, h * n:(h + 1) * n] = tr

    def start_out(b):
        upd = dot_tn(jnp.concatenate([ogb[b], ogb[b + 1]], axis=1), wos[...])
        z1[b] = zs4[b].reshape(n, c) + upd[:n]
        z1[b + 1] = zs4[b + 1].reshape(n, c) + upd[n:]
    def start_norm(b):
        for r in range(2):
            ub[b + r] = norm_t(z1[b + r].astype(BF).astype(F32).T)

    def start_mix(b, buf=s):
        for r in range(2):
            block_mix(buf, r, biasp, b // npair, vst, gb, ogb, b + r, b % npair + r, heads)

    def start_scores(b, buf=s):
        for r in range(2):
            block_scores(knp, qb, buf, r, b + r, b % npair + r, heads)

    def start_step(t, _):
        for by, stage in ((3, start_norm), (2, start_out), (1, start_mix), (0, start_scores)):
            if not isinstance(t, int) or 0 <= t - by < npair:
                stage(2 * (t - by))
        return _

    chunks = 4
    cols = rows // chunks
    groups = [(0, TILE), (TILE, TILE), (GROUP, GROUP)]
    near = [(0, GROUP), (GROUP, GROUP)]

    def h_copy(gi, ch, k, t, owner):
        r0, size = groups[gi]
        return remote(hsend.at[0, pl.ds(t % 2 * rows + ch * cols, cols), r0:r0 + size],
                      hcol.at[pl.ds(ch * cols, cols), pl.ds(pl.multiple_of(owner * rows + r0, TILE), size)],
                      out_s, h_r.at[ch], t)

    def near_copy(gi, owner):
        r0, size = near[gi]
        return remote(hsend.at[1, pl.ds(pl.multiple_of((1 - core) * rows, rows), rows), r0:r0 + size],
                      hcol.at[:, pl.ds(pl.multiple_of(owner * rows + r0, TILE), size)],
                      out_s, o_r, peers[2])

    def shuffle_rows(side, r0, size):
        def body(jb, _):
            j0 = pl.multiple_of(jb * TILE, TILE)
            parts = []
            for row in range(r0, r0 + size):
                b = side * npair + row // 2
                parts.append(z1[b:b + 1, pl.ds(row % 2 * half + j0, TILE)])
            blk = jnp.swapaxes(jnp.concatenate(parts, axis=0), 0, 1)
            hsend[side, pl.ds(j0, TILE), r0:r0 + size] = blk.astype(BF)
            return _
        lax.fori_loop(0, half // TILE, body, 0, unroll=8)

    def send_h(gi, chs):
        for ch in chs:
            for k in range(2):
                h_copy(gi, ch, k, peers[k], sp).start()

    start_project(0, 1)
    start_project(2, 3)
    start_scores(0)
    start_scores(2, s_next)
    arrived(ball.at[:, 0:rows], bs_r.at[1])
    start_bias(0)
    start_mix(0)
    start_mix(2, s_next)
    start_out(0)
    start_out(2)
    shuffle_rows(0, 0, TILE)
    send_h(0, range(chunks))
    start_project(4, 5)
    start_scores(4)
    start_project(6, 7)
    start_norm(0)
    start_mix(4)
    start_scores(6)
    start_project(TILE, 9)
    start_norm(2)
    start_out(4)
    start_mix(6)
    start_scores(TILE)
    start_project(10, 11)
    start_step(5, 0)
    shuffle_rows(0, TILE, TILE)
    send_h(1, range(chunks))
    for t in (6, 7):
        start_project(2 * t, 2 * t + 1)
        start_step(t, 0)
    start_step(TILE, 0)
    arrived(ball.at[:, 0:2 * rows], bs_r.at[0])
    start_bias(1)
    start_step(9, 0)
    shuffle_rows(0, GROUP, GROUP)
    send_h(2, [0])
    lax.fori_loop(10, 14, start_step, 0, unroll=4)
    shuffle_rows(1, 0, GROUP)
    near_copy(0, sp).start()
    start_step(14, 0)
    bias_rows(wbe8[...], ub, besend, 0, x == 1)
    end_bias_send(0)
    for t in range(15, npair + 3):
        start_step(t, 0)
    bias_rows(wbe8[...], ub, besend, 1, x == 1)
    end_bias_send(1)
    beall[:, pl.ds(mine, rows)] = besend[...]
    shuffle_rows(1, GROUP, GROUP)
    near_copy(1, sp).start()
    send_h(2, [1])
    hcol[:, pl.ds(mine, rows)] = hsend[1, pl.ds(pl.multiple_of(core * rows, rows), rows)]
    arrived(hcol.at[0:13], wsem.at[2])
    wqet[...] = wqe[...].T
    woet[...] = woe[...].T
    w1t[...] = w1[...].T
    w2t[...] = w2[...].T

    def end_delta(p):
        hid = jnp.maximum(dot(w1t[...], u2[p % 2]), 0.0).astype(BF)
        delta = (eb[p % 2] + dot(w2t[...], hid)).astype(BF)
        dsend[2 * p] = delta[:, :n].T
        dsend[2 * p + 1] = delta[:, n:].T

    def columns(p):
        return jnp.concatenate([hcol[2 * p].astype(F32).T, hcol[2 * p + 1].astype(F32).T], axis=1)

    def end_out(p):
        e = dot(woet[...], og[p])
        eb[p % 2] = e
        u2[p % 2] = norm_t(columns(p) + e)

    def end_mix(p):
        stage_mix(s, biast, qv, g, og, p, heads)

    def end_scores(p):
        turn_keys(kt, kn, p)
        stage_scores(kn, qv, s, p, heads)

    def end_project(p):
        project(wqet, norm_t(columns(p)), n, qv, kt, g, p)

    def end_step(t):
        for by, stage in ((4, end_delta), (3, end_out), (2, end_mix), (1, end_scores), (0, end_project)):
            if not isinstance(t, int) or 0 <= t - by < npair:
                stage(t - by)

    def d_copy(q, count, k, t, first_col):
        return remote(dsend.at[pl.ds(2 * q, 2 * count), pl.ds(pl.multiple_of(t * rows, rows), rows)],
                      drecv.at[pl.ds(first_col + 2 * q, 2 * count)], out_s, d_r.at[chunks if k == 2 else q // (npair // chunks)], t)

    my_cols = pl.multiple_of((2 * (1 - x) + core) * rows, rows)

    def send_d(q, count):
        for k, t in enumerate(peers):
            d_copy(q, count, k, t, my_cols).start()

    def wait_h(ch):
        arrived(hcol.at[pl.ds(ch * cols, cols), 0:2 * rows], h_r.at[ch])

    arrived(hcol.at[:, 0:rows], o_r)
    send_h(2, [2])
    end_bias_forward()
    send_h(2, [3])
    wait_h(0)
    end_step(0)
    end_step(1)
    arrived(beall.at[:, 0:rows], be_r.at[1])
    arrived(beall.at[:, 0:rows + GROUP], be_r.at[2])
    for h in range(heads):
        biast[:, h * n:(h + 1) * n] = beall[h].astype(F32) * LOG2E
    end_step(2)
    end_step(3)

    def segment(i, _):
        @pl.when(i % 2 == 0)
        def _wait():
            wait_h(i // 2)
        end_step(2 * i)
        end_step(2 * i + 1)
        send_d(2 * i - 4, 2)
        return _
    lax.fori_loop(2, npair // 2, segment, 0)
    for t in range(npair, npair + 4):
        end_step(t)
        send_d(t - 4, 1)
    drecv[pl.ds(my_cols, rows)] = dsend[:, pl.ds(mine, rows)]

    def final_block(side, owner_core, first_col, ch):
        j0 = pl.multiple_of(first_col + ch * cols, TILE)
        jj = owner_core * rows + ch * cols
        for gi in range(rows // GROUP):
            blk = jnp.swapaxes(drecv[pl.ds(j0, TILE), gi * GROUP:(gi + 1) * GROUP].astype(F32), 0, 1)
            for r in range(GROUP):
                row = GROUP * gi + r
                part = z1[side * npair + row // 2, pl.ds(pl.multiple_of(row % 2 * half + jj, TILE), TILE)]
                y[row, pl.ds(j0, TILE)] = part + blk[r]

    for ch in range(chunks):
        final_block(1, core, my_cols, ch)
    arrived(drecv.at[0:rows], d_r.at[chunks])
    for ch in range(chunks):
        final_block(1, 1 - core, pl.multiple_of((2 * (1 - x) + 1 - core) * rows, rows), ch)
    for ch in range(chunks):
        arrived(drecv.at[0:2 * cols], d_r.at[ch])
        for t in peers[:2]:
            final_block(0, t % 2, pl.multiple_of((2 * x + t % 2) * rows, rows), ch)
    sent(zs4.at[0:27], out_s)


def solution(mesh):
    row_spec = P(('dp', 'sp'), None, None)
    sp = mesh.shape['sp']

    def local_fn(pair_loc, wqs, wbs, wos, wqe, wbe, woe, w1, w2):
        rows, n, c = pair_loc.shape
        heads = wbs.shape[0]
        dma = pltpu.SemaphoreType.DMA
        vm = pltpu.VMEM
        weights = (wqs, wbs, wos, wqe, wbe, woe, w1, w2)
        npair = rows // 2
        args = (pair_loc.reshape(npair, 2, 2, n // 2, c),) + weights
        return pl.pallas_call(
            kernel,
            out_shape=vm(pair_loc.shape, F32),
            in_specs=[pl.BlockSpec(memory_space=pltpu.HBM)] * 9,
            out_specs=pl.BlockSpec(memory_space=vm),
            scratch_shapes=[
                vm((rows, 2, n // 2, c), F32), vm((rows, n, c), F32), vm((rows, c, n), BF), vm((rows, c, n), BF),
                vm((npair, 2, c, n), BF), vm((npair, 2, n, c), BF), vm((rows, c, n), F32), vm((rows, c, n), BF),
                vm((heads, rows, n), BF), vm((heads, n, n), BF), vm((2, n, heads * n), F32), vm((2, n // 2, rows, c), BF),
                vm((rows, n, c), BF), vm((npair, 2 * c, 2 * n), BF), vm((rows, n, c), BF), vm((npair, c, 2 * n), F32),
                vm((npair, c, 2 * n), BF), vm((heads, rows, n), BF), vm((heads, n, n), BF), vm((n, heads * n), F32),
                vm((rows, n, c), BF), vm((n, rows, c), BF), vm((2, n, heads * n), F32), vm((2, n, heads * n), F32),
                vm((2, c, 2 * n), F32), vm((2, c, 2 * n), BF), vm((c, 2 * n), BF), vm((2, 2, c, n), BF),
                *[vm(w.shape, BF) for w in weights],
                vm(wqs.shape[::-1], BF), vm(wqe.shape[::-1], BF), vm(woe.shape[::-1], BF),
                vm(w1.shape[::-1], BF), vm(w2.shape[::-1], BF),
                vm((heads * GROUP, TILE * c), BF), vm((heads * GROUP, TILE * c), BF),
                dma((4,)), dma((5,)), dma, dma((2,)), dma((4,)), dma, dma((3,)), dma((5,)),
            ],
            compiler_params=pltpu.CompilerParams(collective_id=0, has_side_effects=True, vmem_limit_bytes=36 * 2 ** 20),
            name="pair_block",
        )(*[pltpu.with_memory_space_constraint(a, pltpu.HBM) for a in args])

    return jax.shard_map(local_fn, mesh=mesh, in_specs=(row_spec,) + (P(),) * TILE, out_specs=row_spec, check_vma=False)
```
